32 devices in a mesh: cluster: 4 (over z), tm: 8 (over y, x, core).
Axes of the slice: x: 2, y: 2, z: 4, core: 2. Of those that a mesh axis runs over, the one named last changes fastest.
Arguments:
- obs: float32 [12, 512, 128], P('cluster', 'tm'), parts along dimension 0, may hold values from -6 to 6
- present: int32 [12, 512], P('cluster', 'tm'), parts along dimension 0, may hold values 0 or 1
- sensors: int32 [4], P('cluster'), parts along dimension 0, may hold values from 32 to 128
- log_prec: float32 [512], P('cluster'), parts along dimension 0, may hold values from -1 to 1
- dynamics: float32 [512, 128], P('cluster'), parts along dimension 0, may hold values from -1 to 1
- prior_var: float32 [512], P('cluster'), parts along dimension 0, may hold values from 0 to 0.06, as said below
- obs_map: float32 [512, 128], P('cluster'), parts along dimension 0, may hold values from -0.5 to 0.5
- init_state: float32 [12, 128], P('cluster'), parts along dimension 0, may hold values from -6 to 6
Outputs:
- smoothed: float32 [12, 512, 128], P('cluster', 'tm'), parts along dimension 0
- new_log_prec: float32 [512], P('cluster'), parts along dimension 0
- mean_loglik: float32 [4], P('cluster'), parts along dimension 0
The draws below stay inside these ranges and needn't reach their ends.
There are 4 independent parts, one for each index of `cluster`. The reference program is written for one: setup_inputs(seed, part) draws one part's arguments, and reference() takes and returns one part's arrays. A program takes and returns all parts, laid end to end along the dimension named above; each array names one. Nothing has to cross between parts.
Inputs may be any that keep to these rules, and one draw needn't show every extreme that they name: `prior_var`: positive variances.
All inputs are finite; a program needn't handle non-finite values. No bound on the sum of `present` on one device may be relied on, other than what follows from the above.
Results may differ from the reference program's by a relative error of at most 0.0003.
Values sent between devices are 32-bit elements; how exact they have to be, the bound alone decides.
A program may use at most 128 MiB of HBM per device.

```python
import math
import jax
import jax.numpy as jnp
from jax import lax

S = 128
P_SIZE = 128
SEQS = 3
STEPS = 512


def structure(key):
    folded = jax.random.fold_in(key, 31)
    subkeys = jax.random.split(folded, 4)
    share = 0.5
    slow_mask = jax.random.uniform(subkeys[0], (S,)) < share
    slow_rate = jnp.exp(jnp.log(0.3) / STEPS)
    memory_steps = jax.random.uniform(subkeys[1], (S,), minval=30.0, maxval=50.0)
    decay_rates = jnp.where(slow_mask, slow_rate, jnp.exp(-1.0 / memory_steps))
    same_group = (slow_mask[:, None] == slow_mask[None, :]).astype(jnp.float32)
    mixing_noise = jax.random.normal(subkeys[2], (S, S)) * (0.35 / math.sqrt(S))
    initial = (jnp.eye(S, dtype=jnp.float32) + mixing_noise * same_group) / 1.8

    def refine(repeat, matrix):
        cubic = jnp.dot(jnp.dot(matrix, matrix.T, precision=lax.Precision.HIGHEST), matrix, precision=lax.Precision.HIGHEST)
        return 1.5 * matrix - 0.5 * cubic
    rotation = lax.fori_loop(0, 40, refine, initial)
    transition = decay_rates[:, None] * rotation
    variances = jnp.where(slow_mask, 0.3 / STEPS, 0.05) * jax.random.uniform(subkeys[3], (S,), minval=0.9, maxval=1.1)
    return (transition.astype(jnp.float32), variances.astype(jnp.float32))


def draw_dynamics(key, part):
    return structure(key)[0]


def draw_prior_var(key, part):
    return structure(key)[1]


def set_ends(entries, key, smallest, high):
    dims = entries.shape
    place = [jax.random.randint(jax.random.fold_in(key, axis), (), 0, dims[axis]) for axis in range(len(dims))]
    entries = entries.at[tuple(place)].set(smallest)
    longest = dims.index(max(dims))
    place[longest] = (place[longest] + 1) % dims[longest]
    return entries.at[tuple(place)].set(high)


def steps_of(own_key, dims, shards, least, high):
    def one(position, shards_of):
        steps = jax.random.uniform(jax.random.fold_in(jax.random.fold_in(own_key, 6), position), (shards_of,), jnp.float32, least / len(shards), high / len(shards))
        return jnp.repeat(jnp.exp(steps), dims[position] // shards_of).reshape((-1,) + (1,) * (len(dims) - position - 1))

    level = one(*shards[0])
    for cut in shards[1:]:
        level = level * one(*cut)
    return level


def normal_values(rng, shape, spread, bound, cuts=(), held_as=jnp.bfloat16):
    entries = jax.random.normal(rng, shape, jnp.float32) * spread
    if len(cuts) > 0:
        entries = steps_of(rng, shape, cuts, -0.22, 0.18) * entries
    return jnp.clip(entries, min=-bound, max=bound).astype(held_as)


def setup_inputs(seed: int = 0, part: int = 0) -> dict:
    splits = jax.random.split(jax.random.key(seed), 9)
    own_keys = jax.random.split(jax.random.fold_in(splits[8], part), 9)
    obs = normal_values(own_keys[0], (SEQS, STEPS, P_SIZE), 1.0, 6.0, ((1, 8),), jnp.float32)
    present = set_ends((jax.random.randint(own_keys[1], (SEQS, STEPS), 0, 5) < 4).astype(jnp.int32), jax.random.fold_in(own_keys[1], 1), 0, 1)
    sensors = jax.random.randint(own_keys[2], (1,), P_SIZE // 4, P_SIZE + 1).astype(jnp.int32)
    log_prec = jnp.clip(jax.random.uniform(own_keys[3], (P_SIZE,), jnp.float32, -1.0, 1.0), -1.0, 1.0)
    dynamics = draw_dynamics(jax.random.fold_in(jax.random.fold_in(splits[8], part), 71), part)
    prior_var = draw_prior_var(jax.random.fold_in(jax.random.fold_in(splits[8], part), 71), part)
    obs_map = normal_values(own_keys[6], (P_SIZE, S), S ** -0.5, 0.5, (), jnp.float32)
    init_state = normal_values(own_keys[7], (SEQS, S), 1.0, 6.0, (), jnp.float32)
    return dict(obs=obs, present=present, sensors=sensors, log_prec=log_prec, dynamics=dynamics, prior_var=prior_var, obs_map=obs_map, init_state=init_state)


def reference(obs, present, sensors, log_prec, dynamics, prior_var, obs_map, init_state):
    highest = lax.Precision.HIGHEST
    channel_on = (jnp.arange(P_SIZE) < sensors[0]).astype(jnp.float32)
    sensor_precision = jnp.exp(log_prec)
    gain_matrix = prior_var[:, None] * (obs_map.T * (sensor_precision * channel_on)[None, :])
    outputs = []
    gradient = jnp.zeros((P_SIZE,), jnp.float32)
    loglik = jnp.zeros((), jnp.float32)
    for sequence in range(SEQS):
        def forward(carried, inputs):
            reading, flag = inputs
            predicted = jnp.dot(dynamics, carried, precision=highest)
            innovation = channel_on * (reading - jnp.dot(obs_map, predicted, precision=highest))
            updated = predicted + flag.astype(jnp.float32) * jnp.dot(gain_matrix, innovation, precision=highest)
            return updated, (updated, innovation)

        last_state, (filtered, innovations) = lax.scan(forward, init_state[sequence], (obs[sequence], present[sequence]))

        def backward(later, current):
            moved = later - jnp.dot(dynamics, current, precision=highest)
            smooth = current + jnp.dot(dynamics.T, moved, precision=highest)
            return smooth, smooth

        boundary = jnp.dot(dynamics, last_state, precision=highest)
        ignored, smooth_states = lax.scan(backward, boundary, filtered, reverse=True)
        outputs.append(smooth_states)
        observed = present[sequence].astype(jnp.float32)[:, None]
        weighted = sensor_precision * innovations * innovations
        gradient = gradient + 0.5 * jnp.sum(observed * channel_on * (1.0 - weighted), axis=0)
        loglik = loglik + 0.5 * jnp.sum(observed * channel_on * (log_prec - weighted))
    count_all = SEQS * STEPS
    smoothed = jnp.stack(outputs)
    new_log_prec = log_prec + gradient / count_all
    mean_loglik = (loglik / (count_all * P_SIZE)).reshape(1)
    return smoothed, new_log_prec, mean_loglik
```

```python
import functools
import math

import jax
import jax.numpy as jnp
from jax import lax
from jax.experimental import pallas as pl
from jax.experimental.pallas import tpu as pltpu
from jax.sharding import PartitionSpec as P

F32 = jnp.float32
BF16 = jnp.bfloat16
MESH = pl.DeviceIdType.MESH
WORD = 4


def stacked(a):
    high = a.astype(BF16).astype(F32)
    return jnp.concatenate([high, a - high], axis=0).astype(BF16)


def twice(s):
    return jnp.concatenate([s, s], axis=1)


def product(left, right):
    full = jnp.dot(left, right, preferred_element_type=F32)
    rows = full.shape[0] // 2
    return full[:rows] + full[rows:]


def times(a, right):
    return product(twice(stacked(a)), right)


def over(count, width, body):
    if count <= width:
        for i in range(count):
            body(i)
        return
    assert count % width == 0

    def step(lap, _):
        for i in range(width):
            body(lap * width + i)
        return 0

    lax.fori_loop(0, count // width, step, 0)


def kernel(
    n, seqs, steps,
    present_s, sensors_s, obs, present_v, log_prec, dyn, prior_var, obs_map, init,
    out, new_prec, loglik,
    words, table, nodes, vecs, ents, heads, head_vecs, power_rows, power_cols, lap_rhs, pair_rhs, step_rhs, drive, mask, offs, prior, filt,
    suffix, chunk8, in_buf, out_buf, off_buf, off_in, sum_buf, sum_in,
    chain_sem, off_send, off_recv, sum_send, sum_recv,
):
    pos = lax.axis_index("tm")
    states = dyn.shape[0]
    chunks = steps // WORD
    total = seqs * chunks
    levels = int(math.log2(chunks))
    first = [0]
    for level in range(1, levels + 1):
        first.append(first[-1] + (total >> (level - 1) if level > 1 else 0))

    in_buf[...] = jnp.zeros_like(in_buf)
    off_in[...] = jnp.zeros_like(off_in)
    barrier = pltpu.get_barrier_semaphore()
    for d in range(1, n):
        pl.semaphore_signal(barrier, inc=1, device_id={"tm": lax.rem(pos + d, n)}, device_id_type=MESH)

    lane = lax.broadcasted_iota(jnp.int32, (1, states), 1)
    active = (lane < sensors_s[0]).astype(F32)
    weight = jnp.exp(log_prec[...])
    weight_on = weight * active
    pv = prior_var[...]
    d_mat = dyn[...]
    d_t = d_mat.T
    h_mat = obs_map[...]
    h_rhs = stacked(h_mat)
    d_rhs = stacked(d_mat)
    readout = times(h_mat, d_rhs).T
    f_t = d_t - times(readout * weight_on, h_rhs) * pv

    for b in range(seqs):
        def word(k, b=b):
            t = k * WORD
            w = present_s[b, t]
            for i in range(1, WORD):
                w = w * 2 + present_s[b, t + i]
            words[b * chunks + k] = w
        over(chunks, 16, word)
        row = jnp.broadcast_to(present_v[b : b + 1, :].astype(F32), (steps, steps))
        same = lax.broadcasted_iota(jnp.int32, (steps, steps), 0) == lax.broadcasted_iota(jnp.int32, (steps, steps), 1)
        column = jnp.sum(jnp.where(same, row, 0.0), axis=1, keepdims=True)
        mask[b * steps : (b + 1) * steps, :] = jnp.broadcast_to(column, (steps, states))

    drive[...] = times(obs[...] * weight_on, h_rhs) * pv * mask[...]

    both = jnp.concatenate([d_t, f_t], axis=1)
    step_rhs[...] = stacked(both)
    pairs = []
    for a in (d_t, f_t):
        pairs.append(times(a, step_rhs[...]))
    pair_rhs[...] = stacked(jnp.concatenate(pairs, axis=1))
    for a in range(4):
        rows = pairs[a // 2][:, (a % 2) * states : (a % 2 + 1) * states]
        quad = times(rows, pair_rhs[...])
        for c in range(4):
            table[a * 4 + c] = stacked(quad[:, c * states : (c + 1) * states])

    def at(ref, i):
        return ref[pl.ds(i, total, stride=WORD), :]

    def advance(x, i):
        y = times(x, step_rhs[...])
        return jnp.where(at(mask, i) > 0.5, y[:, states:], y[:, :states]) + at(drive, i)

    x = at(drive, 0)
    for i in range(1, WORD):
        x = advance(x, i)
    offs[...] = x

    eye = (
        lax.broadcasted_iota(jnp.int32, (states, states), 0)
        == lax.broadcasted_iota(jnp.int32, (states, states), 1)
    ).astype(F32)
    residual = eye - times(d_t, d_rhs)
    by_one = times(jnp.concatenate([residual, d_mat], axis=0), d_rhs)
    r_1, d_2 = by_one[:states], by_one[states:]
    by_two = times(jnp.concatenate([residual, r_1, d_mat, d_2], axis=0), stacked(d_2))
    r_2, r_3 = by_two[:states], by_two[states : 2 * states]
    d_3, d_4 = by_two[2 * states : 3 * states], by_two[3 * states :]
    tail_rhs = stacked(jnp.concatenate([residual, r_1, r_2, r_3], axis=1))
    fill_rhs = stacked(jnp.concatenate([d_4, d_3, d_2, d_mat], axis=1))

    def keep_power(e, stack):
        if e < chunks:
            power_rows[e * 2 * states : (e + 1) * 2 * states, :] = stack
            power_cols[:, (chunks - 1 - e) * states : (chunks - e) * states] = stack
        else:
            lap_rhs[0 : 2 * states, :] = stack

    def power_of(e):
        return power_rows[e * 2 * states : (e + 1) * 2 * states, :]

    keep_power(0, stacked(eye))
    keep_power(1, stacked(d_4))

    for level in range(1, levels + 1):
        base, below = first[level], first[level - 1]

        def compose(j, level=level, base=base, below=below):
            if level == 1:
                left, right = table[words[2 * j]], table[words[2 * j + 1]]
                v_left, v_right = offs[pl.ds(2 * j, 1), :], offs[pl.ds(2 * j + 1, 1), :]
            else:
                left, right = nodes[below + 2 * j], nodes[below + 2 * j + 1]
                v_left, v_right = vecs[pl.ds(below + 2 * j, 1), :], vecs[pl.ds(below + 2 * j + 1, 1), :]
            rows = jnp.concatenate([left, stacked(jnp.broadcast_to(v_left, (8, states)))], axis=0)
            y = jnp.dot(twice(rows), right, preferred_element_type=F32)
            nodes[base + j] = stacked(y[:states] + y[states : 2 * states])
            vecs[pl.ds(base + j, 1), :] = (
                y[2 * states : 2 * states + 1] + y[2 * states + 8 : 2 * states + 9] + v_right
            )

        over(total >> level, total, compose)
        half = power_of(1 << (level - 1))
        keep_power(1 << level, stacked(product(twice(half), half)))

    def prepare():
        for b in range(seqs):
            rows = slice(b * 2 * states, (b + 1) * 2 * states)
            heads[rows, 0:states] = stacked(eye)
            for level in range(levels, 0, -1):
                for p in range(chunks >> level):
                    j = b * (chunks >> (level - 1)) + 2 * p
                    k = (p << level) + (1 << (level - 1))
                    if level == 1:
                        mat, v = table[words[j]], offs[j : j + 1, :]
                    else:
                        j = first[level - 1] + j
                        mat, v = nodes[j], vecs[j : j + 1, :]
                    if p > 0:
                        before = p << level
                        e_rows = head_vecs[b * chunks + before : b * chunks + before + 1, :]
                        left = jnp.concatenate(
                            [heads[rows, before * states : (before + 1) * states],
                             stacked(jnp.broadcast_to(e_rows, (8, states)))], axis=0)
                        y = jnp.dot(twice(left), mat, preferred_element_type=F32)
                        mat = stacked(y[:states] + y[states : 2 * states])
                        v = y[2 * states : 2 * states + 1] + y[2 * states + 8 : 2 * states + 9] + v
                    heads[rows, k * states : (k + 1) * states] = mat
                    head_vecs[b * chunks + k : b * chunks + k + 1, :] = v
        for level in range(1, levels):
            base = power_of(1 << level)
            for e in range(1, 1 << level):
                keep_power((1 << level) + e, stacked(product(twice(power_of(e)), base)))
        for d in range(1, n - 2):
            half = (d + 1) // 2 - 1
            other = d - 1 - half
            lap_rhs[d * 2 * states : (d + 1) * 2 * states, :] = stacked(
                product(
                    twice(lap_rhs[half * 2 * states : (half + 1) * 2 * states, :]),
                    lap_rhs[other * 2 * states : (other + 1) * 2 * states, :],
                )
            )

    head_vecs[...] = jnp.zeros_like(head_vecs)
    early = n // 2

    @pl.when(pos >= early)
    def _():
        prepare()

    pl.semaphore_wait(barrier, n - 1)
    row8 = lax.broadcasted_iota(jnp.int32, (8, states), 0)

    chain = pltpu.make_async_remote_copy(
        src_ref=out_buf, dst_ref=in_buf, send_sem=chain_sem.at[0], recv_sem=chain_sem.at[1],
        device_id={"tm": lax.rem(pos + 1, n)}, device_id_type=MESH,
    )

    @pl.when(pos == 0)
    def _():
        in_buf[0:seqs, :] = init[...]

    @pl.when(pos > 0)
    def _():
        chain.wait_recv()

    entering = in_buf[...]
    top = first[levels]
    left = jnp.concatenate(
        [twice(stacked(jnp.where(row8 == b, entering, 0.0))) for b in range(seqs)], axis=1
    )

    @pl.when(pos < n - 1)
    def _():
        leaving = product(left, nodes[top : top + seqs].reshape(seqs * 2 * states, states))
        for b in range(seqs):
            leaving = leaving + jnp.where(row8 == b, vecs[top + b : top + b + 1, :], 0.0)
        out_buf[...] = leaving
        chain.start()

    @pl.when(pos < early)
    def _():
        prepare()

    y = product(left, heads[...])
    for k in range(chunks):
        ents[pl.ds(k, seqs, stride=chunks), :] = y[0:seqs, k * states : (k + 1) * states]
    x = ents[...] + head_vecs[...]
    for i in range(WORD):
        prior[i * total : (i + 1) * total, :] = x
        x = advance(x, i)
        filt[i * total : (i + 1) * total, :] = x

    y = times(filt[...], tail_rhs)

    def part(i, k):
        return y[i * total : (i + 1) * total, k * states : (k + 1) * states]

    chunk8[...] = jnp.zeros_like(chunk8)
    for i in range(WORD):
        z = part(i, 0)
        for j in range(i + 1, WORD):
            z = z + part(j, j - i)
        suffix[i * total : (i + 1) * total, :] = z
        if i == 0:
            for b in range(seqs):
                chunk8[pl.ds(b, chunks, stride=8), :] = z[b * chunks : (b + 1) * chunks]

    last = jnp.zeros((8, states), F32)
    for b in range(seqs):
        r = (WORD - 1) * total + (b + 1) * chunks - 1
        last = jnp.where(row8 == b, jnp.broadcast_to(filt[r : r + 1, :], (8, states)), last)
    final = times(last, stacked(d_t))
    ends = chunk8[...].reshape(chunks, 8, states)
    left = jnp.concatenate([twice(stacked(ends[k])) for k in range(chunks)], axis=1)
    own = product(left, power_rows[...])
    own = own + jnp.where(pos == n - 1, times(final, lap_rhs[0 : 2 * states, :]), 0.0)
    off_buf[...] = own

    def send_off(d):
        return pltpu.make_async_remote_copy(
            src_ref=off_buf, dst_ref=off_in.at[d], send_sem=off_send.at[d], recv_sem=off_recv.at[d],
            device_id={"tm": lax.rem(pos + n - 1 - d, n)}, device_id_type=MESH,
        )

    for d in range(n - 1):
        @pl.when(pos - 1 - d >= 0)
        def _(d=d):
            send_off(d).start()

    obs_rows = [at(obs, i) for i in range(WORD)]
    mask_rows = [at(mask, i) for i in range(WORD)]
    errors = jnp.concatenate(obs_rows, axis=0) - times(prior[...], stacked(readout))
    seen = jnp.concatenate(mask_rows, axis=0)
    squares = jnp.sum(seen * active * errors * errors, axis=0, keepdims=True)
    number = jnp.sum(seen, axis=0, keepdims=True)
    sums = jnp.where(row8 == 0, jnp.broadcast_to(squares, (8, states)), jnp.broadcast_to(number, (8, states)))
    sum_buf[...] = sums

    def send_sum(d):
        return pltpu.make_async_remote_copy(
            src_ref=sum_buf, dst_ref=sum_in.at[d], send_sem=sum_send.at[d], recv_sem=sum_recv.at[d],
            device_id={"tm": lax.rem(pos + d + 1, n)}, device_id_type=MESH,
        )

    for d in range(n - 1):
        send_sum(d).start()

    ups = [ends]
    for level in range(levels):
        pair = ups[-1].reshape(ups[-1].shape[0] // 2, 2, 8, states)
        half = pair.shape[0]
        later = times(pair[:, 1].reshape(half * 8, states), power_of(1 << level))
        ups.append(pair[:, 0] + later.reshape(half, 8, states))
    x = jnp.zeros((1, 8, states), F32)
    for level in range(levels - 1, -1, -1):
        count = x.shape[0]
        pair = ups[level].reshape(count, 2, 8, states)
        if level == levels - 1:
            sooner = pair[:, 1]
        else:
            moved = times(x.reshape(count * 8, states), power_of(1 << level))
            sooner = moved.reshape(count, 8, states) + pair[:, 1]
        x = jnp.stack([sooner, x], axis=1).reshape(2 * count, 8, states)
    chunk8[...] = x.reshape(chunks * 8, states)

    for d in range(n - 1):
        @pl.when(pos + 1 + d < n)
        def _(d=d):
            send_off(d).wait_recv()

    left = jnp.concatenate([twice(stacked(off_in[d])) for d in range(1, n - 1)], axis=1)
    x = jnp.where(pos == n - 1, final, off_in[0] + product(left, lap_rhs[...]))
    y = times(x, power_cols[...])
    for k in range(chunks):
        chunk8[k * 8 : (k + 1) * 8, :] += y[:, k * states : (k + 1) * states]
    x = jnp.concatenate([chunk8[pl.ds(b, chunks, stride=8), :] for b in range(seqs)], axis=0)
    y = times(x, fill_rhs)
    for i in range(WORD):
        out[pl.ds(i, total, stride=WORD), :] = (
            suffix[i * total : (i + 1) * total, :] + y[:, i * states : (i + 1) * states]
        )

    for d in range(n - 1):
        send_sum(d).wait_recv()
        sums = sums + sum_in[d]
    squares, number = sums[0:1], sums[1:2]
    grad = 0.5 * active * (number - weight * squares)
    new_prec[...] = log_prec[...] + grad / (seqs * steps * n)
    terms = 0.5 * active * (log_prec[...] * number - weight * squares)
    loglik[...] = jnp.zeros_like(terms) + jnp.sum(terms, axis=1, keepdims=True) / (seqs * steps * n * states)

    @pl.when(pos < n - 1)
    def _():
        chain.wait_send()

    for d in range(n - 1):
        @pl.when(pos - 1 - d >= 0)
        def _(d=d):
            send_off(d).wait_send()
        send_sum(d).wait_send()


def finish(smoothed, new_prec, loglik, out, out_prec, out_loglik):
    out[...] = smoothed[...]
    out_prec[...] = new_prec[...]
    out_loglik[...] = loglik[:, 0:1]


def local(n, obs, present, sensors, log_prec, dynamics, prior_var, obs_map, init_state):
    seqs, steps, channels = obs.shape
    states = dynamics.shape[0]
    chunks = steps // WORD
    total = seqs * chunks
    inner = sum(total >> level for level in range(1, int(math.log2(chunks)) + 1))
    vmem = pl.BlockSpec(memory_space=pltpu.VMEM)
    smem = pl.BlockSpec(memory_space=pltpu.SMEM)
    rows = seqs * steps
    smoothed, new_prec, loglik = pl.pallas_call(
        functools.partial(kernel, n, seqs, steps),
        out_shape=(
            pltpu.VMEM((rows, states), F32),
            pltpu.VMEM((1, channels), F32),
            pltpu.VMEM((1, channels), F32),
        ),
        in_specs=[smem, smem] + [vmem] * 7,
        out_specs=(vmem, vmem, vmem),
        scratch_shapes=[
            pltpu.SMEM((total,), jnp.int32),
            pltpu.VMEM((2**WORD, 2 * states, states), BF16),
            pltpu.VMEM((inner, 2 * states, states), BF16),
            pltpu.VMEM(((inner + 7) // 8 * 8, states), F32),
            pltpu.VMEM((total, states), F32),
            pltpu.VMEM((seqs * 2 * states, chunks * states), BF16),
            pltpu.VMEM((total, states), F32),
            pltpu.VMEM((chunks * 2 * states, states), BF16),
            pltpu.VMEM((2 * states, chunks * states), BF16),
            pltpu.VMEM(((n - 2) * 2 * states, states), BF16),
            pltpu.VMEM((2 * states, 4 * states), BF16),
            pltpu.VMEM((2 * states, 2 * states), BF16),
            pltpu.VMEM((rows, states), F32),
            pltpu.VMEM((rows, states), F32),
            pltpu.VMEM((total, states), F32),
            pltpu.VMEM((rows, states), F32),
            pltpu.VMEM((rows, states), F32),
            pltpu.VMEM((rows, states), F32),
            pltpu.VMEM((chunks * 8, states), F32),
            pltpu.VMEM((8, states), F32),
            pltpu.VMEM((8, states), F32),
            pltpu.VMEM((8, states), F32),
            pltpu.VMEM((n, 8, states), F32),
            pltpu.VMEM((8, states), F32),
            pltpu.VMEM((n, 8, states), F32),
            pltpu.SemaphoreType.DMA((2,)),
            pltpu.SemaphoreType.DMA((n,)),
            pltpu.SemaphoreType.DMA((n,)),
            pltpu.SemaphoreType.DMA((n,)),
            pltpu.SemaphoreType.DMA((n,)),
        ],
        compiler_params=pltpu.CompilerParams(collective_id=0, has_side_effects=True),
        name="kalman",
    )(
        present, sensors, obs.reshape(rows, channels), present, log_prec.reshape(1, channels),
        dynamics, prior_var.reshape(1, states), obs_map, init_state,
    )
    held = [pltpu.with_memory_space_constraint(a, pltpu.VMEM) for a in (smoothed, new_prec, loglik)]
    smoothed, new_prec, loglik = pl.pallas_call(
        finish,
        out_shape=(
            jax.ShapeDtypeStruct((rows, states), F32),
            jax.ShapeDtypeStruct((1, channels), F32),
            jax.ShapeDtypeStruct((1, 1), F32),
        ),
        in_specs=[vmem] * 3,
        out_specs=(vmem, vmem, vmem),
        name="finish",
    )(*held)
    return smoothed.reshape(seqs, steps, states), new_prec.reshape(channels), loglik.reshape(1)


def solution(mesh):
    in_specs = (
        P("cluster", "tm", None),
        P("cluster", "tm"),
        P("cluster"),
        P("cluster"),
        P("cluster", None),
        P("cluster"),
        P("cluster", None),
        P("cluster", None),
    )
    out_specs = (P("cluster", "tm", None), P("cluster"), P("cluster"))
    body = functools.partial(local, mesh.shape["tm"])
    return jax.shard_map(body, mesh=mesh, in_specs=in_specs, out_specs=out_specs, check_vma=False)
```

```python
import functools
import math

import jax
import jax.numpy as jnp
from jax import lax
from jax.experimental import pallas as pl
from jax.experimental.pallas import tpu as pltpu
from jax.sharding import PartitionSpec as P

F32 = jnp.float32
BF16 = jnp.bfloat16
MESH = pl.DeviceIdType.MESH
WORD = 4
EXTRA = 8


def split(a):
    high = a.astype(BF16).astype(F32)
    return jnp.concatenate([high, a - high], axis=1).astype(BF16)


def stacked(a):
    high = a.astype(BF16).astype(F32)
    return jnp.concatenate([high, a - high], axis=0).astype(BF16)


def deep(node):
    return jnp.concatenate([node, node], axis=0)


def tall(node):
    width = node.shape[1] // 2
    return jnp.concatenate([node[:, :width], node[:, width:]], axis=0)


def twice(s):
    return jnp.concatenate([s, s], axis=1)


def product(left, right):
    full = jnp.dot(left, right, preferred_element_type=F32)
    rows = full.shape[0] // 2
    return full[:rows] + full[rows:]


def times(a, right):
    return product(twice(stacked(a)), right)


def wide(left, right):
    full = jnp.dot(left, right, preferred_element_type=F32)
    half = left.shape[1] // 2 if left.shape[1] < 256 else 128
    return [
        full[:, 2 * k * half : (2 * k + 1) * half] + full[:, (2 * k + 1) * half : (2 * k + 2) * half]
        for k in range(full.shape[1] // (2 * half))
    ]


def mul(a, node):
    return wide(split(a), deep(node))[0]


def kernel(
    n, seqs, steps,
    present_s, sensors_s, obs, present_v, log_prec, dyn, prior_var, obs_map, init,
    out, new_prec, loglik,
    words, table, theta, theta_4, nodes, vecs, psi_f, psi_n, us, offs, u_rows, u_4, ents, powers, laps, step_rhs,
    drive, mask, prior, filt, suffix, chunk8,
    even_node, even_v, pair_node, pair_v, prev_node, prev_v, omega_node, omega_v, psi_own, psi_v, state,
    vec_in, vec_out, vec_back, mat_out, mat_in, comp_out, comp_in, psi_out, psi_in,
    off_out, off_in, near_out, near_in, sum_buf, sum_in,
    vec_send, vec_recv, mat_sem, comp_sem, psi_sem, near_sem, off_send, off_recv, sum_send, sum_recv,
):
    pos = lax.axis_index("tm")
    par = lax.rem(pos, 2)
    quarter = lax.rem(pos, 4)
    chip = lax.div(pos, 2)
    chips = n // 2
    states = dyn.shape[0]
    block = states + EXTRA
    chunks = steps // WORD
    total = seqs * chunks
    levels = int(math.log2(chunks))
    first = [0]
    for level in range(1, levels + 1):
        first.append(first[-1] + (total >> (level - 1) if level > 1 else 0))
    top = first[levels]

    vec_in[...] = jnp.zeros_like(vec_in)
    off_in[...] = jnp.zeros_like(off_in)
    near_in[...] = jnp.zeros_like(near_in)
    barrier = pltpu.get_barrier_semaphore()
    for d in range(1, n):
        pl.semaphore_signal(barrier, inc=1, device_id={"tm": lax.rem(pos + d, n)}, device_id_type=MESH)

    lane = lax.broadcasted_iota(jnp.int32, (1, states), 1)
    row8 = lax.broadcasted_iota(jnp.int32, (8, states), 0)
    active = (lane < sensors_s[0]).astype(F32)
    weight = jnp.exp(log_prec[...])
    weight_on = weight * active
    pv = prior_var[...]
    d_mat = dyn[...]
    d_t = d_mat.T
    h_mat = obs_map[...]
    h_2 = split(h_mat)
    d_2n = split(d_mat)
    d_t2 = split(d_t)
    readout = wide(d_t2, deep(split(h_mat.T)))[0]
    f_t = d_t - mul(readout * weight_on, h_2) * pv
    f_t2 = split(f_t)

    for b in range(seqs):
        for k in range(chunks):
            t = k * WORD
            w = present_s[b, t]
            for i in range(1, WORD):
                w = w * 2 + present_s[b, t + i]
            words[b * chunks + k] = w
        row = jnp.broadcast_to(present_v[b : b + 1, :].astype(F32), (steps, steps))
        same = lax.broadcasted_iota(jnp.int32, (steps, steps), 0) == lax.broadcasted_iota(jnp.int32, (steps, steps), 1)
        column = jnp.sum(jnp.where(same, row, 0.0), axis=1, keepdims=True)
        mask[b * steps : (b + 1) * steps, :] = jnp.broadcast_to(column, (steps, states))

    drive[...] = mul(obs[...] * weight_on, h_2) * pv * mask[...]

    step_rhs[...] = stacked(jnp.concatenate([d_t, f_t], axis=1))
    singles = [d_t2, f_t2]
    both = deep(jnp.concatenate(singles, axis=1))
    pairs = []
    for a in range(2):
        pairs += [split(q) for q in wide(singles[a], both)]
    quad_rhs = deep(jnp.concatenate(pairs, axis=1))
    for a in range(4):
        quad = wide(pairs[a], quad_rhs)
        for c in range(4):
            table[a * 4 + c] = split(quad[c])

    def at(ref, i):
        return ref[pl.ds(i, total, stride=WORD), :]

    def advance(x, i):
        y = times(x, step_rhs[...])
        return jnp.where(at(mask, i) > 0.5, y[:, states:], y[:, :states]) + at(drive, i)

    zero_states = [at(drive, 0)]
    for i in range(1, WORD):
        zero_states.append(advance(zero_states[-1], i))
    offs[...] = zero_states[-1]

    def leading(matrix, v):
        return jnp.concatenate([matrix, split(jnp.broadcast_to(v, (16, states)))], axis=0)

    def child(level, j):
        if level == 1:
            return table[words[j]], offs[j : j + 1, :]
        j = first[level - 1] + j
        return nodes[j], vecs[j : j + 1, :]

    for level in range(1, levels + 1):
        for j in range(total >> level):
            left, v_left = child(level, 2 * j)
            right, v_right = child(level, 2 * j + 1)
            y = wide(leading(left, v_left), deep(right))[0]
            j = first[level] + j
            v = y[states : states + EXTRA] + v_right
            nodes[j] = split(y[:states])
            vecs[j : j + 1, :] = v[0:1]
            if level == levels:
                b = j - top
                mat_out[b * block : b * block + states, :] = y[:states]
                mat_out[b * block + states : (b + 1) * block, :] = v

    def lefts(x):
        return jnp.concatenate([twice(stacked(jnp.where(row8 == b, x, 0.0))) for b in range(seqs)], axis=1)

    def apply(left, node, v):
        rhs = jnp.concatenate([tall(node[b]) for b in range(seqs)], axis=0)
        return product(left, rhs) + v

    def rows_of(ref):
        v = jnp.zeros((8, states), F32)
        for b in range(seqs):
            v = jnp.where(row8 == b, ref[b * block + states : (b + 1) * block, :], v)
        return v

    own = nodes.at[pl.ds(top, seqs)]

    def own_v():
        v = jnp.zeros((8, states), F32)
        for b in range(seqs):
            v = jnp.where(row8 == b, vecs[top + b : top + b + 1, :], v)
        return v

    def send_vec(src, slot, to):
        return pltpu.make_async_remote_copy(
            src_ref=src, dst_ref=vec_in, send_sem=vec_send.at[slot], recv_sem=vec_recv,
            device_id={"tm": to}, device_id_type=MESH,
        )

    def shift(by):
        return lax.rem(pos + (by + n), n)

    def send_mat(src, dst, sem, by):
        return pltpu.make_async_remote_copy(
            src_ref=src, dst_ref=dst, send_sem=sem.at[0], recv_sem=sem.at[1],
            device_id={"tm": shift(by)}, device_id_type=MESH,
        )

    mat = send_mat(mat_out, mat_in, mat_sem, 1)
    comp = send_mat(comp_out, comp_in, comp_sem, 2)
    psi = send_mat(psi_out, psi_in, psi_sem, 1)
    near = send_mat(near_out, near_in, near_sem, -1)
    to_next = [send_vec(vec_out, k, shift(by)) for k, by in enumerate((1, 2, 4))]
    to_back = send_vec(vec_back, 3, shift(-1))

    even = par == 0
    odd = par == 1
    has_mat = jnp.logical_and(odd, pos >= 2)
    gives_mat = jnp.logical_and(even, pos >= 2)
    gives_comp = jnp.logical_and(quarter == 1, pos >= 4)
    has_comp = jnp.logical_and(quarter == 3, pos >= 4)
    last_of_four = jnp.logical_and(quarter == 3, pos < n - 1)

    pl.semaphore_wait(barrier, n - 1)

    @pl.when(gives_mat)
    def _():
        mat.start()

    @pl.when(pos == 0)
    def _():
        vec_in[0:seqs, :] = init[...]
        vec_out[...] = apply(lefts(vec_in[...]), own, own_v())
        to_next[0].start()

    eye = (
        lax.broadcasted_iota(jnp.int32, (states, states), 0)
        == lax.broadcasted_iota(jnp.int32, (states, states), 1)
    ).astype(F32)
    residual = eye - mul(d_t, d_2n)
    r_1, d_2 = [mul(a, d_2n) for a in (residual, d_mat)]
    d_2s = split(d_2)
    r_2, r_3, d_3, d_4 = [mul(a, d_2s) for a in (residual, r_1, d_mat, d_2)]
    d_4s = split(d_4)
    tails = [split(a) for a in (residual, r_1, r_2, r_3)]
    powers[0] = split(eye)
    powers[1] = d_4s
    left = jnp.concatenate([twice(stacked(z)) for z in zero_states], axis=1)
    u = product(left, jnp.concatenate([tall(a) for a in tails], axis=0))
    u_rows[...] = u
    u_4[...] = times(u, tall(d_4s))
    theta_2 = []
    for a in range(4):
        left = jnp.concatenate([singles[a // 2], pairs[a]], axis=1)
        rhs = jnp.concatenate([deep(tails[0]), deep(tails[1])], axis=0)
        theta_2.append(wide(left, rhs)[0])
    theta_rhs = deep(jnp.concatenate([split(mul(a, d_2s)) for a in theta_2], axis=1))
    for a in range(4):
        full = wide(pairs[a], theta_rhs)
        for c in range(4):
            whole = theta_2[a] + full[c]
            theta[a * 4 + c] = whole
            theta_4[a * 4 + c] = split(mul(whole, d_4s))

    @pl.when(pos == 1)
    def _():
        to_back.wait_recv()
        vec_out[...] = apply(lefts(vec_in[...]), own, own_v())
        to_next[0].start()
        to_next[1].start()

    @pl.when(has_mat)
    def _():
        mat.wait_recv()
        even_v[...] = rows_of(mat_in)
        for b in range(seqs):
            left = split(mat_in[b * block : b * block + states, :])
            even_node[b] = left
            v_left = mat_in[b * block + states : b * block + states + 1, :]
            y = wide(leading(left, v_left), deep(nodes[top + b]))[0]
            pair_node[b] = split(y[:states])
            comp_out[b * block : b * block + states, :] = y[:states]
            comp_out[b * block + states : (b + 1) * block, :] = y[states : states + EXTRA] + vecs[top + b : top + b + 1, :]
        pair_v[...] = rows_of(comp_out)

    @pl.when(gives_comp)
    def _():
        comp.start()

    @pl.when(pos == 3)
    def _():
        to_back.wait_recv()
        vec_out[...] = apply(lefts(vec_in[...]), pair_node, pair_v[...])

        @pl.when(pos < n - 1)
        def _():
            for copy in to_next:
                copy.start()

    for level in range(1, levels + 1):
        lag = powers[1 << (level - 1)]
        for j in range(total >> level):
            left, v_left = child(level, 2 * j)
            lead = leading(left, v_left)
            a, b = 2 * j, 2 * j + 1
            if level == 1:
                y = wide(lead, deep(theta_4[words[b]]))[0]
                whole = theta[words[a]] + y[:states]
                u = y[states : states + EXTRA] + u_4[b : b + 1, :] + u_rows[a : a + 1, :]
            else:
                a, b = first[level - 1] + a, first[level - 1] + b
                y = wide(lead, deep(psi_n[b]))[0]
                y = jnp.concatenate([y[:states], y[states:] + us[b : b + 1, :]], axis=0)
                y = mul(y, lag)
                whole = psi_f[a] + y[:states]
                u = y[states : states + EXTRA] + us[a : a + 1, :]
            k = first[level] + j
            if level == levels:
                psi_out[j * block : j * block + states, :] = whole
                psi_out[j * block + states : (j + 1) * block, :] = u
            else:
                us[k : k + 1, :] = u[0:1]
                if j % 2 == 0:
                    psi_f[k] = whole
                else:
                    psi_n[k] = split(whole)
        if level < levels:
            base = powers[1 << (level - 1)]
            for e in range(1, (1 << (level - 1)) + 1):
                made = mul_node(powers[e], base)
                powers[(1 << (level - 1)) + e] = made
    base = powers[chunks // 2]
    for e in range(1, chunks // 2 + 1):
        powers[chunks // 2 + e] = mul_node(powers[e], base)
    lap = powers[chunks]
    laps[0] = powers[0]
    laps[1] = lap
    for m in range(2, 2 * chips - 2):
        laps[m] = mul_node(laps[m // 2], laps[m - m // 2])

    @pl.when(gives_mat)
    def _():
        psi.start()

    @pl.when(pos == n - 1)
    def _():
        close = split(mul(d_t, lap))
        for b in range(seqs):
            y = wide(leading(nodes[top + b], vecs[top + b : top + b + 1, :]), deep(close))[0]
            psi_out[b * block : (b + 1) * block, :] += y[:block]

    for b in range(seqs):
        psi_own[b] = split(psi_out[b * block : b * block + states, :])
    psi_v[...] = rows_of(psi_out)

    @pl.when(has_mat)
    def _():
        parts = []
        for b in range(seqs):
            v_left = mat_in[b * block + states : b * block + states + 1, :]
            y = wide(leading(even_node[b], v_left), deep(psi_own[b]))[0]
            u = psi_out[b * block + states : b * block + states + 1, :]
            y = jnp.concatenate([y[:states], y[states:] + u], axis=0)
            parts.append(mul(y, lap)[:block])
        psi.wait_recv()
        for b in range(seqs):
            psi_in[b * block : (b + 1) * block, :] += parts[b]
            omega_node[b] = split(psi_in[b * block : b * block + states, :])
        omega_v[...] = rows_of(psi_in)

    def send_off(d, side):
        return pltpu.make_async_remote_copy(
            src_ref=off_out, dst_ref=off_in.at[d - 1], send_sem=off_send.at[2 * d - 2 + side], recv_sem=off_recv.at[d - 1],
            device_id={"tm": lax.rem(2 * (chip + chips - d) + side, n)}, device_id_type=MESH,
        )

    @pl.when(jnp.logical_or(pos == 2, pos >= 4))
    def _():
        to_back.wait_recv()

    @pl.when(has_comp)
    def _():
        comp.wait_recv()
        prev_v[...] = rows_of(comp_in)
        for b in range(seqs):
            prev_node[b] = split(comp_in[b * block : b * block + states, :])
        back = apply(lefts(vec_in[...]), prev_node, prev_v[...])
        vec_back[...] = back
        to_back.start()
        state[...] = back

    @pl.when(jnp.logical_not(has_comp))
    def _():
        state[...] = vec_in[...]

    @pl.when(jnp.logical_and(has_comp, pos < n - 1))
    def _():
        vec_out[...] = apply(lefts(state[...]), pair_node, pair_v[...])
        for copy in to_next:
            copy.start()

    @pl.when(has_mat)
    def _():
        left = lefts(state[...])
        off_out[...] = apply(left, omega_node, omega_v[...])
        for d in range(1, chips):
            @pl.when(chip - d >= 0)
            def _(d=d):
                send_off(d, 1).start()
                send_off(d, 0).start()
        state[...] = apply(left, even_node, even_v[...])

    @pl.when(odd)
    def _():
        near_out[...] = apply(lefts(state[...]), psi_own, psi_v[...])
        near.start()

    x = state[...]
    entering = []
    for b in range(seqs):
        entering.append(jnp.broadcast_to(x[b : b + 1], (8, states)))
    for level in range(levels, 0, -1):
        below = []
        for j in range(total >> level):
            node, v = child(level, 2 * j)
            below.append(entering[j])
            below.append(times(entering[j], tall(node)) + v)
        entering = below
    for j in range(total):
        ents[j : j + 1, :] = entering[j][0:1]

    x = ents[...]
    for i in range(WORD):
        prior[i * total : (i + 1) * total, :] = x
        x = advance(x, i)
        filt[i * total : (i + 1) * total, :] = x

    chunk8[...] = jnp.zeros_like(chunk8)
    for i in range(WORD):
        left = jnp.concatenate([twice(stacked(filt[j * total : (j + 1) * total, :])) for j in range(i, WORD)], axis=1)
        z = product(left, jnp.concatenate([tall(tails[j]) for j in range(WORD - i)], axis=0))
        suffix[i * total : (i + 1) * total, :] = z
        if i == 0:
            for b in range(seqs):
                chunk8[pl.ds(b, chunks, stride=8), :] = z[b * chunks : (b + 1) * chunks]
    ends = chunk8[...].reshape(chunks, 8, states)

    errors = jnp.concatenate([at(obs, i) for i in range(WORD)], axis=0) - mul(prior[...], split(readout))
    seen = jnp.concatenate([at(mask, i) for i in range(WORD)], axis=0)
    squares = jnp.sum(seen * active * errors * errors, axis=0, keepdims=True)
    number = jnp.sum(seen, axis=0, keepdims=True)
    sums = jnp.where(row8 == 0, jnp.broadcast_to(squares, (8, states)), jnp.broadcast_to(number, (8, states)))
    sum_buf[...] = sums

    def send_sum(d):
        return pltpu.make_async_remote_copy(
            src_ref=sum_buf, dst_ref=sum_in.at[d], send_sem=sum_send.at[d], recv_sem=sum_recv.at[d],
            device_id={"tm": lax.rem(pos + d + 1, n)}, device_id_type=MESH,
        )

    for d in range(n - 1):
        send_sum(d).start()

    last = jnp.zeros((8, states), F32)
    for b in range(seqs):
        r = (WORD - 1) * total + (b + 1) * chunks - 1
        last = jnp.where(row8 == b, jnp.broadcast_to(filt[r : r + 1, :], (8, states)), last)
    final = times(last, tall(d_t2))

    ups = [ends]
    for level in range(levels):
        pair = ups[-1].reshape(ups[-1].shape[0] // 2, 2, 8, states)
        half = pair.shape[0]
        later = times(pair[:, 1].reshape(half * 8, states), tall(powers[1 << level]))
        ups.append(pair[:, 0] + later.reshape(half, 8, states))
    x = jnp.zeros((1, 8, states), F32)
    for level in range(levels - 1, -1, -1):
        count = x.shape[0]
        pair = ups[level].reshape(count, 2, 8, states)
        if level == levels - 1:
            sooner = pair[:, 1]
        else:
            moved = times(x.reshape(count * 8, states), tall(powers[1 << level]))
            sooner = moved.reshape(count, 8, states) + pair[:, 1]
        x = jnp.stack([sooner, x], axis=1).reshape(2 * count, 8, states)
    chunk8[...] = x.reshape(chunks * 8, states)

    @pl.when(even)
    def _():
        near.wait_recv()

    for d in range(1, chips):
        @pl.when(chip + d < chips)
        def _(d=d):
            send_off(d, 0).wait_recv()

    left = jnp.concatenate([twice(stacked(off_in[d])) for d in range(chips - 1)], axis=1)
    rhs = jnp.concatenate([tall(laps[2 * d + 1 - par]) for d in range(chips - 1)], axis=0)
    x = jnp.where(pos == n - 1, final, near_in[...] + product(left, rhs))
    y = times(x, jnp.concatenate([tall(powers[chunks - 1 - k]) for k in range(chunks)], axis=1))
    for k in range(chunks):
        chunk8[k * 8 : (k + 1) * 8, :] += y[:, k * states : (k + 1) * states]
    x = jnp.concatenate([chunk8[pl.ds(b, chunks, stride=8), :] for b in range(seqs)], axis=0)
    y = times(x, jnp.concatenate([tall(a) for a in (d_4s, split(d_3), d_2s, d_2n)], axis=1))
    for i in range(WORD):
        out[pl.ds(i, total, stride=WORD), :] = (
            suffix[i * total : (i + 1) * total, :] + y[:, i * states : (i + 1) * states]
        )

    for d in range(n - 1):
        send_sum(d).wait_recv()
        sums = sums + sum_in[d]
    squares, number = sums[0:1], sums[1:2]
    grad = 0.5 * active * (number - weight * squares)
    new_prec[...] = log_prec[...] + grad / (seqs * steps * n)
    terms = 0.5 * active * (log_prec[...] * number - weight * squares)
    loglik[...] = jnp.zeros_like(terms) + jnp.sum(terms, axis=1, keepdims=True) / (seqs * steps * n * states)

    @pl.when(gives_mat)
    def _():
        mat.wait_send()
        psi.wait_send()

    @pl.when(gives_comp)
    def _():
        comp.wait_send()

    @pl.when(pos == 0)
    def _():
        to_next[0].wait_send()

    @pl.when(pos == 1)
    def _():
        to_next[0].wait_send()
        to_next[1].wait_send()

    @pl.when(last_of_four)
    def _():
        for copy in to_next:
            copy.wait_send()

    @pl.when(has_comp)
    def _():
        to_back.wait_send()

    @pl.when(odd)
    def _():
        near.wait_send()

    for d in range(1, chips):
        @pl.when(jnp.logical_and(has_mat, chip - d >= 0))
        def _(d=d):
            send_off(d, 0).wait_send()
            send_off(d, 1).wait_send()

    for d in range(n - 1):
        send_sum(d).wait_send()


def mul_node(left, right):
    return split(wide(left, deep(right))[0])


def finish(smoothed, new_prec, loglik, out, out_prec, out_loglik):
    out[...] = smoothed[...]
    out_prec[...] = new_prec[...]
    out_loglik[...] = loglik[:, 0:1]


def local(n, obs, present, sensors, log_prec, dynamics, prior_var, obs_map, init_state):
    seqs, steps, channels = obs.shape
    states = dynamics.shape[0]
    assert n % 4 == 0 and states == 128 and channels == 128
    chunks = steps // WORD
    total = seqs * chunks
    chips = n // 2
    inner = sum(total >> level for level in range(1, int(math.log2(chunks)) + 1))
    vmem = pl.BlockSpec(memory_space=pltpu.VMEM)
    smem = pl.BlockSpec(memory_space=pltpu.SMEM)
    rows = seqs * steps
    block = seqs * (states + EXTRA)
    node = (states, 2 * states)
    tile = pltpu.VMEM((8, states), F32)
    whole = pltpu.VMEM((block, states), F32)
    level_rows = (inner + 7) // 8 * 8
    dma = pltpu.SemaphoreType.DMA
    smoothed, new_prec, loglik = pl.pallas_call(
        functools.partial(kernel, n, seqs, steps),
        out_shape=(
            pltpu.VMEM((rows, states), F32),
            pltpu.VMEM((1, channels), F32),
            pltpu.VMEM((1, channels), F32),
        ),
        in_specs=[smem, smem] + [vmem] * 7,
        out_specs=(vmem, vmem, vmem),
        scratch_shapes=[
            pltpu.SMEM((total,), jnp.int32),
            pltpu.VMEM((2**WORD,) + node, BF16),
            pltpu.VMEM((2**WORD, states, states), F32),
            pltpu.VMEM((2**WORD,) + node, BF16),
            pltpu.VMEM((inner,) + node, BF16),
            pltpu.VMEM((level_rows, states), F32),
            pltpu.VMEM((inner, states, states), F32),
            pltpu.VMEM((inner,) + node, BF16),
            pltpu.VMEM((level_rows, states), F32),
            pltpu.VMEM((total, states), F32),
            pltpu.VMEM((total, states), F32),
            pltpu.VMEM((total, states), F32),
            pltpu.VMEM((total, states), F32),
            pltpu.VMEM((chunks + 1,) + node, BF16),
            pltpu.VMEM((2 * chips - 2,) + node, BF16),
            pltpu.VMEM((2 * states, 2 * states), BF16),
            pltpu.VMEM((rows, states), F32),
            pltpu.VMEM((rows, states), F32),
            pltpu.VMEM((rows, states), F32),
            pltpu.VMEM((rows, states), F32),
            pltpu.VMEM((rows, states), F32),
            pltpu.VMEM((chunks * 8, states), F32),
            pltpu.VMEM((seqs,) + node, BF16), tile,
            pltpu.VMEM((seqs,) + node, BF16), tile,
            pltpu.VMEM((seqs,) + node, BF16), tile,
            pltpu.VMEM((seqs,) + node, BF16), tile,
            pltpu.VMEM((seqs,) + node, BF16), tile,
            tile,
            tile, tile, tile, whole, whole, whole, whole, whole, whole,
            tile, pltpu.VMEM((chips - 1, 8, states), F32), tile, tile, tile, pltpu.VMEM((n, 8, states), F32),
            dma((4,)), dma(()), dma((2,)), dma((2,)), dma((2,)), dma((2,)),
            dma((2 * chips - 2,)), dma((chips - 1,)), dma((n,)), dma((n,)),
        ],
        compiler_params=pltpu.CompilerParams(collective_id=0, has_side_effects=True),
        name="kalman",
    )(
        present, sensors, obs.reshape(rows, channels), present, log_prec.reshape(1, channels),
        dynamics, prior_var.reshape(1, states), obs_map, init_state,
    )
    held = [pltpu.with_memory_space_constraint(a, pltpu.VMEM) for a in (smoothed, new_prec, loglik)]
    smoothed, new_prec, loglik = pl.pallas_call(
        finish,
        out_shape=(
            jax.ShapeDtypeStruct((rows, states), F32),
            jax.ShapeDtypeStruct((1, channels), F32),
            jax.ShapeDtypeStruct((1, 1), F32),
        ),
        in_specs=[vmem] * 3,
        out_specs=(vmem, vmem, vmem),
        name="finish",
    )(*held)
    return smoothed.reshape(seqs, steps, states), new_prec.reshape(channels), loglik.reshape(1)


def solution(mesh):
    in_specs = (
        P("cluster", "tm", None),
        P("cluster", "tm"),
        P("cluster"),
        P("cluster"),
        P("cluster", None),
        P("cluster"),
        P("cluster", None),
        P("cluster", None),
    )
    out_specs = (P("cluster", "tm", None), P("cluster"), P("cluster"))
    body = functools.partial(local, mesh.shape["tm"])
    return jax.shard_map(body, mesh=mesh, in_specs=in_specs, out_specs=out_specs, check_vma=False)
```

```python
import functools
import math

import jax
import jax.numpy as jnp
from jax import lax
from jax.experimental import pallas as pl
from jax.experimental.pallas import tpu as pltpu
from jax.sharding import PartitionSpec as P

F32 = jnp.float32
BF16 = jnp.bfloat16
MESH = pl.DeviceIdType.MESH
WORD = 4
EXTRA = 8


def split(a):
    high = a.astype(BF16).astype(F32)
    return jnp.concatenate([high, a - high], axis=1).astype(BF16)


def stacked(a):
    high = a.astype(BF16).astype(F32)
    return jnp.concatenate([high, a - high], axis=0).astype(BF16)


def deep(node):
    return jnp.concatenate([node, node], axis=0)


def tall(node):
    width = node.shape[1] // 2
    return jnp.concatenate([node[:, :width], node[:, width:]], axis=0)


def twice(s):
    return jnp.concatenate([s, s], axis=1)


def product(left, right):
    full = jnp.dot(left, right, preferred_element_type=F32)
    rows = full.shape[0] // 2
    return full[:rows] + full[rows:]


def times(a, right):
    return product(twice(stacked(a)), right)


def wide(left, right):
    full = jnp.dot(left, right, preferred_element_type=F32)
    half = left.shape[1] // 2 if left.shape[1] < 256 else 128
    return [
        full[:, 2 * k * half : (2 * k + 1) * half] + full[:, (2 * k + 1) * half : (2 * k + 2) * half]
        for k in range(full.shape[1] // (2 * half))
    ]


def mul(a, node):
    return wide(split(a), deep(node))[0]


def kernel(
    n, seqs, steps,
    present_s, sensors_s, obs, present_v, log_prec, dyn, prior_var, obs_map, init,
    out, new_prec, loglik,
    words, table, theta, theta_4, nodes, vecs, psi_f, psi_n, us, offs, u_rows, u_4, ents, powers, laps, step_rhs,
    drive, mask, prior, filt, suffix, chunk8, moves, held, pair_2, heads, head_vecs,
    even_node, even_v, pair_node, pair_v, prev_node, prev_v, omega_node, omega_v, psi_own, psi_v, state,
    vec_in, vec_out, vec_back, mat_out, mat_in, comp_out, comp_in, psi_out, psi_in,
    off_out, off_in, first_in, near_out, near_in, sum_buf, sum_in,
    vec_send, vec_recv, mat_sem, comp_sem, psi_sem, near_sem, off_send, off_recv, first_sem, sum_send, sum_recv,
):
    pos = lax.axis_index("tm")
    par = lax.rem(pos, 2)
    quarter = lax.rem(pos, 4)
    chip = lax.div(pos, 2)
    chips = n // 2
    states = dyn.shape[0]
    block = states + EXTRA
    chunks = steps // WORD
    total = seqs * chunks
    levels = int(math.log2(chunks))
    first = [0]
    for level in range(1, levels + 1):
        first.append(first[-1] + (total >> (level - 1) if level > 1 else 0))
    top = first[levels]

    vec_in[...] = jnp.zeros_like(vec_in)
    off_in[...] = jnp.zeros_like(off_in)
    near_in[...] = jnp.zeros_like(near_in)
    first_in[...] = jnp.zeros_like(first_in)
    barrier = pltpu.get_barrier_semaphore()
    for d in range(1, n):
        pl.semaphore_signal(barrier, inc=1, device_id={"tm": lax.rem(pos + d, n)}, device_id_type=MESH)

    lane = lax.broadcasted_iota(jnp.int32, (1, states), 1)
    row8 = lax.broadcasted_iota(jnp.int32, (8, states), 0)
    active = (lane < sensors_s[0]).astype(F32)
    weight = jnp.exp(log_prec[...])
    weight_on = weight * active
    pv = prior_var[...]
    d_mat = dyn[...]
    d_t = d_mat.T
    h_mat = obs_map[...]
    h_2 = split(h_mat)
    d_2n = split(d_mat)
    d_t2 = split(d_t)
    readout = wide(d_t2, deep(split(h_mat.T)))[0]
    gain = -(mul(readout * weight_on, h_2) * pv)
    f_t2 = split(d_t + gain)
    held[0] = d_2n
    held[4] = d_t2
    held[5] = split(gain)
    held[6] = split(readout)

    for b in range(seqs):
        for k in range(chunks):
            t = k * WORD
            w = present_s[b, t]
            for i in range(1, WORD):
                w = w * 2 + present_s[b, t + i]
            words[b * chunks + k] = w
        row = jnp.broadcast_to(present_v[b : b + 1, :].astype(F32), (steps, steps))
        same = lax.broadcasted_iota(jnp.int32, (steps, steps), 0) == lax.broadcasted_iota(jnp.int32, (steps, steps), 1)
        column = jnp.sum(jnp.where(same, row, 0.0), axis=1, keepdims=True)
        mask[b * steps : (b + 1) * steps, :] = jnp.broadcast_to(column, (steps, states))

    drive[...] = mul(obs[...] * weight_on, h_2) * pv * mask[...]

    step_rhs[...] = stacked(jnp.concatenate([d_t, gain], axis=1))
    singles = [d_t2, f_t2]
    both = deep(jnp.concatenate(singles, axis=1))
    pairs = []
    for a in range(2):
        pairs += [split(q) for q in wide(singles[a], both)]
    for a in range(4):
        pair_2[a] = pairs[a]
    held[7] = f_t2
    quad_rhs = deep(jnp.concatenate(pairs, axis=1))
    for a in range(4):
        quad = wide(pairs[a], quad_rhs)
        for c in range(4):
            table[a * 4 + c] = split(quad[c])

    def at(ref, i):
        return ref[pl.ds(i, total, stride=WORD), :]

    def advance(x, i):
        y = times(x, step_rhs[...])
        move = jnp.where(at(mask, i) > 0.5, y[:, states:], 0.0) + at(drive, i)
        return y[:, :states] + move, move

    x = at(drive, 0)
    moves[0:total, :] = x
    for i in range(1, WORD):
        x, move = advance(x, i)
        moves[i * total : (i + 1) * total, :] = move
    offs[...] = x

    def combine(moved, first):
        left = jnp.concatenate([twice(stacked(moved[j * total : (j + 1) * total, :])) for j in range(first + 1, WORD)], axis=1)
        return product(left, jnp.concatenate([tall(held[j]) for j in range(WORD - 1 - first)], axis=0))

    def leading(matrix, v):
        return jnp.concatenate([matrix, split(jnp.broadcast_to(v, (16, states)))], axis=0)

    def child(level, j):
        if level == 1:
            return table[words[j]], offs[j : j + 1, :]
        j = first[level - 1] + j
        return nodes[j], vecs[j : j + 1, :]

    for level in range(1, levels + 1):
        for j in range(total >> level):
            left, v_left = child(level, 2 * j)
            right, v_right = child(level, 2 * j + 1)
            y = wide(leading(left, v_left), deep(right))[0]
            j = first[level] + j
            v = y[states : states + EXTRA] + v_right
            nodes[j] = split(y[:states])
            vecs[j : j + 1, :] = v[0:1]
            if level == levels:
                b = j - top
                mat_out[b * block : b * block + states, :] = y[:states]
                mat_out[b * block + states : (b + 1) * block, :] = v

    def lefts(x):
        return jnp.concatenate([twice(stacked(jnp.where(row8 == b, x, 0.0))) for b in range(seqs)], axis=1)

    def apply(left, node, v):
        rhs = jnp.concatenate([tall(node[b]) for b in range(seqs)], axis=0)
        return product(left, rhs) + v

    def rows_of(ref):
        v = jnp.zeros((8, states), F32)
        for b in range(seqs):
            v = jnp.where(row8 == b, ref[b * block + states : (b + 1) * block, :], v)
        return v

    own = nodes.at[pl.ds(top, seqs)]

    def own_v():
        v = jnp.zeros((8, states), F32)
        for b in range(seqs):
            v = jnp.where(row8 == b, vecs[top + b : top + b + 1, :], v)
        return v

    def send_vec(src, slot, to):
        return pltpu.make_async_remote_copy(
            src_ref=src, dst_ref=vec_in, send_sem=vec_send.at[slot], recv_sem=vec_recv,
            device_id={"tm": to}, device_id_type=MESH,
        )

    def shift(by):
        return lax.rem(pos + (by + n), n)

    def send_mat(src, dst, sem, by):
        return pltpu.make_async_remote_copy(
            src_ref=src, dst_ref=dst, send_sem=sem.at[0], recv_sem=sem.at[1],
            device_id={"tm": shift(by)}, device_id_type=MESH,
        )

    mat = send_mat(mat_out, mat_in, mat_sem, 1)
    comp = send_mat(comp_out, comp_in, comp_sem, 2)
    psi = send_mat(psi_out, psi_in, psi_sem, 1)
    near = send_mat(near_out, near_in, near_sem, -1)
    to_next = [send_vec(vec_out, k, shift(by)) for k, by in enumerate((2, 4, 1))]
    to_back = send_vec(vec_back, 3, shift(-1))

    even = par == 0
    odd = par == 1
    has_mat = jnp.logical_and(odd, pos >= 2)
    gives_mat = jnp.logical_and(even, pos >= 2)
    gives_comp = jnp.logical_and(quarter == 1, pos >= 4)
    has_comp = jnp.logical_and(quarter == 3, pos >= 4)
    last_of_four = jnp.logical_and(quarter == 3, pos < n - 1)

    pl.semaphore_wait(barrier, n - 1)

    @pl.when(gives_mat)
    def _():
        mat.start()

    @pl.when(pos == 0)
    def _():
        vec_in[0:seqs, :] = init[...]
        vec_out[...] = apply(lefts(vec_in[...]), own, own_v())
        to_next[2].start()

    near_4 = pos < 4
    far = pos >= 4

    base = held[0]
    held[1] = mul_node(base, base)
    square = held[1]
    held[2] = mul_node(base, square)
    held[3] = mul_node(square, square)
    powers[1] = held[3]

    @pl.when(pos == 1)
    def _():
        to_back.wait_recv()
        vec_out[...] = apply(lefts(vec_in[...]), own, own_v())
        to_next[0].start()
        to_next[2].start()

    @pl.when(far)
    def _():
        fourth = held[3]
        u = moves[0:total, :] + combine(moves, 0)
        u_rows[...] = u
        u_4[...] = times(u, tall(fourth))
        gain = held[5]
        whole = gain[:, :states].astype(F32) + gain[:, states:].astype(F32)
        rhs = deep(mul_node(gain, held[0]))
        theta_2 = [None, wide(held[4], rhs)[0], whole, whole + wide(held[7], rhs)[0]]
        rhs = deep(held[1])
        rhs = deep(jnp.concatenate([split(wide(split(a), rhs)[0]) for a in theta_2[1:]], axis=1))
        theta[0] = jnp.zeros_like(whole)
        theta_4[0] = split(jnp.zeros_like(whole))
        for a in range(4):
            full = [None] + wide(pair_2[a], rhs)
            for c in range(4):
                if a + c > 0:
                    parts = [q for q in (theta_2[a], full[c]) if q is not None]
                    whole = sum(parts[1:], parts[0])
                    theta[a * 4 + c] = whole
                    theta_4[a * 4 + c] = split(mul(whole, fourth))

    @pl.when(has_mat)
    def _():
        mat.wait_recv()
        even_v[...] = rows_of(mat_in)
        for b in range(seqs):
            left = split(mat_in[b * block : b * block + states, :])
            even_node[b] = left
            v_left = mat_in[b * block + states : b * block + states + 1, :]
            y = wide(leading(left, v_left), deep(nodes[top + b]))[0]
            pair_node[b] = split(y[:states])
            comp_out[b * block : b * block + states, :] = y[:states]
            comp_out[b * block + states : (b + 1) * block, :] = y[states : states + EXTRA] + vecs[top + b : top + b + 1, :]
        pair_v[...] = rows_of(comp_out)

    @pl.when(gives_comp)
    def _():
        comp.start()

    def double(level):
        half = 1 << (level - 1)
        powers[2 * half] = mul_node(powers[half], powers[half])

    def fill():
        powers[0] = split(
            (
                lax.broadcasted_iota(jnp.int32, (states, states), 0)
                == lax.broadcasted_iota(jnp.int32, (states, states), 1)
            ).astype(F32)
        )
        for level in range(1, levels):
            base = powers[1 << level]
            for e in range(1, 1 << level):
                powers[(1 << level) + e] = mul_node(powers[e], base)
        laps[0] = powers[0]
        laps[1] = powers[chunks]
        for m in range(2, 2 * chips - 2):
            laps[m] = mul_node(laps[m // 2], laps[m - m // 2])

    @pl.when(pos == 3)
    def _():
        to_back.wait_recv()
        vec_out[...] = apply(lefts(vec_in[...]), pair_node, pair_v[...])

        @pl.when(pos < n - 1)
        def _():
            for copy in to_next:
                copy.start()

    @pl.when(near_4)
    def _():
        for level in range(1, levels + 1):
            double(level)
        fill()

    def prepare():
        for b in range(seqs):
            for level in range(levels, 0, -1):
                for p in range(chunks >> level):
                    mat_2, v = child(level, (b * (chunks >> level) + p) * 2)
                    k = (p << level) + (1 << (level - 1))
                    if p > 0:
                        before = b * chunks + (p << level)
                        lead = leading(heads[before], head_vecs[before : before + 1, :])
                        y = wide(lead, deep(mat_2))[0]
                        mat_2 = split(y[:states])
                        v = y[states : states + 1] + v
                    heads[b * chunks + k] = mat_2
                    head_vecs[b * chunks + k : b * chunks + k + 1, :] = v

    @pl.when(far)
    def _():
        for level in range(1, levels + 1):
            lag = powers[1 << (level - 1)]
            double(level)
            for j in range(total >> level):
                left, v_left = child(level, 2 * j)
                lead = leading(left, v_left)
                a, b = 2 * j, 2 * j + 1
                if level == 1:
                    y = wide(lead, deep(theta_4[words[b]]))[0]
                    whole = theta[words[a]] + y[:states]
                    u = y[states : states + EXTRA] + u_4[b : b + 1, :] + u_rows[a : a + 1, :]
                else:
                    a, b = first[level - 1] + a, first[level - 1] + b
                    y = wide(lead, deep(psi_n[b]))[0]
                    y = jnp.concatenate([y[:states], y[states:] + us[b : b + 1, :]], axis=0)
                    y = mul(y, lag)
                    whole = psi_f[a] + y[:states]
                    u = y[states : states + EXTRA] + us[a : a + 1, :]
                k = first[level] + j
                if level == levels:
                    psi_out[j * block : j * block + states, :] = whole
                    psi_out[j * block + states : (j + 1) * block, :] = u
                else:
                    us[k : k + 1, :] = u[0:1]
                    if j % 2 == 0:
                        psi_f[k] = whole
                    else:
                        psi_n[k] = split(whole)

    @pl.when(jnp.logical_and(gives_mat, far))
    def _():
        psi.start()

    @pl.when(far)
    def _():
        for b in range(seqs):
            psi_own[b] = split(psi_out[b * block : b * block + states, :])
        psi_v[...] = rows_of(psi_out)
        fill()

    @pl.when(jnp.logical_and(odd, far))
    def _():
        parts = []
        lap = powers[chunks]
        for b in range(seqs):
            v_left = mat_in[b * block + states : b * block + states + 1, :]
            y = wide(leading(even_node[b], v_left), deep(psi_own[b]))[0]
            u = psi_out[b * block + states : b * block + states + 1, :]
            y = jnp.concatenate([y[:states], y[states:] + u], axis=0)
            parts.append(mul(y, lap)[:block])
        psi.wait_recv()
        for b in range(seqs):
            psi_in[b * block : (b + 1) * block, :] += parts[b]
            omega_node[b] = split(psi_in[b * block : b * block + states, :])
        omega_v[...] = rows_of(psi_in)

    direct = jnp.logical_and(odd, far)

    headed = jnp.logical_and(even, far)

    @pl.when(headed)
    def _():
        prepare()

    def send_off(d, side):
        return pltpu.make_async_remote_copy(
            src_ref=off_out, dst_ref=off_in.at[d - 1], send_sem=off_send.at[2 * d - 2 + side], recv_sem=off_recv.at[d - 1],
            device_id={"tm": lax.rem(2 * (chip + chips - d) + side, n)}, device_id_type=MESH,
        )

    @pl.when(jnp.logical_or(pos == 2, pos >= 4))
    def _():
        to_back.wait_recv()

    @pl.when(has_comp)
    def _():
        comp.wait_recv()
        prev_v[...] = rows_of(comp_in)
        for b in range(seqs):
            prev_node[b] = split(comp_in[b * block : b * block + states, :])
        back = apply(lefts(vec_in[...]), prev_node, prev_v[...])
        vec_back[...] = back
        to_back.start()
        state[...] = back

    @pl.when(jnp.logical_not(has_comp))
    def _():
        state[...] = vec_in[...]

    @pl.when(jnp.logical_and(has_comp, pos < n - 1))
    def _():
        vec_out[...] = apply(lefts(state[...]), pair_node, pair_v[...])
        for copy in to_next:
            copy.start()

    @pl.when(jnp.logical_and(odd, far))
    def _():
        left = lefts(state[...])
        off_out[...] = apply(left, omega_node, omega_v[...])
        for d in range(chips - 1, 0, -1):
            @pl.when(chip - d >= 0)
            def _(d=d):
                send_off(d, 1).start()
                send_off(d, 0).start()
        x = apply(left, even_node, even_v[...])
        state[...] = x
        near_out[...] = apply(lefts(x), psi_own, psi_v[...])
        near.start()

    @pl.when(pos == 3)
    def _():
        state[...] = apply(lefts(state[...]), even_node, even_v[...])

    @pl.when(headed)
    def _():
        x = state[...]
        spread = jnp.concatenate([jnp.concatenate([tall(heads[b * chunks + k]) for k in range(1, chunks)], axis=1) for b in range(seqs)], axis=0)
        y = product(lefts(x), spread)
        for b in range(seqs):
            ents[b * chunks : b * chunks + 1, :] = x[b : b + 1]
            for k in range(1, chunks):
                r = b * chunks + k
                ents[r : r + 1, :] = y[b : b + 1, (k - 1) * states : k * states] + head_vecs[r : r + 1, :]

    @pl.when(jnp.logical_not(headed))
    def _():
        x = state[...]
        entering = [jnp.broadcast_to(x[b : b + 1], (8, states)) for b in range(seqs)]
        for level in range(levels, 0, -1):
            below = []
            for j in range(total >> level):
                node, v = child(level, 2 * j)
                below.append(entering[j])
                below.append(times(entering[j], tall(node)) + v)
            entering = below
        for j in range(total):
            ents[j : j + 1, :] = entering[j][0:1]

    x = ents[...]
    for i in range(WORD):
        prior[i * total : (i + 1) * total, :] = x
        x, move = advance(x, i)
        filt[i * total : (i + 1) * total, :] = x
        moves[i * total : (i + 1) * total, :] = move

    def send_sum(d):
        return pltpu.make_async_remote_copy(
            src_ref=sum_buf, dst_ref=sum_in.at[d], send_sem=sum_send.at[d], recv_sem=sum_recv.at[d],
            device_id={"tm": lax.rem(pos + d + 1, n)}, device_id_type=MESH,
        )

    def score():
        errors = jnp.concatenate([at(obs, i) for i in range(WORD)], axis=0) - mul(prior[...], held[6])
        seen = jnp.concatenate([at(mask, i) for i in range(WORD)], axis=0)
        squares = jnp.sum(seen * active * errors * errors, axis=0, keepdims=True)
        number = jnp.sum(seen, axis=0, keepdims=True)
        sums = jnp.where(row8 == 0, jnp.broadcast_to(squares, (8, states)), jnp.broadcast_to(number, (8, states)))
        sum_buf[...] = sums
        for e in range(1, n):
            d = e - 1
            @pl.when(pos + e >= n)
            def _(d=d):
                send_sum(d).start()

        for e in range(n - 1, 0, -1):
            d = e - 1
            @pl.when(pos + e < n)
            def _(d=d):
                send_sum(d).start()

    @pl.when(far)
    def _():
        score()

    chunk8[...] = jnp.zeros_like(chunk8)
    for i in range(WORD - 1):
        z = combine(moves, i)
        suffix[i * total : (i + 1) * total, :] = filt[i * total : (i + 1) * total, :] + z
        if i == 0:
            z = z + moves[0:total, :]
            for b in range(seqs):
                chunk8[pl.ds(b, chunks, stride=8), :] = z[b * chunks : (b + 1) * chunks]
    i = WORD - 1
    suffix[i * total : (i + 1) * total, :] = filt[i * total : (i + 1) * total, :]
    ends = chunk8[...].reshape(chunks, 8, states)

    ups = [ends]
    for level in range(levels):
        pair = ups[-1].reshape(ups[-1].shape[0] // 2, 2, 8, states)
        half = pair.shape[0]
        later = times(pair[:, 1].reshape(half * 8, states), tall(powers[1 << level]))
        ups.append(pair[:, 0] + later.reshape(half, 8, states))

    def send_first(slot, side):
        dst = off_in.at[0] if slot == 0 else first_in
        return pltpu.make_async_remote_copy(
            src_ref=off_out, dst_ref=dst, send_sem=off_send.at[side],
            recv_sem=off_recv.at[0] if slot == 0 else first_sem,
            device_id={"tm": side}, device_id_type=MESH,
        )

    @pl.when(near_4)
    def _():
        off_out[...] = ups[-1].reshape(8, states)
        near_out[...] = ups[-1].reshape(8, states)
        for slot in range(2):
            @pl.when(pos == 2 + slot)
            def _(slot=slot):
                send_first(slot, 0).start()
                send_first(slot, 1).start()

        @pl.when(odd)
        def _():
            near.start()

        score()

    x = jnp.zeros((1, 8, states), F32)
    for level in range(levels - 1, -1, -1):
        count = x.shape[0]
        pair = ups[level].reshape(count, 2, 8, states)
        if level == levels - 1:
            sooner = pair[:, 1]
        else:
            moved = times(x.reshape(count * 8, states), tall(powers[1 << level]))
            sooner = moved.reshape(count, 8, states) + pair[:, 1]
        x = jnp.stack([sooner, x], axis=1).reshape(2 * count, 8, states)
    chunk8[...] = x.reshape(chunks * 8, states)

    @pl.when(even)
    def _():
        near.wait_recv()

    @pl.when(chip == 0)
    def _():
        send_first(1, 0).wait_recv()

    for d in range(1, chips):
        @pl.when(chip + d < chips)
        def _(d=d):
            send_off(d, 0).wait_recv()

    left = jnp.concatenate([twice(stacked(a)) for a in [first_in[...]] + [off_in[d] for d in range(chips - 1)]], axis=1)
    rhs = jnp.concatenate([tall(laps[2 - par])] + [tall(laps[2 * d + 1 - par]) for d in range(chips - 1)], axis=0)
    x = near_in[...] + product(left, rhs)
    y = times(x, jnp.concatenate([tall(powers[chunks - 1 - k]) for k in range(chunks)], axis=1))
    for k in range(chunks):
        chunk8[k * 8 : (k + 1) * 8, :] += y[:, k * states : (k + 1) * states]
    x = jnp.concatenate([chunk8[pl.ds(b, chunks, stride=8), :] for b in range(seqs)], axis=0)
    y = times(x, jnp.concatenate([tall(a) for a in (held[3], held[2], held[1], held[0])], axis=1))
    for i in range(WORD):
        out[pl.ds(i, total, stride=WORD), :] = (
            suffix[i * total : (i + 1) * total, :] + y[:, i * states : (i + 1) * states]
        )

    sums = sum_buf[...]
    for d in range(n - 1):
        send_sum(d).wait_recv()
        sums = sums + sum_in[d]
    squares, number = sums[0:1], sums[1:2]
    grad = 0.5 * active * (number - weight * squares)
    new_prec[...] = log_prec[...] + grad / (seqs * steps * n)
    terms = 0.5 * active * (log_prec[...] * number - weight * squares)
    loglik[...] = jnp.zeros_like(terms) + jnp.sum(terms, axis=1, keepdims=True) / (seqs * steps * n * states)

    @pl.when(gives_mat)
    def _():
        mat.wait_send()

    @pl.when(jnp.logical_and(gives_mat, far))
    def _():
        psi.wait_send()

    @pl.when(gives_comp)
    def _():
        comp.wait_send()

    @pl.when(pos == 0)
    def _():
        to_next[2].wait_send()

    @pl.when(pos == 1)
    def _():
        to_next[0].wait_send()
        to_next[2].wait_send()

    @pl.when(last_of_four)
    def _():
        for copy in to_next:
            copy.wait_send()

    @pl.when(has_comp)
    def _():
        to_back.wait_send()

    @pl.when(odd)
    def _():
        near.wait_send()

    for d in range(1, chips):
        @pl.when(jnp.logical_and(jnp.logical_and(odd, far), chip - d >= 0))
        def _(d=d):
            send_off(d, 0).wait_send()
            send_off(d, 1).wait_send()

    for slot in range(2):
        @pl.when(pos == 2 + slot)
        def _(slot=slot):
            send_first(slot, 0).wait_send()
            send_first(slot, 1).wait_send()

    for d in range(n - 1):
        send_sum(d).wait_send()


def mul_node(left, right):
    return split(wide(left, deep(right))[0])


def finish(smoothed, new_prec, loglik, out, out_prec, out_loglik):
    out[...] = smoothed[...]
    out_prec[...] = new_prec[...]
    out_loglik[...] = loglik[:, 0:1]


def local(n, obs, present, sensors, log_prec, dynamics, prior_var, obs_map, init_state):
    seqs, steps, channels = obs.shape
    states = dynamics.shape[0]
    assert n % 4 == 0 and states == 128 and channels == 128
    chunks = steps // WORD
    total = seqs * chunks
    chips = n // 2
    inner = sum(total >> level for level in range(1, int(math.log2(chunks)) + 1))
    vmem = pl.BlockSpec(memory_space=pltpu.VMEM)
    smem = pl.BlockSpec(memory_space=pltpu.SMEM)
    rows = seqs * steps
    block = seqs * (states + EXTRA)
    node = (states, 2 * states)
    tile = pltpu.VMEM((8, states), F32)
    whole = pltpu.VMEM((block, states), F32)
    level_rows = (inner + 7) // 8 * 8
    dma = pltpu.SemaphoreType.DMA
    smoothed, new_prec, loglik = pl.pallas_call(
        functools.partial(kernel, n, seqs, steps),
        out_shape=(
            pltpu.VMEM((rows, states), F32),
            pltpu.VMEM((1, channels), F32),
            pltpu.VMEM((1, channels), F32),
        ),
        in_specs=[smem, smem] + [vmem] * 7,
        out_specs=(vmem, vmem, vmem),
        scratch_shapes=[
            pltpu.SMEM((total,), jnp.int32),
            pltpu.VMEM((2**WORD,) + node, BF16),
            pltpu.VMEM((2**WORD, states, states), F32),
            pltpu.VMEM((2**WORD,) + node, BF16),
            pltpu.VMEM((inner,) + node, BF16),
            pltpu.VMEM((level_rows, states), F32),
            pltpu.VMEM((inner, states, states), F32),
            pltpu.VMEM((inner,) + node, BF16),
            pltpu.VMEM((level_rows, states), F32),
            pltpu.VMEM((total, states), F32),
            pltpu.VMEM((total, states), F32),
            pltpu.VMEM((total, states), F32),
            pltpu.VMEM((total, states), F32),
            pltpu.VMEM((chunks + 1,) + node, BF16),
            pltpu.VMEM((2 * chips - 2,) + node, BF16),
            pltpu.VMEM((2 * states, 2 * states), BF16),
            pltpu.VMEM((rows, states), F32),
            pltpu.VMEM((rows, states), F32),
            pltpu.VMEM((rows, states), F32),
            pltpu.VMEM((rows, states), F32),
            pltpu.VMEM((rows, states), F32),
            pltpu.VMEM((chunks * 8, states), F32),
            pltpu.VMEM((rows, states), F32),
            pltpu.VMEM((8,) + node, BF16),
            pltpu.VMEM((4,) + node, BF16),
            pltpu.VMEM((total,) + node, BF16),
            pltpu.VMEM((total, states), F32),
            pltpu.VMEM((seqs,) + node, BF16), tile,
            pltpu.VMEM((seqs,) + node, BF16), tile,
            pltpu.VMEM((seqs,) + node, BF16), tile,
            pltpu.VMEM((seqs,) + node, BF16), tile,
            pltpu.VMEM((seqs,) + node, BF16), tile,
            tile,
            tile, tile, tile, whole, whole, whole, whole, whole, whole,
            tile, pltpu.VMEM((chips - 1, 8, states), F32), tile, tile, tile, tile, pltpu.VMEM((n, 8, states), F32),
            dma((4,)), dma(()), dma((2,)), dma((2,)), dma((2,)), dma((2,)),
            dma((2 * chips - 2,)), dma((chips - 1,)), dma(()), dma((n,)), dma((n,)),
        ],
        compiler_params=pltpu.CompilerParams(collective_id=0, has_side_effects=True),
        name="kalman",
    )(
        present, sensors, obs.reshape(rows, channels), present, log_prec.reshape(1, channels),
        dynamics, prior_var.reshape(1, states), obs_map, init_state,
    )
    held = [pltpu.with_memory_space_constraint(a, pltpu.VMEM) for a in (smoothed, new_prec, loglik)]
    smoothed, new_prec, loglik = pl.pallas_call(
        finish,
        out_shape=(
            jax.ShapeDtypeStruct((rows, states), F32),
            jax.ShapeDtypeStruct((1, channels), F32),
            jax.ShapeDtypeStruct((1, 1), F32),
        ),
        in_specs=[vmem] * 3,
        out_specs=(vmem, vmem, vmem),
        name="finish",
    )(*held)
    return smoothed.reshape(seqs, steps, states), new_prec.reshape(channels), loglik.reshape(1)


def solution(mesh):
    in_specs = (
        P("cluster", "tm", None),
        P("cluster", "tm"),
        P("cluster"),
        P("cluster"),
        P("cluster", None),
        P("cluster"),
        P("cluster", None),
        P("cluster", None),
    )
    out_specs = (P("cluster", "tm", None), P("cluster"), P("cluster"))
    body = functools.partial(local, mesh.shape["tm"])
    return jax.shard_map(body, mesh=mesh, in_specs=in_specs, out_specs=out_specs, check_vma=False)
```

```python
import functools
import math

import jax
import jax.numpy as jnp
from jax import lax
from jax.experimental import pallas as pl
from jax.experimental.pallas import tpu as pltpu
from jax.sharding import PartitionSpec as P

F32 = jnp.float32
BF16 = jnp.bfloat16
MESH = pl.DeviceIdType.MESH
WORD = 4
EXTRA = 8


def split(a):
    high = a.astype(BF16).astype(F32)
    return jnp.concatenate([high, a - high], axis=1).astype(BF16)


def stacked(a):
    high = a.astype(BF16).astype(F32)
    return jnp.concatenate([high, a - high], axis=0).astype(BF16)


def deep(node):
    return jnp.concatenate([node, node], axis=0)


def tall(node):
    width = node.shape[1] // 2
    return jnp.concatenate([node[:, :width], node[:, width:]], axis=0)


def twice(s):
    return jnp.concatenate([s, s], axis=1)


def product(left, right):
    full = jnp.dot(left, right, preferred_element_type=F32)
    rows = full.shape[0] // 2
    return full[:rows] + full[rows:]


def times(a, right):
    return product(twice(stacked(a)), right)


def wide(left, right):
    full = jnp.dot(left, right, preferred_element_type=F32)
    half = left.shape[1] // 2 if left.shape[1] < 256 else 128
    return [
        full[:, 2 * k * half : (2 * k + 1) * half] + full[:, (2 * k + 1) * half : (2 * k + 2) * half]
        for k in range(full.shape[1] // (2 * half))
    ]


def mul(a, node):
    return wide(split(a), deep(node))[0]


def kernel(
    n, seqs, steps,
    present_s, sensors_s, obs, present_v, log_prec, dyn, prior_var, obs_map, init,
    out, new_prec, loglik,
    words, table, theta, theta_4, nodes, vecs, psi_f, psi_n, us, offs, u_rows, u_4, ents, powers, laps, step_rhs,
    drive, mask, prior, filt, suffix, chunk8, moves, held, pair_2, zero_2, theta_2, theta_d, later, heads, head_vecs,
    even_node, even_v, pair_node, pair_v, prev_node, prev_v, omega_node, omega_v, psi_own, psi_v, state,
    vec_in, vec_out, vec_back, mat_out, mat_in, comp_out, comp_in, psi_out, psi_in,
    off_out, off_in, first_in, near_out, near_in, sum_buf, sum_in,
    vec_send, vec_recv, mat_sem, comp_sem, psi_sem, near_sem, off_send, off_recv, first_sem, sum_sem,
):
    pos = lax.axis_index("tm")
    par = lax.rem(pos, 2)
    quarter = lax.rem(pos, 4)
    chip = lax.div(pos, 2)
    chips = n // 2
    states = dyn.shape[0]
    block = states + EXTRA
    chunks = steps // WORD
    total = seqs * chunks
    levels = int(math.log2(chunks))
    first = [0]
    for level in range(1, levels + 1):
        first.append(first[-1] + (total >> (level - 1) if level > 1 else 0))
    top = first[levels]

    vec_in[...] = jnp.zeros_like(vec_in)
    off_in[...] = jnp.zeros_like(off_in)
    near_in[...] = jnp.zeros_like(near_in)
    first_in[...] = jnp.zeros_like(first_in)
    barrier = pltpu.get_barrier_semaphore()
    for d in range(1, n):
        pl.semaphore_signal(barrier, inc=1, device_id={"tm": lax.rem(pos + d, n)}, device_id_type=MESH)

    lane = lax.broadcasted_iota(jnp.int32, (1, states), 1)
    row8 = lax.broadcasted_iota(jnp.int32, (8, states), 0)
    active = (lane < sensors_s[0]).astype(F32)
    weight = jnp.exp(log_prec[...])
    weight_on = weight * active
    pv = prior_var[...]
    d_mat = dyn[...]
    d_t = d_mat.T
    h_mat = obs_map[...]
    h_2 = split(h_mat)
    d_2n = split(d_mat)
    d_t2 = split(d_t)
    readout = wide(d_t2, deep(split(h_mat.T)))[0]
    gain = -(mul(readout * weight_on, h_2) * pv)
    f_t2 = split(d_t + gain)
    held[0] = d_2n
    held[4] = d_t2
    held[5] = split(gain)
    held[6] = split(readout)

    for b in range(seqs):
        for k in range(chunks):
            t = k * WORD
            w = present_s[b, t]
            for i in range(1, WORD):
                w = w * 2 + present_s[b, t + i]
            words[b * chunks + k] = w
        row = jnp.broadcast_to(present_v[b : b + 1, :].astype(F32), (steps, steps))
        same = lax.broadcasted_iota(jnp.int32, (steps, steps), 0) == lax.broadcasted_iota(jnp.int32, (steps, steps), 1)
        column = jnp.sum(jnp.where(same, row, 0.0), axis=1, keepdims=True)
        mask[b * steps : (b + 1) * steps, :] = jnp.broadcast_to(column, (steps, states))

    drive[...] = mul(obs[...] * weight_on, h_2) * pv * mask[...]

    step_rhs[...] = stacked(jnp.concatenate([d_t, gain], axis=1))
    singles = [d_t2, f_t2]
    both = deep(jnp.concatenate(singles, axis=1))
    pairs = []
    for a in range(2):
        pairs += [split(q) for q in wide(singles[a], both)]
    for a in range(4):
        pair_2[a] = pairs[a]
    held[7] = f_t2
    quad_rhs = deep(jnp.concatenate(pairs, axis=1))
    for a in range(4):
        quad = wide(pairs[a], quad_rhs)
        for c in range(4):
            table[a * 4 + c] = split(quad[c])

    def at(ref, i):
        return ref[pl.ds(i, total, stride=WORD), :]

    def advance(x, i):
        y = times(x, step_rhs[...])
        move = jnp.where(at(mask, i) > 0.5, y[:, states:], 0.0) + at(drive, i)
        return y[:, :states] + move, move

    x = at(drive, 0)
    moves[0:total, :] = x
    for i in range(1, WORD):
        x, move = advance(x, i)
        moves[i * total : (i + 1) * total, :] = move
        if i == 1:
            zero_2[...] = x
    offs[...] = x

    def combine(moved, first):
        left = jnp.concatenate([twice(stacked(moved[j * total : (j + 1) * total, :])) for j in range(first + 1, WORD)], axis=1)
        return product(left, jnp.concatenate([tall(held[j]) for j in range(WORD - 1 - first)], axis=0))

    def leading(matrix, v):
        return jnp.concatenate([matrix, split(jnp.broadcast_to(v, (16, states)))], axis=0)

    def child(level, j):
        if level == 1:
            return table[words[j]], offs[j : j + 1, :]
        j = first[level - 1] + j
        return nodes[j], vecs[j : j + 1, :]

    for level in range(1, levels + 1):
        for j in range(total >> level):
            left, v_left = child(level, 2 * j)
            right, v_right = child(level, 2 * j + 1)
            y = wide(leading(left, v_left), deep(right))[0]
            j = first[level] + j
            v = y[states : states + EXTRA] + v_right
            nodes[j] = split(y[:states])
            vecs[j : j + 1, :] = v[0:1]
            if level == levels:
                b = j - top
                mat_out[b * block : b * block + states, :] = y[:states]
                mat_out[b * block + states : (b + 1) * block, :] = v

    def lefts(x):
        return jnp.concatenate([twice(stacked(jnp.where(row8 == b, x, 0.0))) for b in range(seqs)], axis=1)

    def apply(left, node, v):
        rhs = jnp.concatenate([tall(node[b]) for b in range(seqs)], axis=0)
        return product(left, rhs) + v

    def rows_of(ref):
        v = jnp.zeros((8, states), F32)
        for b in range(seqs):
            v = jnp.where(row8 == b, ref[b * block + states : (b + 1) * block, :], v)
        return v

    own = nodes.at[pl.ds(top, seqs)]

    def own_v():
        v = jnp.zeros((8, states), F32)
        for b in range(seqs):
            v = jnp.where(row8 == b, vecs[top + b : top + b + 1, :], v)
        return v

    def send_vec(src, slot, to):
        return pltpu.make_async_remote_copy(
            src_ref=src, dst_ref=vec_in, send_sem=vec_send.at[slot // 3], recv_sem=vec_recv,
            device_id={"tm": to}, device_id_type=MESH,
        )

    def shift(by):
        return lax.rem(pos + (by + n), n)

    def send_mat(src, dst, sem, by):
        return pltpu.make_async_remote_copy(
            src_ref=src, dst_ref=dst, send_sem=sem.at[0], recv_sem=sem.at[1],
            device_id={"tm": shift(by)}, device_id_type=MESH,
        )

    def arrived(ref, sem):
        pltpu.make_async_copy(ref, ref, sem).wait()

    def send_part(src, dst, sem, by, b):
        rows = pl.ds(b * block, block)
        return pltpu.make_async_remote_copy(
            src_ref=src.at[rows], dst_ref=dst.at[rows], send_sem=sem.at[0], recv_sem=sem.at[1 + (b if by == 1 else 0)],
            device_id={"tm": shift(by)}, device_id_type=MESH,
        )

    mats = [send_part(mat_out, mat_in, mat_sem, 1, b) for b in range(seqs)]
    comps = [send_part(comp_out, comp_in, comp_sem, 2, b) for b in range(seqs)]
    psi = send_mat(psi_out, psi_in, psi_sem, 1)
    near = send_mat(near_out, near_in, near_sem, -1)
    to_next = [send_vec(vec_out, k, shift(by)) for k, by in enumerate((2, 4, 1))]
    to_back = send_vec(vec_back, 3, shift(-1))

    even = par == 0
    odd = par == 1
    has_mat = jnp.logical_and(odd, pos >= 2)
    gives_mat = jnp.logical_and(even, pos >= 2)
    gives_comp = jnp.logical_and(quarter == 1, pos >= 4)
    has_comp = jnp.logical_and(quarter == 3, pos >= 4)
    last_of_four = jnp.logical_and(quarter == 3, pos < n - 1)

    pl.semaphore_wait(barrier, n - 1)

    @pl.when(gives_mat)
    def _():
        for copy in mats:
            copy.start()

    @pl.when(pos == 0)
    def _():
        vec_in[0:seqs, :] = init[...]
        vec_out[...] = apply(lefts(vec_in[...]), own, own_v())
        to_next[2].start()

    near_4 = pos < 4
    far = pos >= 4

    base = held[0]
    held[1] = mul_node(base, base)
    square = held[1]
    held[2] = mul_node(base, square)
    held[3] = mul_node(square, square)
    powers[1] = held[3]
    rhs = deep(mul_node(held[5], base))
    change = held[5]
    change = change[:, :states].astype(F32) + change[:, states:].astype(F32)
    parts = [wide(held[4], rhs)[0], change, change + wide(held[7], rhs)[0]]
    for a in range(3):
        theta_2[a] = parts[a]
        theta_d[:, 2 * a * states : 2 * (a + 1) * states] = split(mul(parts[a], square))

    @pl.when(pos == 1)
    def _():
        to_back.wait_recv()
        vec_out[...] = apply(lefts(vec_in[...]), own, own_v())
        to_next[0].start()
        to_next[2].start()

    def pair(b):
        left = split(mat_in[b * block : b * block + states, :])
        even_node[b] = left
        v_left = mat_in[b * block + states : b * block + states + 1, :]
        y = wide(leading(left, v_left), deep(nodes[top + b]))[0]
        pair_node[b] = split(y[:states])
        comp_out[b * block : b * block + states, :] = y[:states]
        comp_out[b * block + states : (b + 1) * block, :] = y[states : states + EXTRA] + vecs[top + b : top + b + 1, :]

    def tables():
        fourth = held[3]
        u = moves[0:total, :] + combine(moves, 0)
        u_rows[...] = u
        u_4[...] = times(u, tall(fourth))
        rhs = deep(theta_d[...])
        whole = jnp.zeros((states, states), F32)
        theta[0] = jnp.zeros_like(whole)
        theta_4[0] = split(jnp.zeros_like(whole))
        for a in range(4):
            full = [None] + wide(pair_2[a], rhs)
            for c in range(4):
                if a + c > 0:
                    parts = [q for q in (theta_2[a - 1] if a > 0 else None, full[c]) if q is not None]
                    whole = sum(parts[1:], parts[0])
                    theta[a * 4 + c] = whole
                    theta_4[a * 4 + c] = split(mul(whole, fourth))

    @pl.when(jnp.logical_and(far, jnp.logical_not(gives_comp)))
    def _():
        tables()

    @pl.when(gives_comp)
    def _():
        for b in range(seqs):
            mats[b].wait_recv()
            pair(b)
            comps[b].start()
        even_v[...] = rows_of(mat_in)
        pair_v[...] = rows_of(comp_out)

    @pl.when(gives_comp)
    def _():
        tables()

    @pl.when(jnp.logical_and(has_mat, jnp.logical_not(gives_comp)))
    def _():
        for b in range(seqs):
            mats[b].wait_recv()
        for b in range(seqs):
            pair(b)
        even_v[...] = rows_of(mat_in)
        pair_v[...] = rows_of(comp_out)

    def double(level):
        half = 1 << (level - 1)
        powers[2 * half] = mul_node(powers[half], powers[half])

    def fill():
        powers[0] = split(
            (
                lax.broadcasted_iota(jnp.int32, (states, states), 0)
                == lax.broadcasted_iota(jnp.int32, (states, states), 1)
            ).astype(F32)
        )
        for level in range(1, levels):
            base = powers[1 << level]
            for e in range(1, 1 << level):
                powers[(1 << level) + e] = mul_node(powers[e], base)
        laps[0] = powers[0]
        laps[1] = powers[chunks]
        for m in range(2, 2 * chips - 2):
            laps[m] = mul_node(laps[m // 2], laps[m - m // 2])

    @pl.when(pos == 3)
    def _():
        to_back.wait_recv()
        vec_out[...] = apply(lefts(vec_in[...]), pair_node, pair_v[...])

        @pl.when(pos < n - 1)
        def _():
            for copy in to_next:
                copy.start()

    @pl.when(near_4)
    def _():
        for level in range(1, levels + 1):
            double(level)

    def prepare():
        for b in range(seqs):
            for level in range(levels, 0, -1):
                for p in range(chunks >> level):
                    mat_2, v = child(level, (b * (chunks >> level) + p) * 2)
                    k = (p << level) + (1 << (level - 1))
                    if p > 0:
                        before = b * chunks + (p << level)
                        lead = leading(heads[before], head_vecs[before : before + 1, :])
                        y = wide(lead, deep(mat_2))[0]
                        mat_2 = split(y[:states])
                        v = y[states : states + 1] + v
                    heads[b * chunks + k] = mat_2
                    head_vecs[b * chunks + k : b * chunks + k + 1, :] = v

    @pl.when(far)
    def _():
        for level in range(1, levels + 1):
            lag = powers[1 << (level - 1)]
            double(level)
            for j in range(total >> level):
                left, v_left = child(level, 2 * j)
                lead = leading(left, v_left)
                a, b = 2 * j, 2 * j + 1
                if level == 1:
                    y = wide(lead, deep(theta_4[words[b]]))[0]
                    whole = theta[words[a]] + y[:states]
                    u = y[states : states + EXTRA] + u_4[b : b + 1, :] + u_rows[a : a + 1, :]
                else:
                    a, b = first[level - 1] + a, first[level - 1] + b
                    y = wide(lead, deep(psi_n[b]))[0]
                    y = jnp.concatenate([y[:states], y[states:] + us[b : b + 1, :]], axis=0)
                    y = mul(y, lag)
                    whole = psi_f[a] + y[:states]
                    u = y[states : states + EXTRA] + us[a : a + 1, :]
                k = first[level] + j
                if level == levels:
                    psi_out[j * block : j * block + states, :] = whole
                    psi_out[j * block + states : (j + 1) * block, :] = u
                else:
                    us[k : k + 1, :] = u[0:1]
                    if j % 2 == 0:
                        psi_f[k] = whole
                    else:
                        psi_n[k] = split(whole)

    @pl.when(jnp.logical_and(gives_mat, far))
    def _():
        psi.start()

    @pl.when(far)
    def _():
        for b in range(seqs):
            psi_own[b] = split(psi_out[b * block : b * block + states, :])
        psi_v[...] = rows_of(psi_out)

    @pl.when(jnp.logical_and(odd, far))
    def _():
        lap = powers[chunks]
        for b in range(seqs):
            v_left = mat_in[b * block + states : b * block + states + 1, :]
            y = wide(leading(even_node[b], v_left), deep(psi_own[b]))[0]
            u = psi_out[b * block + states : b * block + states + 1, :]
            y = jnp.concatenate([y[:states], y[states:] + u], axis=0)
            later[b * block : (b + 1) * block, :] = mul(y, lap)[:block]

    direct = jnp.logical_and(odd, far)

    headed = jnp.logical_and(even, far)

    @pl.when(headed)
    def _():
        prepare()

    def send_off(d, side):
        return pltpu.make_async_remote_copy(
            src_ref=off_out, dst_ref=off_in.at[d - 1], send_sem=off_send.at[d - 1], recv_sem=off_recv.at[d - 1],
            device_id={"tm": lax.rem(2 * (chip + chips - d) + side, n)}, device_id_type=MESH,
        )

    @pl.when(has_comp)
    def _():
        to_back.wait_recv()
        arrived(comp_in, comp_sem.at[1])
        for b in range(seqs):
            prev_node[b] = split(comp_in[b * block : b * block + states, :])
        prev_v[...] = rows_of(comp_in)
        back = apply(lefts(vec_in[...]), prev_node, prev_v[...])
        vec_back[...] = back
        to_back.start()
        state[...] = back

    @pl.when(direct)
    def _():
        psi.wait_recv()
        for b in range(seqs):
            psi_in[b * block : (b + 1) * block, :] += later[b * block : (b + 1) * block, :]
            omega_node[b] = split(psi_in[b * block : b * block + states, :])
        omega_v[...] = rows_of(psi_in)

    @pl.when(jnp.logical_and(jnp.logical_or(pos == 2, pos >= 4), jnp.logical_not(has_comp)))
    def _():
        to_back.wait_recv()

    @pl.when(jnp.logical_not(has_comp))
    def _():
        state[...] = vec_in[...]

    @pl.when(jnp.logical_and(has_comp, pos < n - 1))
    def _():
        vec_out[...] = apply(lefts(state[...]), pair_node, pair_v[...])
        for copy in to_next:
            copy.start()

    @pl.when(jnp.logical_and(odd, far))
    def _():
        left = lefts(state[...])
        off_out[...] = apply(left, omega_node, omega_v[...])
        for d in range(chips - 1, 0, -1):
            @pl.when(chip - d >= 0)
            def _(d=d):
                send_off(d, 1).start()
                send_off(d, 0).start()
        x = apply(left, even_node, even_v[...])
        state[...] = x
        near_out[...] = apply(lefts(x), psi_own, psi_v[...])
        near.start()

    @pl.when(pos == 3)
    def _():
        state[...] = apply(lefts(state[...]), even_node, even_v[...])

    def send_sum(d):
        return pltpu.make_async_remote_copy(
            src_ref=sum_buf, dst_ref=sum_in.at[d], send_sem=sum_sem.at[0], recv_sem=sum_sem.at[1],
            device_id={"tm": lax.rem(pos + d + 1, n)}, device_id_type=MESH,
        )

    def score(priors):
        squares = jnp.zeros((total, states), F32)
        seen = jnp.zeros((total, states), F32)
        for i in range(WORD):
            error = at(obs, i) - mul(priors[i], held[6])
            squares = squares + at(mask, i) * error * error
            seen = seen + at(mask, i)
        squares = active * jnp.sum(squares, axis=0, keepdims=True)
        number = jnp.sum(seen, axis=0, keepdims=True)
        sum_buf[...] = jnp.where(row8 == 0, jnp.broadcast_to(squares, (8, states)), jnp.broadcast_to(number, (8, states)))
        for e in range(1, n):
            @pl.when(pos + e >= n)
            def _(e=e):
                send_sum(e - 1).start()

        for e in range(n - 1, 0, -1):
            @pl.when(pos + e < n)
            def _(e=e):
                send_sum(e - 1).start()

    def priors_held():
        return [prior[i * total : (i + 1) * total, :] for i in range(WORD)]

    @pl.when(headed)
    def _():
        x = state[...]
        spread = jnp.concatenate([jnp.concatenate([tall(heads[b * chunks + k]) for k in range(1, chunks)], axis=1) for b in range(seqs)], axis=0)
        y = product(lefts(x), spread)
        for b in range(seqs):
            ents[b * chunks : b * chunks + 1, :] = x[b : b + 1]
            for k in range(1, chunks):
                r = b * chunks + k
                ents[r : r + 1, :] = y[b : b + 1, (k - 1) * states : k * states] + head_vecs[r : r + 1, :]
        start = ents[...]
        y = times(start, jnp.concatenate([step_rhs[...]] + [tall(pair_2[a]) for a in range(4)], axis=1))
        y = [y[:, k * states : (k + 1) * states] for k in range(6)]
        on = [at(mask, i) > 0.5 for i in range(2)]
        one = y[0] + jnp.where(on[0], y[1], 0.0) + at(drive, 0)
        two = jnp.where(on[0], jnp.where(on[1], y[5], y[4]), jnp.where(on[1], y[3], y[2])) + zero_2[...]
        score([start, one, two, advance(two, 2)[0]])

    @pl.when(jnp.logical_not(headed))
    def _():
        x = state[...]
        entering = [jnp.broadcast_to(x[b : b + 1], (8, states)) for b in range(seqs)]
        for level in range(levels, 0, -1):
            below = []
            for j in range(total >> level):
                node, v = child(level, 2 * j)
                below.append(entering[j])
                below.append(times(entering[j], tall(node)) + v)
            entering = below
        for j in range(total):
            ents[j : j + 1, :] = entering[j][0:1]

    x = ents[...]
    for i in range(WORD):
        prior[i * total : (i + 1) * total, :] = x
        x, move = advance(x, i)
        filt[i * total : (i + 1) * total, :] = x
        moves[i * total : (i + 1) * total, :] = move

    @pl.when(direct)
    def _():
        score(priors_held())

    chunk8[...] = jnp.zeros_like(chunk8)
    for i in range(WORD - 1):
        z = combine(moves, i)
        suffix[i * total : (i + 1) * total, :] = filt[i * total : (i + 1) * total, :] + z
        if i == 0:
            z = z + moves[0:total, :]
            for b in range(seqs):
                chunk8[pl.ds(b, chunks, stride=8), :] = z[b * chunks : (b + 1) * chunks]
    i = WORD - 1
    suffix[i * total : (i + 1) * total, :] = filt[i * total : (i + 1) * total, :]
    ends = chunk8[...].reshape(chunks, 8, states)

    ups = [ends]
    for level in range(levels):
        pair = ups[-1].reshape(ups[-1].shape[0] // 2, 2, 8, states)
        half = pair.shape[0]
        later = times(pair[:, 1].reshape(half * 8, states), tall(powers[1 << level]))
        ups.append(pair[:, 0] + later.reshape(half, 8, states))

    def send_first(slot, side):
        dst = off_in.at[0] if slot == 0 else first_in
        return pltpu.make_async_remote_copy(
            src_ref=off_out, dst_ref=dst, send_sem=off_send.at[0],
            recv_sem=off_recv.at[0] if slot == 0 else first_sem,
            device_id={"tm": side}, device_id_type=MESH,
        )

    @pl.when(near_4)
    def _():
        off_out[...] = ups[-1].reshape(8, states)
        near_out[...] = ups[-1].reshape(8, states)
        for slot in range(2):
            @pl.when(pos == 2 + slot)
            def _(slot=slot):
                send_first(slot, 0).start()
                send_first(slot, 1).start()

        @pl.when(odd)
        def _():
            near.start()

        score(priors_held())

    x = jnp.zeros((1, 8, states), F32)
    for level in range(levels - 1, -1, -1):
        count = x.shape[0]
        pair = ups[level].reshape(count, 2, 8, states)
        if level == levels - 1:
            sooner = pair[:, 1]
        else:
            moved = times(x.reshape(count * 8, states), tall(powers[1 << level]))
            sooner = moved.reshape(count, 8, states) + pair[:, 1]
        x = jnp.stack([sooner, x], axis=1).reshape(2 * count, 8, states)
    chunk8[...] = x.reshape(chunks * 8, states)
    fill()

    @pl.when(even)
    def _():
        near.wait_recv()

    @pl.when(chip == 0)
    def _():
        send_first(1, 0).wait_recv()

    for d in range(1, chips):
        @pl.when(chip + d < chips)
        def _(d=d):
            send_off(d, 0).wait_recv()

    left = jnp.concatenate([twice(stacked(a)) for a in [first_in[...]] + [off_in[d] for d in range(chips - 1)]], axis=1)
    rhs = jnp.concatenate([tall(laps[2 - par])] + [tall(laps[2 * d + 1 - par]) for d in range(chips - 1)], axis=0)
    x = near_in[...] + product(left, rhs)
    y = times(x, jnp.concatenate([tall(powers[chunks - 1 - k]) for k in range(chunks)], axis=1))
    for k in range(chunks):
        chunk8[k * 8 : (k + 1) * 8, :] += y[:, k * states : (k + 1) * states]
    x = jnp.concatenate([chunk8[pl.ds(b, chunks, stride=8), :] for b in range(seqs)], axis=0)
    y = times(x, jnp.concatenate([tall(a) for a in (held[3], held[2], held[1], held[0])], axis=1))
    for i in range(WORD):
        out[pl.ds(i, total, stride=WORD), :] = (
            suffix[i * total : (i + 1) * total, :] + y[:, i * states : (i + 1) * states]
        )

    arrived(sum_in.at[pl.ds(0, n - 1)], sum_sem.at[1])
    sums = sum_buf[...]
    for d in range(n - 1):
        sums = sums + sum_in[d]
    squares, number = sums[0:1], sums[1:2]
    grad = 0.5 * active * (number - weight * squares)
    new_prec[...] = log_prec[...] + grad / (seqs * steps * n)
    terms = 0.5 * active * (log_prec[...] * number - weight * squares)
    loglik[...] = jnp.zeros_like(terms) + jnp.sum(terms, axis=1, keepdims=True) / (seqs * steps * n * states)

    @pl.when(gives_mat)
    def _():
        arrived(mat_out, mat_sem.at[0])

    @pl.when(jnp.logical_and(gives_mat, far))
    def _():
        psi.wait_send()

    @pl.when(gives_comp)
    def _():
        arrived(comp_out, comp_sem.at[0])

    @pl.when(pos == 0)
    def _():
        to_next[2].wait_send()

    @pl.when(pos == 1)
    def _():
        arrived(off_in.at[pl.ds(0, 2)], vec_send.at[0])

    @pl.when(last_of_four)
    def _():
        arrived(off_in.at[pl.ds(0, 3)], vec_send.at[0])

    @pl.when(has_comp)
    def _():
        to_back.wait_send()

    @pl.when(odd)
    def _():
        near.wait_send()

    for d in range(1, chips):
        @pl.when(jnp.logical_and(jnp.logical_and(odd, far), chip - d >= 0))
        def _(d=d):
            arrived(off_in.at[pl.ds(0, 2)], off_send.at[d - 1])

    for slot in range(2):
        @pl.when(pos == 2 + slot)
        def _(slot=slot):
            arrived(off_in.at[pl.ds(0, 2)], off_send.at[0])

    arrived(sum_in.at[pl.ds(0, n - 1)], sum_sem.at[0])


def mul_node(left, right):
    return split(wide(left, deep(right))[0])


def finish(smoothed, new_prec, loglik, out, out_prec, out_loglik):
    out[...] = smoothed[...]
    out_prec[...] = new_prec[...]
    out_loglik[...] = loglik[:, 0:1]


def local(n, obs, present, sensors, log_prec, dynamics, prior_var, obs_map, init_state):
    seqs, steps, channels = obs.shape
    states = dynamics.shape[0]
    assert n % 4 == 0 and states == 128 and channels == 128
    chunks = steps // WORD
    total = seqs * chunks
    chips = n // 2
    inner = sum(total >> level for level in range(1, int(math.log2(chunks)) + 1))
    vmem = pl.BlockSpec(memory_space=pltpu.VMEM)
    smem = pl.BlockSpec(memory_space=pltpu.SMEM)
    rows = seqs * steps
    block = seqs * (states + EXTRA)
    node = (states, 2 * states)
    tile = pltpu.VMEM((8, states), F32)
    whole = pltpu.VMEM((block, states), F32)
    level_rows = (inner + 7) // 8 * 8
    dma = pltpu.SemaphoreType.DMA
    smoothed, new_prec, loglik = pl.pallas_call(
        functools.partial(kernel, n, seqs, steps),
        out_shape=(
            pltpu.VMEM((rows, states), F32),
            pltpu.VMEM((1, channels), F32),
            pltpu.VMEM((1, channels), F32),
        ),
        in_specs=[smem, smem] + [vmem] * 7,
        out_specs=(vmem, vmem, vmem),
        scratch_shapes=[
            pltpu.SMEM((total,), jnp.int32),
            pltpu.VMEM((2**WORD,) + node, BF16),
            pltpu.VMEM((2**WORD, states, states), F32),
            pltpu.VMEM((2**WORD,) + node, BF16),
            pltpu.VMEM((inner,) + node, BF16),
            pltpu.VMEM((level_rows, states), F32),
            pltpu.VMEM((inner, states, states), F32),
            pltpu.VMEM((inner,) + node, BF16),
            pltpu.VMEM((level_rows, states), F32),
            pltpu.VMEM((total, states), F32),
            pltpu.VMEM((total, states), F32),
            pltpu.VMEM((total, states), F32),
            pltpu.VMEM((total, states), F32),
            pltpu.VMEM((chunks + 1,) + node, BF16),
            pltpu.VMEM((2 * chips - 2,) + node, BF16),
            pltpu.VMEM((2 * states, 2 * states), BF16),
            pltpu.VMEM((rows, states), F32),
            pltpu.VMEM((rows, states), F32),
            pltpu.VMEM((rows, states), F32),
            pltpu.VMEM((rows, states), F32),
            pltpu.VMEM((rows, states), F32),
            pltpu.VMEM((chunks * 8, states), F32),
            pltpu.VMEM((rows, states), F32),
            pltpu.VMEM((8,) + node, BF16),
            pltpu.VMEM((4,) + node, BF16),
            pltpu.VMEM((total, states), F32),
            pltpu.VMEM((3, states, states), F32),
            pltpu.VMEM((states, 6 * states), BF16),
            whole,
            pltpu.VMEM((total,) + node, BF16),
            pltpu.VMEM((total, states), F32),
            pltpu.VMEM((seqs,) + node, BF16), tile,
            pltpu.VMEM((seqs,) + node, BF16), tile,
            pltpu.VMEM((seqs,) + node, BF16), tile,
            pltpu.VMEM((seqs,) + node, BF16), tile,
            pltpu.VMEM((seqs,) + node, BF16), tile,
            tile,
            tile, tile, tile, whole, whole, whole, whole, whole, whole,
            tile, pltpu.VMEM((chips - 1, 8, states), F32), tile, tile, tile, tile, pltpu.VMEM((n, 8, states), F32),
            dma((2,)), dma(()), dma((1 + seqs,)), dma((2,)), dma((2,)), dma((2,)),
            dma((chips - 1,)), dma((chips - 1,)), dma(()), dma((2,)),
        ],
        compiler_params=pltpu.CompilerParams(collective_id=0, has_side_effects=True),
        name="kalman",
    )(
        present, sensors, obs.reshape(rows, channels), present, log_prec.reshape(1, channels),
        dynamics, prior_var.reshape(1, states), obs_map, init_state,
    )
    held = [pltpu.with_memory_space_constraint(a, pltpu.VMEM) for a in (smoothed, new_prec, loglik)]
    smoothed, new_prec, loglik = pl.pallas_call(
        finish,
        out_shape=(
            jax.ShapeDtypeStruct((rows, states), F32),
            jax.ShapeDtypeStruct((1, channels), F32),
            jax.ShapeDtypeStruct((1, 1), F32),
        ),
        in_specs=[vmem] * 3,
        out_specs=(vmem, vmem, vmem),
        name="finish",
    )(*held)
    return smoothed.reshape(seqs, steps, states), new_prec.reshape(channels), loglik.reshape(1)


def solution(mesh):
    in_specs = (
        P("cluster", "tm", None),
        P("cluster", "tm"),
        P("cluster"),
        P("cluster"),
        P("cluster", None),
        P("cluster"),
        P("cluster", None),
        P("cluster", None),
    )
    out_specs = (P("cluster", "tm", None), P("cluster"), P("cluster"))
    body = functools.partial(local, mesh.shape["tm"])
    return jax.shard_map(body, mesh=mesh, in_specs=in_specs, out_specs=out_specs, check_vma=False)
```

```python
import functools
import math

import jax
import jax.numpy as jnp
from jax import lax
from jax.experimental import pallas as pl
from jax.experimental.pallas import tpu as pltpu
from jax.sharding import PartitionSpec as P

F32 = jnp.float32
BF16 = jnp.bfloat16
MESH = pl.DeviceIdType.MESH
WORD = 4
EXTRA = 8


def split(a):
    high = a.astype(BF16).astype(F32)
    return jnp.concatenate([high, a - high], axis=1).astype(BF16)


def stacked(a):
    high = a.astype(BF16).astype(F32)
    return jnp.concatenate([high, a - high], axis=0).astype(BF16)


def deep(node):
    return jnp.concatenate([node, node], axis=0)


def tall(node):
    width = node.shape[1] // 2
    return jnp.concatenate([node[:, :width], node[:, width:]], axis=0)


def twice(s):
    return jnp.concatenate([s, s], axis=1)


def product(left, right):
    full = jnp.dot(left, right, preferred_element_type=F32)
    rows = full.shape[0] // 2
    return full[:rows] + full[rows:]


def times(a, right):
    return product(twice(stacked(a)), right)


def wide(left, right):
    full = jnp.dot(left, right, preferred_element_type=F32)
    half = left.shape[1] // 2 if left.shape[1] < 256 else 128
    return [
        full[:, 2 * k * half : (2 * k + 1) * half] + full[:, (2 * k + 1) * half : (2 * k + 2) * half]
        for k in range(full.shape[1] // (2 * half))
    ]


def mul(a, node):
    return wide(split(a), deep(node))[0]


def kernel(
    n, seqs, steps,
    present_s, sensors_s, obs, present_v, log_prec, dyn, prior_var, obs_map, init,
    out, new_prec, loglik,
    words, table, theta, theta_4, nodes, vecs, psi_f, psi_n, us, offs, u_rows, u_4, ents, powers, laps, step_rhs,
    drive, mask, prior, filt, suffix, chunk8, moves, held, pair_2, zero_2, theta_2, theta_d, later, heads, head_vecs,
    even_node, even_v, pair_node, pair_v, prev_node, prev_v, omega_node, omega_v, psi_own, psi_v, state,
    vec_in, vec_out, vec_back, mat_out, mat_in, comp_out, comp_in, early_in, psi_out, psi_in,
    off_out, off_in, first_in, near_out, near_in, sum_buf, sum_in,
    vec_send, vec_recv, mat_sem, early_sem, comp_sem, psi_sem, near_sem, off_send, off_recv, first_sem, sum_sem,
):
    pos = lax.axis_index("tm")
    par = lax.rem(pos, 2)
    quarter = lax.rem(pos, 4)
    chip = lax.div(pos, 2)
    chips = n // 2
    states = dyn.shape[0]
    block = states + EXTRA
    chunks = steps // WORD
    total = seqs * chunks
    levels = int(math.log2(chunks))
    first = [0]
    for level in range(1, levels + 1):
        first.append(first[-1] + (total >> (level - 1) if level > 1 else 0))
    top = first[levels]

    vec_in[...] = jnp.zeros_like(vec_in)
    off_in[...] = jnp.zeros_like(off_in)
    near_in[...] = jnp.zeros_like(near_in)
    first_in[...] = jnp.zeros_like(first_in)
    barrier = pltpu.get_barrier_semaphore()
    for d in range(1, n):
        pl.semaphore_signal(barrier, inc=1, device_id={"tm": lax.rem(pos + d, n)}, device_id_type=MESH)

    lane = lax.broadcasted_iota(jnp.int32, (1, states), 1)
    row8 = lax.broadcasted_iota(jnp.int32, (8, states), 0)
    active = (lane < sensors_s[0]).astype(F32)
    weight = jnp.exp(log_prec[...])
    weight_on = weight * active
    pv = prior_var[...]
    d_mat = dyn[...]
    d_t = d_mat.T
    h_mat = obs_map[...]
    h_2 = split(h_mat)
    d_2n = split(d_mat)
    d_t2 = split(d_t)
    readout = wide(d_t2, deep(split(h_mat.T)))[0]
    gain = -(mul(readout * weight_on, h_2) * pv)
    f_t2 = split(d_t + gain)
    held[0] = d_2n
    held[4] = d_t2
    held[5] = split(gain)
    held[6] = split(readout)

    for b in range(seqs):
        for k in range(chunks):
            t = k * WORD
            w = present_s[b, t]
            for i in range(1, WORD):
                w = w * 2 + present_s[b, t + i]
            words[b * chunks + k] = w
        row = jnp.broadcast_to(present_v[b : b + 1, :].astype(F32), (steps, steps))
        same = lax.broadcasted_iota(jnp.int32, (steps, steps), 0) == lax.broadcasted_iota(jnp.int32, (steps, steps), 1)
        column = jnp.sum(jnp.where(same, row, 0.0), axis=1, keepdims=True)
        mask[b * steps : (b + 1) * steps, :] = jnp.broadcast_to(column, (steps, states))

    drive[...] = mul(obs[...] * weight_on, h_2) * pv * mask[...]

    step_rhs[...] = stacked(jnp.concatenate([d_t, gain], axis=1))
    singles = [d_t2, f_t2]
    both = deep(jnp.concatenate(singles, axis=1))
    pairs = []
    for a in range(2):
        pairs += [split(q) for q in wide(singles[a], both)]
    for a in range(4):
        pair_2[a] = pairs[a]
    held[7] = f_t2
    quad_rhs = deep(jnp.concatenate(pairs, axis=1))
    for a in range(4):
        quad = wide(pairs[a], quad_rhs)
        for c in range(4):
            table[a * 4 + c] = split(quad[c])

    def at(ref, i):
        return ref[pl.ds(i, total, stride=WORD), :]

    def advance(x, i):
        y = times(x, step_rhs[...])
        move = jnp.where(at(mask, i) > 0.5, y[:, states:], 0.0) + at(drive, i)
        return y[:, :states] + move, move

    x = at(drive, 0)
    moves[0:total, :] = x
    for i in range(1, WORD):
        x, move = advance(x, i)
        moves[i * total : (i + 1) * total, :] = move
        if i == 1:
            zero_2[...] = x
    offs[...] = x

    def combine(moved, first):
        left = jnp.concatenate([twice(stacked(moved[j * total : (j + 1) * total, :])) for j in range(first + 1, WORD)], axis=1)
        return product(left, jnp.concatenate([tall(held[j]) for j in range(WORD - 1 - first)], axis=0))

    def leading(matrix, v):
        return jnp.concatenate([matrix, split(jnp.broadcast_to(v, (16, states)))], axis=0)

    def child(level, j):
        if level == 1:
            return table[words[j]], offs[j : j + 1, :]
        j = first[level - 1] + j
        return nodes[j], vecs[j : j + 1, :]

    for level in range(1, levels + 1):
        for j in range(total >> level):
            left, v_left = child(level, 2 * j)
            right, v_right = child(level, 2 * j + 1)
            y = wide(leading(left, v_left), deep(right))[0]
            j = first[level] + j
            v = y[states : states + EXTRA] + v_right
            nodes[j] = split(y[:states])
            vecs[j : j + 1, :] = v[0:1]
            if level == levels:
                b = j - top
                mat_out[b * block : b * block + states, :] = y[:states]
                mat_out[b * block + states : (b + 1) * block, :] = v

    def lefts(x):
        return jnp.concatenate([twice(stacked(jnp.where(row8 == b, x, 0.0))) for b in range(seqs)], axis=1)

    def apply(left, node, v):
        rhs = jnp.concatenate([tall(node[b]) for b in range(seqs)], axis=0)
        return product(left, rhs) + v

    def rows_of(ref):
        v = jnp.zeros((8, states), F32)
        for b in range(seqs):
            v = jnp.where(row8 == b, ref[b * block + states : (b + 1) * block, :], v)
        return v

    own = nodes.at[pl.ds(top, seqs)]

    def own_v():
        v = jnp.zeros((8, states), F32)
        for b in range(seqs):
            v = jnp.where(row8 == b, vecs[top + b : top + b + 1, :], v)
        return v

    def send_vec(src, slot, to):
        return pltpu.make_async_remote_copy(
            src_ref=src, dst_ref=vec_in, send_sem=vec_send.at[slot // 3], recv_sem=vec_recv,
            device_id={"tm": to}, device_id_type=MESH,
        )

    def shift(by):
        return lax.rem(pos + (by + n), n)

    def send_mat(src, dst, sem, by):
        return pltpu.make_async_remote_copy(
            src_ref=src, dst_ref=dst, send_sem=sem.at[0], recv_sem=sem.at[1],
            device_id={"tm": shift(by)}, device_id_type=MESH,
        )

    def arrived(ref, sem):
        pltpu.make_async_copy(ref, ref, sem).wait()

    def send_part(src, dst, sem, by, b):
        rows = pl.ds(b * block, block)
        return pltpu.make_async_remote_copy(
            src_ref=src.at[rows], dst_ref=dst.at[rows], send_sem=sem.at[0], recv_sem=sem.at[1 + (b if by == 1 else 0)],
            device_id={"tm": shift(by)}, device_id_type=MESH,
        )

    def send_early(slot, by):
        return pltpu.make_async_remote_copy(
            src_ref=mat_out.at[pl.ds(0, block)], dst_ref=early_in.at[pl.ds(slot * block, block)],
            send_sem=early_sem.at[0], recv_sem=early_sem.at[1 + slot],
            device_id={"tm": shift(by)}, device_id_type=MESH,
        )

    early = [send_early(0, 3), send_early(1, 2)]
    order = list(range(1, seqs)) + [0]
    mats = [send_part(mat_out, mat_in, mat_sem, 1, b) for b in range(seqs)]
    comps = [None] + [send_part(comp_out, comp_in, comp_sem, 2, b) for b in range(1, seqs)]
    psi = send_mat(psi_out, psi_in, psi_sem, 1)
    near = send_mat(near_out, near_in, near_sem, -1)
    to_next = [send_vec(vec_out, k, shift(by)) for k, by in enumerate((2, 4, 1))]
    to_back = send_vec(vec_back, 3, shift(-1))

    even = par == 0
    odd = par == 1
    has_mat = jnp.logical_and(odd, pos >= 2)
    gives_mat = jnp.logical_and(even, pos >= 2)
    gives_comp = jnp.logical_and(quarter == 1, pos >= 4)
    has_comp = jnp.logical_and(quarter == 3, pos >= 4)
    last_of_four = jnp.logical_and(quarter == 3, pos < n - 1)

    pl.semaphore_wait(barrier, n - 1)

    @pl.when(gives_mat)
    def _():
        for b in order:
            mats[b].start()

        @pl.when(quarter == 0)
        def _():
            early[0].start()

    @pl.when(gives_comp)
    def _():
        early[1].start()

    @pl.when(pos == 0)
    def _():
        vec_in[0:seqs, :] = init[...]
        vec_out[...] = apply(lefts(vec_in[...]), own, own_v())
        to_next[2].start()

    near_4 = pos < 4
    far = pos >= 4

    base = held[0]
    held[1] = mul_node(base, base)
    square = held[1]
    held[2] = mul_node(base, square)
    held[3] = mul_node(square, square)
    powers[1] = held[3]
    rhs = deep(mul_node(held[5], base))
    change = held[5]
    change = change[:, :states].astype(F32) + change[:, states:].astype(F32)
    parts = [wide(held[4], rhs)[0], change, change + wide(held[7], rhs)[0]]
    for a in range(3):
        theta_2[a] = parts[a]
        theta_d[:, 2 * a * states : 2 * (a + 1) * states] = split(mul(parts[a], square))

    @pl.when(pos == 1)
    def _():
        to_back.wait_recv()
        vec_out[...] = apply(lefts(vec_in[...]), own, own_v())
        to_next[0].start()
        to_next[2].start()

    def pair(b):
        left = split(mat_in[b * block : b * block + states, :])
        even_node[b] = left
        v_left = mat_in[b * block + states : b * block + states + 1, :]
        y = wide(leading(left, v_left), deep(nodes[top + b]))[0]
        pair_node[b] = split(y[:states])
        comp_out[b * block : b * block + states, :] = y[:states]
        comp_out[b * block + states : (b + 1) * block, :] = y[states : states + EXTRA] + vecs[top + b : top + b + 1, :]

    def tables():
        fourth = held[3]
        u = moves[0:total, :] + combine(moves, 0)
        u_rows[...] = u
        u_4[...] = times(u, tall(fourth))
        rhs = deep(theta_d[...])
        whole = jnp.zeros((states, states), F32)
        theta[0] = jnp.zeros_like(whole)
        theta_4[0] = split(jnp.zeros_like(whole))
        for a in range(4):
            full = [None] + wide(pair_2[a], rhs)
            for c in range(4):
                if a + c > 0:
                    parts = [q for q in (theta_2[a - 1] if a > 0 else None, full[c]) if q is not None]
                    whole = sum(parts[1:], parts[0])
                    theta[a * 4 + c] = whole
                    theta_4[a * 4 + c] = split(mul(whole, fourth))

    @pl.when(jnp.logical_and(far, jnp.logical_not(gives_comp)))
    def _():
        tables()

    @pl.when(gives_comp)
    def _():
        for b in order:
            mats[b].wait_recv()
            if b > 0:
                pair(b)
                comps[b].start()
            else:
                even_node[b] = split(mat_in[b * block : b * block + states, :])
        even_v[...] = rows_of(mat_in)

    @pl.when(gives_comp)
    def _():
        tables()

    @pl.when(jnp.logical_and(has_mat, jnp.logical_not(gives_comp)))
    def _():
        for b in range(seqs):
            mats[b].wait_recv()
        for b in range(seqs):
            pair(b)
        even_v[...] = rows_of(mat_in)
        pair_v[...] = rows_of(comp_out)

    def double(level):
        half = 1 << (level - 1)
        powers[2 * half] = mul_node(powers[half], powers[half])

    def fill():
        powers[0] = split(
            (
                lax.broadcasted_iota(jnp.int32, (states, states), 0)
                == lax.broadcasted_iota(jnp.int32, (states, states), 1)
            ).astype(F32)
        )
        for level in range(1, levels):
            base = powers[1 << level]
            for e in range(1, 1 << level):
                powers[(1 << level) + e] = mul_node(powers[e], base)
        laps[0] = powers[0]
        laps[1] = powers[chunks]
        for m in range(2, 2 * chips - 2):
            laps[m] = mul_node(laps[m // 2], laps[m - m // 2])

    @pl.when(pos == 3)
    def _():
        to_back.wait_recv()
        vec_out[...] = apply(lefts(vec_in[...]), pair_node, pair_v[...])

        @pl.when(pos < n - 1)
        def _():
            for copy in to_next:
                copy.start()

    @pl.when(near_4)
    def _():
        for level in range(1, levels + 1):
            double(level)

    def prepare():
        for b in range(seqs):
            for level in range(levels, 0, -1):
                for p in range(chunks >> level):
                    mat_2, v = child(level, (b * (chunks >> level) + p) * 2)
                    k = (p << level) + (1 << (level - 1))
                    if p > 0:
                        before = b * chunks + (p << level)
                        lead = leading(heads[before], head_vecs[before : before + 1, :])
                        y = wide(lead, deep(mat_2))[0]
                        mat_2 = split(y[:states])
                        v = y[states : states + 1] + v
                    heads[b * chunks + k] = mat_2
                    head_vecs[b * chunks + k : b * chunks + k + 1, :] = v

    @pl.when(far)
    def _():
        for level in range(1, levels + 1):
            lag = powers[1 << (level - 1)]
            double(level)
            for j in range(total >> level):
                left, v_left = child(level, 2 * j)
                lead = leading(left, v_left)
                a, b = 2 * j, 2 * j + 1
                if level == 1:
                    y = wide(lead, deep(theta_4[words[b]]))[0]
                    whole = theta[words[a]] + y[:states]
                    u = y[states : states + EXTRA] + u_4[b : b + 1, :] + u_rows[a : a + 1, :]
                else:
                    a, b = first[level - 1] + a, first[level - 1] + b
                    y = wide(lead, deep(psi_n[b]))[0]
                    y = jnp.concatenate([y[:states], y[states:] + us[b : b + 1, :]], axis=0)
                    y = mul(y, lag)
                    whole = psi_f[a] + y[:states]
                    u = y[states : states + EXTRA] + us[a : a + 1, :]
                k = first[level] + j
                if level == levels:
                    psi_out[j * block : j * block + states, :] = whole
                    psi_out[j * block + states : (j + 1) * block, :] = u
                else:
                    us[k : k + 1, :] = u[0:1]
                    if j % 2 == 0:
                        psi_f[k] = whole
                    else:
                        psi_n[k] = split(whole)

    @pl.when(jnp.logical_and(gives_mat, far))
    def _():
        psi.start()

    @pl.when(far)
    def _():
        for b in range(seqs):
            psi_own[b] = split(psi_out[b * block : b * block + states, :])
        psi_v[...] = rows_of(psi_out)

    @pl.when(jnp.logical_and(odd, far))
    def _():
        lap = powers[chunks]
        for b in range(seqs):
            v_left = mat_in[b * block + states : b * block + states + 1, :]
            y = wide(leading(even_node[b], v_left), deep(psi_own[b]))[0]
            u = psi_out[b * block + states : b * block + states + 1, :]
            y = jnp.concatenate([y[:states], y[states:] + u], axis=0)
            later[b * block : (b + 1) * block, :] = mul(y, lap)[:block]

    direct = jnp.logical_and(odd, far)

    headed = jnp.logical_and(even, far)

    @pl.when(headed)
    def _():
        prepare()

    def send_off(d, side):
        return pltpu.make_async_remote_copy(
            src_ref=off_out, dst_ref=off_in.at[d - 1], send_sem=off_send.at[d - 1], recv_sem=off_recv.at[d - 1],
            device_id={"tm": lax.rem(2 * (chip + chips - d) + side, n)}, device_id_type=MESH,
        )

    rest = pl.ds(block, (seqs - 1) * block)

    @pl.when(has_comp)
    def _():
        for copy in early:
            copy.wait_recv()
        v_left = early_in[states : states + 1, :]
        y = wide(leading(split(early_in[0:states, :]), v_left), deep(split(early_in[block : block + states, :])))[0]
        comp_in[0:states, :] = y[:states]
        comp_in[states:block, :] = y[states : states + EXTRA] + early_in[block + states : 2 * block, :]
        to_back.wait_recv()
        arrived(comp_in.at[rest], comp_sem.at[1])
        for b in range(seqs):
            prev_node[b] = split(comp_in[b * block : b * block + states, :])
        prev_v[...] = rows_of(comp_in)
        back = apply(lefts(vec_in[...]), prev_node, prev_v[...])
        vec_back[...] = back
        to_back.start()
        state[...] = back

    @pl.when(direct)
    def _():
        psi.wait_recv()
        for b in range(seqs):
            psi_in[b * block : (b + 1) * block, :] += later[b * block : (b + 1) * block, :]
            omega_node[b] = split(psi_in[b * block : b * block + states, :])
        omega_v[...] = rows_of(psi_in)

    @pl.when(jnp.logical_and(jnp.logical_or(pos == 2, pos >= 4), jnp.logical_not(has_comp)))
    def _():
        to_back.wait_recv()

    @pl.when(jnp.logical_not(has_comp))
    def _():
        state[...] = vec_in[...]

    @pl.when(jnp.logical_and(has_comp, pos < n - 1))
    def _():
        vec_out[...] = apply(lefts(state[...]), pair_node, pair_v[...])
        for copy in to_next:
            copy.start()

    @pl.when(jnp.logical_and(odd, far))
    def _():
        left = lefts(state[...])
        off_out[...] = apply(left, omega_node, omega_v[...])
        for d in range(chips - 1, 0, -1):
            @pl.when(chip - d >= 0)
            def _(d=d):
                send_off(d, 1).start()
                send_off(d, 0).start()
        x = apply(left, even_node, even_v[...])
        state[...] = x
        near_out[...] = apply(lefts(x), psi_own, psi_v[...])
        near.start()

    @pl.when(pos == 3)
    def _():
        state[...] = apply(lefts(state[...]), even_node, even_v[...])

    def send_sum(d):
        return pltpu.make_async_remote_copy(
            src_ref=sum_buf, dst_ref=sum_in.at[d], send_sem=sum_sem.at[0], recv_sem=sum_sem.at[1],
            device_id={"tm": lax.rem(pos + d + 1, n)}, device_id_type=MESH,
        )

    def score(priors):
        squares = jnp.zeros((total, states), F32)
        seen = jnp.zeros((total, states), F32)
        for i in range(WORD):
            error = at(obs, i) - mul(priors[i], held[6])
            squares = squares + at(mask, i) * error * error
            seen = seen + at(mask, i)
        squares = active * jnp.sum(squares, axis=0, keepdims=True)
        number = jnp.sum(seen, axis=0, keepdims=True)
        sum_buf[...] = jnp.where(row8 == 0, jnp.broadcast_to(squares, (8, states)), jnp.broadcast_to(number, (8, states)))
        for e in range(1, n):
            @pl.when(pos + e >= n)
            def _(e=e):
                send_sum(e - 1).start()

        for e in range(n - 1, 0, -1):
            @pl.when(pos + e < n)
            def _(e=e):
                send_sum(e - 1).start()

    def quick():
        start = ents[...]
        y = times(start, jnp.concatenate([step_rhs[...]] + [tall(pair_2[a]) for a in range(4)], axis=1))
        y = [y[:, k * states : (k + 1) * states] for k in range(6)]
        on = [at(mask, i) > 0.5 for i in range(2)]
        one = y[0] + jnp.where(on[0], y[1], 0.0) + at(drive, 0)
        two = jnp.where(on[0], jnp.where(on[1], y[5], y[4]), jnp.where(on[1], y[3], y[2])) + zero_2[...]
        score([start, one, two, advance(two, 2)[0]])

    def priors_held():
        return [prior[i * total : (i + 1) * total, :] for i in range(WORD)]

    @pl.when(headed)
    def _():
        x = state[...]
        spread = jnp.concatenate([jnp.concatenate([tall(heads[b * chunks + k]) for k in range(1, chunks)], axis=1) for b in range(seqs)], axis=0)
        y = product(lefts(x), spread)
        for b in range(seqs):
            ents[b * chunks : b * chunks + 1, :] = x[b : b + 1]
            for k in range(1, chunks):
                r = b * chunks + k
                ents[r : r + 1, :] = y[b : b + 1, (k - 1) * states : k * states] + head_vecs[r : r + 1, :]
        quick()

    @pl.when(jnp.logical_not(headed))
    def _():
        x = state[...]
        entering = [jnp.broadcast_to(x[b : b + 1], (8, states)) for b in range(seqs)]
        for level in range(levels, 0, -1):
            below = []
            for j in range(total >> level):
                node, v = child(level, 2 * j)
                below.append(entering[j])
                below.append(times(entering[j], tall(node)) + v)
            entering = below
        for j in range(total):
            ents[j : j + 1, :] = entering[j][0:1]

        @pl.when(far)
        def _():
            quick()

    x = ents[...]
    for i in range(WORD):
        prior[i * total : (i + 1) * total, :] = x
        x, move = advance(x, i)
        filt[i * total : (i + 1) * total, :] = x
        moves[i * total : (i + 1) * total, :] = move

    chunk8[...] = jnp.zeros_like(chunk8)
    for i in range(WORD - 1):
        z = combine(moves, i)
        suffix[i * total : (i + 1) * total, :] = filt[i * total : (i + 1) * total, :] + z
        if i == 0:
            z = z + moves[0:total, :]
            for b in range(seqs):
                chunk8[pl.ds(b, chunks, stride=8), :] = z[b * chunks : (b + 1) * chunks]
    i = WORD - 1
    suffix[i * total : (i + 1) * total, :] = filt[i * total : (i + 1) * total, :]
    ends = chunk8[...].reshape(chunks, 8, states)

    ups = [ends]
    for level in range(levels):
        pair = ups[-1].reshape(ups[-1].shape[0] // 2, 2, 8, states)
        half = pair.shape[0]
        later = times(pair[:, 1].reshape(half * 8, states), tall(powers[1 << level]))
        ups.append(pair[:, 0] + later.reshape(half, 8, states))

    def send_first(slot, side):
        dst = off_in.at[0] if slot == 0 else first_in
        return pltpu.make_async_remote_copy(
            src_ref=off_out, dst_ref=dst, send_sem=off_send.at[0],
            recv_sem=off_recv.at[0] if slot == 0 else first_sem,
            device_id={"tm": side}, device_id_type=MESH,
        )

    @pl.when(near_4)
    def _():
        off_out[...] = ups[-1].reshape(8, states)
        near_out[...] = ups[-1].reshape(8, states)
        for slot in range(2):
            @pl.when(pos == 2 + slot)
            def _(slot=slot):
                send_first(slot, 0).start()
                send_first(slot, 1).start()

        @pl.when(odd)
        def _():
            near.start()

        score(priors_held())

    x = jnp.zeros((1, 8, states), F32)
    for level in range(levels - 1, -1, -1):
        count = x.shape[0]
        pair = ups[level].reshape(count, 2, 8, states)
        if level == levels - 1:
            sooner = pair[:, 1]
        else:
            moved = times(x.reshape(count * 8, states), tall(powers[1 << level]))
            sooner = moved.reshape(count, 8, states) + pair[:, 1]
        x = jnp.stack([sooner, x], axis=1).reshape(2 * count, 8, states)
    chunk8[...] = x.reshape(chunks * 8, states)
    fill()

    @pl.when(even)
    def _():
        near.wait_recv()

    @pl.when(chip == 0)
    def _():
        send_first(1, 0).wait_recv()

    for d in range(1, chips):
        @pl.when(chip + d < chips)
        def _(d=d):
            send_off(d, 0).wait_recv()

    left = jnp.concatenate([twice(stacked(a)) for a in [first_in[...]] + [off_in[d] for d in range(chips - 1)]], axis=1)
    rhs = jnp.concatenate([tall(laps[2 - par])] + [tall(laps[2 * d + 1 - par]) for d in range(chips - 1)], axis=0)
    x = near_in[...] + product(left, rhs)
    y = times(x, jnp.concatenate([tall(powers[chunks - 1 - k]) for k in range(chunks)], axis=1))
    for k in range(chunks):
        chunk8[k * 8 : (k + 1) * 8, :] += y[:, k * states : (k + 1) * states]
    x = jnp.concatenate([chunk8[pl.ds(b, chunks, stride=8), :] for b in range(seqs)], axis=0)
    y = times(x, jnp.concatenate([tall(a) for a in (held[3], held[2], held[1], held[0])], axis=1))
    for i in range(WORD):
        out[pl.ds(i, total, stride=WORD), :] = (
            suffix[i * total : (i + 1) * total, :] + y[:, i * states : (i + 1) * states]
        )

    arrived(sum_in.at[pl.ds(0, n - 1)], sum_sem.at[1])
    sums = sum_buf[...]
    for d in range(n - 1):
        sums = sums + sum_in[d]
    squares, number = sums[0:1], sums[1:2]
    grad = 0.5 * active * (number - weight * squares)
    new_prec[...] = log_prec[...] + grad / (seqs * steps * n)
    terms = 0.5 * active * (log_prec[...] * number - weight * squares)
    loglik[...] = jnp.zeros_like(terms) + jnp.sum(terms, axis=1, keepdims=True) / (seqs * steps * n * states)

    @pl.when(gives_mat)
    def _():
        arrived(mat_out, mat_sem.at[0])

        @pl.when(quarter == 0)
        def _():
            arrived(mat_out.at[pl.ds(0, block)], early_sem.at[0])

    @pl.when(jnp.logical_and(gives_mat, far))
    def _():
        psi.wait_send()

    @pl.when(gives_comp)
    def _():
        arrived(comp_out.at[rest], comp_sem.at[0])
        arrived(mat_out.at[pl.ds(0, block)], early_sem.at[0])

    @pl.when(pos == 0)
    def _():
        to_next[2].wait_send()

    @pl.when(pos == 1)
    def _():
        arrived(off_in.at[pl.ds(0, 2)], vec_send.at[0])

    @pl.when(last_of_four)
    def _():
        arrived(off_in.at[pl.ds(0, 3)], vec_send.at[0])

    @pl.when(has_comp)
    def _():
        to_back.wait_send()

    @pl.when(odd)
    def _():
        near.wait_send()

    for d in range(1, chips):
        @pl.when(jnp.logical_and(jnp.logical_and(odd, far), chip - d >= 0))
        def _(d=d):
            arrived(off_in.at[pl.ds(0, 2)], off_send.at[d - 1])

    for slot in range(2):
        @pl.when(pos == 2 + slot)
        def _(slot=slot):
            arrived(off_in.at[pl.ds(0, 2)], off_send.at[0])

    arrived(sum_in.at[pl.ds(0, n - 1)], sum_sem.at[0])


def mul_node(left, right):
    return split(wide(left, deep(right))[0])


def finish(smoothed, new_prec, loglik, out, out_prec, out_loglik):
    out[...] = smoothed[...]
    out_prec[...] = new_prec[...]
    out_loglik[...] = loglik[:, 0:1]


def local(n, obs, present, sensors, log_prec, dynamics, prior_var, obs_map, init_state):
    seqs, steps, channels = obs.shape
    states = dynamics.shape[0]
    assert n % 4 == 0 and states == 128 and channels == 128
    chunks = steps // WORD
    total = seqs * chunks
    chips = n // 2
    inner = sum(total >> level for level in range(1, int(math.log2(chunks)) + 1))
    vmem = pl.BlockSpec(memory_space=pltpu.VMEM)
    smem = pl.BlockSpec(memory_space=pltpu.SMEM)
    rows = seqs * steps
    block = seqs * (states + EXTRA)
    node = (states, 2 * states)
    tile = pltpu.VMEM((8, states), F32)
    whole = pltpu.VMEM((block, states), F32)
    level_rows = (inner + 7) // 8 * 8
    dma = pltpu.SemaphoreType.DMA
    smoothed, new_prec, loglik = pl.pallas_call(
        functools.partial(kernel, n, seqs, steps),
        out_shape=(
            pltpu.VMEM((rows, states), F32),
            pltpu.VMEM((1, channels), F32),
            pltpu.VMEM((1, channels), F32),
        ),
        in_specs=[smem, smem] + [vmem] * 7,
        out_specs=(vmem, vmem, vmem),
        scratch_shapes=[
            pltpu.SMEM((total,), jnp.int32),
            pltpu.VMEM((2**WORD,) + node, BF16),
            pltpu.VMEM((2**WORD, states, states), F32),
            pltpu.VMEM((2**WORD,) + node, BF16),
            pltpu.VMEM((inner,) + node, BF16),
            pltpu.VMEM((level_rows, states), F32),
            pltpu.VMEM((inner, states, states), F32),
            pltpu.VMEM((inner,) + node, BF16),
            pltpu.VMEM((level_rows, states), F32),
            pltpu.VMEM((total, states), F32),
            pltpu.VMEM((total, states), F32),
            pltpu.VMEM((total, states), F32),
            pltpu.VMEM((total, states), F32),
            pltpu.VMEM((chunks + 1,) + node, BF16),
            pltpu.VMEM((2 * chips - 2,) + node, BF16),
            pltpu.VMEM((2 * states, 2 * states), BF16),
            pltpu.VMEM((rows, states), F32),
            pltpu.VMEM((rows, states), F32),
            pltpu.VMEM((rows, states), F32),
            pltpu.VMEM((rows, states), F32),
            pltpu.VMEM((rows, states), F32),
            pltpu.VMEM((chunks * 8, states), F32),
            pltpu.VMEM((rows, states), F32),
            pltpu.VMEM((8,) + node, BF16),
            pltpu.VMEM((4,) + node, BF16),
            pltpu.VMEM((total, states), F32),
            pltpu.VMEM((3, states, states), F32),
            pltpu.VMEM((states, 6 * states), BF16),
            whole,
            pltpu.VMEM((total,) + node, BF16),
            pltpu.VMEM((total, states), F32),
            pltpu.VMEM((seqs,) + node, BF16), tile,
            pltpu.VMEM((seqs,) + node, BF16), tile,
            pltpu.VMEM((seqs,) + node, BF16), tile,
            pltpu.VMEM((seqs,) + node, BF16), tile,
            pltpu.VMEM((seqs,) + node, BF16), tile,
            tile,
            tile, tile, tile, whole, whole, whole, whole, pltpu.VMEM((2 * (states + EXTRA), states), F32), whole, whole,
            tile, pltpu.VMEM((chips - 1, 8, states), F32), tile, tile, tile, tile, pltpu.VMEM((n, 8, states), F32),
            dma((2,)), dma(()), dma((1 + seqs,)), dma((3,)), dma((2,)), dma((2,)), dma((2,)),
            dma((chips - 1,)), dma((chips - 1,)), dma(()), dma((2,)),
        ],
        compiler_params=pltpu.CompilerParams(collective_id=0, has_side_effects=True),
        name="kalman",
    )(
        present, sensors, obs.reshape(rows, channels), present, log_prec.reshape(1, channels),
        dynamics, prior_var.reshape(1, states), obs_map, init_state,
    )
    held = [pltpu.with_memory_space_constraint(a, pltpu.VMEM) for a in (smoothed, new_prec, loglik)]
    smoothed, new_prec, loglik = pl.pallas_call(
        finish,
        out_shape=(
            jax.ShapeDtypeStruct((rows, states), F32),
            jax.ShapeDtypeStruct((1, channels), F32),
            jax.ShapeDtypeStruct((1, 1), F32),
        ),
        in_specs=[vmem] * 3,
        out_specs=(vmem, vmem, vmem),
        name="finish",
    )(*held)
    return smoothed.reshape(seqs, steps, states), new_prec.reshape(channels), loglik.reshape(1)


def solution(mesh):
    in_specs = (
        P("cluster", "tm", None),
        P("cluster", "tm"),
        P("cluster"),
        P("cluster"),
        P("cluster", None),
        P("cluster"),
        P("cluster", None),
        P("cluster", None),
    )
    out_specs = (P("cluster", "tm", None), P("cluster"), P("cluster"))
    body = functools.partial(local, mesh.shape["tm"])
    return jax.shard_map(body, mesh=mesh, in_specs=in_specs, out_specs=out_specs, check_vma=False)
```

```python
import functools
import math

import jax
import jax.numpy as jnp
from jax import lax
from jax.experimental import pallas as pl
from jax.experimental.pallas import tpu as pltpu
from jax.sharding import PartitionSpec as P

F32 = jnp.float32
BF16 = jnp.bfloat16
MESH = pl.DeviceIdType.MESH
WORD = 4
EXTRA = 8


def split(a):
    high = a.astype(BF16).astype(F32)
    return jnp.concatenate([high, a - high], axis=1).astype(BF16)


def stacked(a):
    high = a.astype(BF16).astype(F32)
    return jnp.concatenate([high, a - high], axis=0).astype(BF16)


def deep(node):
    return jnp.concatenate([node, node], axis=0)


def tall(node):
    width = node.shape[1] // 2
    return jnp.concatenate([node[:, :width], node[:, width:]], axis=0)


def twice(s):
    return jnp.concatenate([s, s], axis=1)


def product(left, right):
    full = jnp.dot(left, right, preferred_element_type=F32)
    rows = full.shape[0] // 2
    return full[:rows] + full[rows:]


def times(a, right):
    return product(twice(stacked(a)), right)


def wide(left, right):
    full = jnp.dot(left, right, preferred_element_type=F32)
    half = left.shape[1] // 2 if left.shape[1] < 256 else 128
    return [
        full[:, 2 * k * half : (2 * k + 1) * half] + full[:, (2 * k + 1) * half : (2 * k + 2) * half]
        for k in range(full.shape[1] // (2 * half))
    ]


def mul(a, node):
    return wide(split(a), deep(node))[0]


def kernel(
    n, seqs, steps,
    present_h, sensors_s, obs_h, log_prec_h, dyn_h, prior_var_h, obs_map_h, init_h,
    out, new_prec, loglik,
    dyn, obs_map, log_prec, prior_var, present_s, present_v, obs, init, in_sem,
    words, table, theta, theta_4, nodes, vecs, psi_f, psi_n, us, offs, u_rows, u_4, ents, powers, laps, step_rhs,
    drive, mask, prior, filt, suffix, chunk8, moves, held, pair_2, zero_2, theta_2, theta_d, later, heads, head_vecs,
    even_node, even_v, pair_node, pair_v, prev_node, prev_v, omega_node, omega_v, psi_own, psi_v, state,
    vec_in, vec_out, vec_back, mat_out, mat_in, comp_out, comp_in, early_in, psi_out, psi_in,
    off_out, off_in, first_in, near_out, near_in, sum_buf, sum_in,
    vec_send, vec_recv, mat_sem, early_sem, comp_sem, psi_sem, near_sem, off_send, off_recv, first_sem, sum_sem,
):
    pos = lax.axis_index("tm")
    par = lax.rem(pos, 2)
    quarter = lax.rem(pos, 4)
    chip = lax.div(pos, 2)
    chips = n // 2
    states = dyn.shape[0]
    block = states + EXTRA
    chunks = steps // WORD
    total = seqs * chunks
    levels = int(math.log2(chunks))
    first = [0]
    for level in range(1, levels + 1):
        first.append(first[-1] + (total >> (level - 1) if level > 1 else 0))
    top = first[levels]

    loads = [
        pltpu.make_async_copy(src, dst, in_sem.at[k])
        for k, (src, dst) in enumerate([
            (dyn_h, dyn), (obs_map_h, obs_map), (log_prec_h, log_prec), (prior_var_h, prior_var),
            (present_h, present_s), (present_h, present_v), (obs_h, obs), (init_h, init),
        ])
    ]
    for copy in loads:
        copy.start()
    vec_in[...] = jnp.zeros_like(vec_in)
    off_in[...] = jnp.zeros_like(off_in)
    near_in[...] = jnp.zeros_like(near_in)
    first_in[...] = jnp.zeros_like(first_in)
    barrier = pltpu.get_barrier_semaphore()
    for d in range(1, n):
        pl.semaphore_signal(barrier, inc=1, device_id={"tm": lax.rem(pos + d, n)}, device_id_type=MESH)

    for copy in loads[:4]:
        copy.wait()
    lane = lax.broadcasted_iota(jnp.int32, (1, states), 1)
    row8 = lax.broadcasted_iota(jnp.int32, (8, states), 0)
    active = (lane < sensors_s[0]).astype(F32)
    weight = jnp.exp(log_prec[...])
    weight_on = weight * active
    pv = prior_var[...]
    d_mat = dyn[...]
    d_t = d_mat.T
    h_mat = obs_map[...]
    h_2 = split(h_mat)
    d_2n = split(d_mat)
    d_t2 = split(d_t)
    readout = wide(d_t2, deep(split(h_mat.T)))[0]
    gain = -(mul(readout * weight_on, h_2) * pv)
    f_t2 = split(d_t + gain)
    held[0] = d_2n
    held[4] = d_t2
    held[5] = split(gain)
    held[6] = split(readout)

    for copy in loads[4:]:
        copy.wait()
    for b in range(seqs):
        for k in range(chunks):
            t = k * WORD
            w = present_s[b, t]
            for i in range(1, WORD):
                w = w * 2 + present_s[b, t + i]
            words[b * chunks + k] = w
        row = jnp.broadcast_to(present_v[b : b + 1, :].astype(F32), (steps, steps))
        same = lax.broadcasted_iota(jnp.int32, (steps, steps), 0) == lax.broadcasted_iota(jnp.int32, (steps, steps), 1)
        column = jnp.sum(jnp.where(same, row, 0.0), axis=1, keepdims=True)
        mask[b * steps : (b + 1) * steps, :] = jnp.broadcast_to(column, (steps, states))

    drive[...] = mul(obs[...] * weight_on, h_2) * pv * mask[...]

    step_rhs[...] = stacked(jnp.concatenate([d_t, gain], axis=1))
    singles = [d_t2, f_t2]
    both = deep(jnp.concatenate(singles, axis=1))
    pairs = []
    for a in range(2):
        pairs += [split(q) for q in wide(singles[a], both)]
    for a in range(4):
        pair_2[a] = pairs[a]
    held[7] = f_t2
    quad_rhs = deep(jnp.concatenate(pairs, axis=1))
    for a in range(4):
        quad = wide(pairs[a], quad_rhs)
        for c in range(4):
            table[a * 4 + c] = split(quad[c])

    def at(ref, i):
        return ref[pl.ds(i, total, stride=WORD), :]

    def advance(x, i):
        y = times(x, step_rhs[...])
        move = jnp.where(at(mask, i) > 0.5, y[:, states:], 0.0) + at(drive, i)
        return y[:, :states] + move, move

    x = at(drive, 0)
    moves[0:total, :] = x
    for i in range(1, WORD):
        x, move = advance(x, i)
        moves[i * total : (i + 1) * total, :] = move
        if i == 1:
            zero_2[...] = x
    offs[...] = x

    def combine(moved, first):
        left = jnp.concatenate([twice(stacked(moved[j * total : (j + 1) * total, :])) for j in range(first + 1, WORD)], axis=1)
        return product(left, jnp.concatenate([tall(held[j]) for j in range(WORD - 1 - first)], axis=0))

    def leading(matrix, v):
        return jnp.concatenate([matrix, split(jnp.broadcast_to(v, (16, states)))], axis=0)

    def child(level, j):
        if level == 1:
            return table[words[j]], offs[j : j + 1, :]
        j = first[level - 1] + j
        return nodes[j], vecs[j : j + 1, :]

    for level in range(1, levels + 1):
        for j in range(total >> level):
            left, v_left = child(level, 2 * j)
            right, v_right = child(level, 2 * j + 1)
            y = wide(leading(left, v_left), deep(right))[0]
            j = first[level] + j
            v = y[states : states + EXTRA] + v_right
            nodes[j] = split(y[:states])
            vecs[j : j + 1, :] = v[0:1]
            if level == levels:
                b = j - top
                mat_out[b * block : b * block + states, :] = y[:states]
                mat_out[b * block + states : (b + 1) * block, :] = v

    def lefts(x):
        return jnp.concatenate([twice(stacked(jnp.where(row8 == b, x, 0.0))) for b in range(seqs)], axis=1)

    def apply(left, node, v):
        rhs = jnp.concatenate([tall(node[b]) for b in range(seqs)], axis=0)
        return product(left, rhs) + v

    def rows_of(ref):
        v = jnp.zeros((8, states), F32)
        for b in range(seqs):
            v = jnp.where(row8 == b, ref[b * block + states : (b + 1) * block, :], v)
        return v

    own = nodes.at[pl.ds(top, seqs)]

    def own_v():
        v = jnp.zeros((8, states), F32)
        for b in range(seqs):
            v = jnp.where(row8 == b, vecs[top + b : top + b + 1, :], v)
        return v

    def send_vec(src, slot, to):
        return pltpu.make_async_remote_copy(
            src_ref=src, dst_ref=vec_in, send_sem=vec_send.at[slot // 3], recv_sem=vec_recv,
            device_id={"tm": to}, device_id_type=MESH,
        )

    def shift(by):
        return lax.rem(pos + (by + n), n)

    def send_mat(src, dst, sem, by):
        return pltpu.make_async_remote_copy(
            src_ref=src, dst_ref=dst, send_sem=sem.at[0], recv_sem=sem.at[1],
            device_id={"tm": shift(by)}, device_id_type=MESH,
        )

    def arrived(ref, sem):
        pltpu.make_async_copy(ref, ref, sem).wait()

    def send_part(src, dst, sem, by, b):
        rows = pl.ds(b * block, block)
        return pltpu.make_async_remote_copy(
            src_ref=src.at[rows], dst_ref=dst.at[rows], send_sem=sem.at[0], recv_sem=sem.at[1 + (b if by == 1 else 0)],
            device_id={"tm": shift(by)}, device_id_type=MESH,
        )

    def send_early(slot, by):
        return pltpu.make_async_remote_copy(
            src_ref=mat_out.at[pl.ds(0, block)], dst_ref=early_in.at[pl.ds(slot * block, block)],
            send_sem=early_sem.at[0], recv_sem=early_sem.at[1 + slot],
            device_id={"tm": shift(by)}, device_id_type=MESH,
        )

    early = [send_early(0, 3), send_early(1, 2)]
    order = list(range(1, seqs)) + [0]
    mats = [send_part(mat_out, mat_in, mat_sem, 1, b) for b in range(seqs)]
    comps = [None] + [send_part(comp_out, comp_in, comp_sem, 2, b) for b in range(1, seqs)]
    psi = send_mat(psi_out, psi_in, psi_sem, 1)
    near = send_mat(near_out, near_in, near_sem, -1)
    to_next = [send_vec(vec_out, k, shift(by)) for k, by in enumerate((2, 4, 1))]
    to_back = send_vec(vec_back, 3, shift(-1))

    even = par == 0
    odd = par == 1
    has_mat = jnp.logical_and(odd, pos >= 2)
    gives_mat = jnp.logical_and(even, pos >= 2)
    gives_comp = jnp.logical_and(quarter == 1, pos >= 4)
    has_comp = jnp.logical_and(quarter == 3, pos >= 4)
    last_of_four = jnp.logical_and(quarter == 3, pos < n - 1)

    pl.semaphore_wait(barrier, n - 1)

    @pl.when(gives_mat)
    def _():
        for b in order:
            mats[b].start()

        @pl.when(quarter == 0)
        def _():
            early[0].start()

    @pl.when(gives_comp)
    def _():
        early[1].start()

    @pl.when(pos == 0)
    def _():
        vec_in[0:seqs, :] = init[...]
        vec_out[...] = apply(lefts(vec_in[...]), own, own_v())
        to_next[2].start()

    near_4 = pos < 4
    far = pos >= 4

    base = held[0]
    held[1] = mul_node(base, base)
    square = held[1]
    held[2] = mul_node(base, square)
    held[3] = mul_node(square, square)
    powers[1] = held[3]
    rhs = deep(mul_node(held[5], base))
    change = held[5]
    change = change[:, :states].astype(F32) + change[:, states:].astype(F32)
    parts = [wide(held[4], rhs)[0], change, change + wide(held[7], rhs)[0]]
    for a in range(3):
        theta_2[a] = parts[a]
        theta_d[:, 2 * a * states : 2 * (a + 1) * states] = split(mul(parts[a], square))

    @pl.when(pos == 1)
    def _():
        to_back.wait_recv()
        vec_out[...] = apply(lefts(vec_in[...]), own, own_v())
        to_next[0].start()
        to_next[2].start()

    def pair(b):
        left = split(mat_in[b * block : b * block + states, :])
        even_node[b] = left
        v_left = mat_in[b * block + states : b * block + states + 1, :]
        y = wide(leading(left, v_left), deep(nodes[top + b]))[0]
        pair_node[b] = split(y[:states])
        comp_out[b * block : b * block + states, :] = y[:states]
        comp_out[b * block + states : (b + 1) * block, :] = y[states : states + EXTRA] + vecs[top + b : top + b + 1, :]

    def tables():
        fourth = held[3]
        u = moves[0:total, :] + combine(moves, 0)
        u_rows[...] = u
        u_4[...] = times(u, tall(fourth))
        rhs = deep(theta_d[...])
        whole = jnp.zeros((states, states), F32)
        theta[0] = jnp.zeros_like(whole)
        theta_4[0] = split(jnp.zeros_like(whole))
        for a in range(4):
            full = [None] + wide(pair_2[a], rhs)
            for c in range(4):
                if a + c > 0:
                    parts = [q for q in (theta_2[a - 1] if a > 0 else None, full[c]) if q is not None]
                    whole = sum(parts[1:], parts[0])
                    theta[a * 4 + c] = whole
                    theta_4[a * 4 + c] = split(mul(whole, fourth))

    @pl.when(jnp.logical_and(far, jnp.logical_not(gives_comp)))
    def _():
        tables()

    @pl.when(gives_comp)
    def _():
        for b in order:
            mats[b].wait_recv()
            if b > 0:
                pair(b)
                comps[b].start()
            else:
                even_node[b] = split(mat_in[b * block : b * block + states, :])
        even_v[...] = rows_of(mat_in)

    @pl.when(gives_comp)
    def _():
        tables()

    @pl.when(jnp.logical_and(has_mat, jnp.logical_not(gives_comp)))
    def _():
        for b in range(seqs):
            mats[b].wait_recv()
        for b in range(seqs):
            pair(b)
        even_v[...] = rows_of(mat_in)
        pair_v[...] = rows_of(comp_out)

    def double(level):
        half = 1 << (level - 1)
        powers[2 * half] = mul_node(powers[half], powers[half])

    def fill():
        powers[0] = split(
            (
                lax.broadcasted_iota(jnp.int32, (states, states), 0)
                == lax.broadcasted_iota(jnp.int32, (states, states), 1)
            ).astype(F32)
        )
        for level in range(1, levels):
            base = powers[1 << level]
            for e in range(1, 1 << level):
                powers[(1 << level) + e] = mul_node(powers[e], base)
        laps[0] = powers[0]
        laps[1] = powers[chunks]
        for m in range(2, 2 * chips - 2):
            laps[m] = mul_node(laps[m // 2], laps[m - m // 2])

    @pl.when(pos == 3)
    def _():
        to_back.wait_recv()
        vec_out[...] = apply(lefts(vec_in[...]), pair_node, pair_v[...])

        @pl.when(pos < n - 1)
        def _():
            for copy in to_next:
                copy.start()

    @pl.when(near_4)
    def _():
        for level in range(1, levels + 1):
            double(level)

    def prepare():
        for b in range(seqs):
            for level in range(levels, 0, -1):
                for p in range(chunks >> level):
                    mat_2, v = child(level, (b * (chunks >> level) + p) * 2)
                    k = (p << level) + (1 << (level - 1))
                    if p > 0:
                        before = b * chunks + (p << level)
                        lead = leading(heads[before], head_vecs[before : before + 1, :])
                        y = wide(lead, deep(mat_2))[0]
                        mat_2 = split(y[:states])
                        v = y[states : states + 1] + v
                    heads[b * chunks + k] = mat_2
                    head_vecs[b * chunks + k : b * chunks + k + 1, :] = v

    def compose(first_level, last_level):
        for level in range(first_level, last_level + 1):
            lag = powers[1 << (level - 1)]
            double(level)
            for j in range(total >> level):
                left, v_left = child(level, 2 * j)
                lead = leading(left, v_left)
                a, b = 2 * j, 2 * j + 1
                if level == 1:
                    y = wide(lead, deep(theta_4[words[b]]))[0]
                    whole = theta[words[a]] + y[:states]
                    u = y[states : states + EXTRA] + u_4[b : b + 1, :] + u_rows[a : a + 1, :]
                else:
                    a, b = first[level - 1] + a, first[level - 1] + b
                    y = wide(lead, deep(psi_n[b]))[0]
                    y = jnp.concatenate([y[:states], y[states:] + us[b : b + 1, :]], axis=0)
                    y = mul(y, lag)
                    whole = psi_f[a] + y[:states]
                    u = y[states : states + EXTRA] + us[a : a + 1, :]
                k = first[level] + j
                if level == levels:
                    psi_out[j * block : j * block + states, :] = whole
                    psi_out[j * block + states : (j + 1) * block, :] = u
                else:
                    us[k : k + 1, :] = u[0:1]
                    if j % 2 == 0:
                        psi_f[k] = whole
                    else:
                        psi_n[k] = split(whole)

    @pl.when(far)
    def _():
        compose(1, levels - 1)

    @pl.when(jnp.logical_and(far, jnp.logical_not(has_comp)))
    def _():
        compose(levels, levels)

    @pl.when(has_comp)
    def _():
        for copy in early:
            copy.wait_recv()
        v_left = early_in[states : states + 1, :]
        y = wide(leading(split(early_in[0:states, :]), v_left), deep(split(early_in[block : block + states, :])))[0]
        comp_in[0:states, :] = y[:states]
        comp_in[states:block, :] = y[states : states + EXTRA] + early_in[block + states : 2 * block, :]
        compose(levels, levels)

    @pl.when(jnp.logical_and(gives_mat, far))
    def _():
        psi.start()

    direct = jnp.logical_and(odd, far)

    headed = jnp.logical_and(even, far)

    @pl.when(headed)
    def _():
        prepare()

    def send_off(d, side):
        return pltpu.make_async_remote_copy(
            src_ref=off_out, dst_ref=off_in.at[d - 1], send_sem=off_send.at[d - 1], recv_sem=off_recv.at[d - 1],
            device_id={"tm": lax.rem(2 * (chip + chips - d) + side, n)}, device_id_type=MESH,
        )

    rest = pl.ds(block, (seqs - 1) * block)

    def sweep(x):
        entering = [jnp.broadcast_to(x[b : b + 1], (8, states)) for b in range(seqs)]
        for level in range(levels, 0, -1):
            below = []
            for j in range(total >> level):
                node, v = child(level, 2 * j)
                below.append(entering[j])
                below.append(times(entering[j], tall(node)) + v)
            entering = below
        for j in range(total):
            ents[j : j + 1, :] = entering[j][0:1]

    @pl.when(has_comp)
    def _():
        to_back.wait_recv()
        arrived(comp_in.at[rest], comp_sem.at[1])
        for b in range(seqs):
            prev_node[b] = split(comp_in[b * block : b * block + states, :])
        prev_v[...] = rows_of(comp_in)
        back = apply(lefts(vec_in[...]), prev_node, prev_v[...])
        vec_back[...] = back
        to_back.start()
        vec_in[...] = back
        x = apply(lefts(back), even_node, even_v[...])
        state[...] = x
        sweep(x)

    @pl.when(far)
    def _():
        for b in range(seqs):
            psi_own[b] = split(psi_out[b * block : b * block + states, :])
        psi_v[...] = rows_of(psi_out)

    @pl.when(jnp.logical_and(odd, far))
    def _():
        lap = powers[chunks]
        for b in range(seqs):
            v_left = mat_in[b * block + states : b * block + states + 1, :]
            y = wide(leading(even_node[b], v_left), deep(psi_own[b]))[0]
            u = psi_out[b * block + states : b * block + states + 1, :]
            y = jnp.concatenate([y[:states], y[states:] + u], axis=0)
            later[b * block : (b + 1) * block, :] = mul(y, lap)[:block]

    @pl.when(direct)
    def _():
        psi.wait_recv()
        for b in range(seqs):
            psi_in[b * block : (b + 1) * block, :] += later[b * block : (b + 1) * block, :]
            omega_node[b] = split(psi_in[b * block : b * block + states, :])
        omega_v[...] = rows_of(psi_in)

    @pl.when(jnp.logical_and(jnp.logical_or(pos == 2, pos >= 4), jnp.logical_not(has_comp)))
    def _():
        to_back.wait_recv()

    @pl.when(jnp.logical_not(has_comp))
    def _():
        state[...] = vec_in[...]

    @pl.when(jnp.logical_and(has_comp, pos < n - 1))
    def _():
        vec_out[...] = apply(lefts(vec_in[...]), pair_node, pair_v[...])
        for copy in to_next:
            copy.start()

    @pl.when(jnp.logical_and(odd, far))
    def _():
        left = lefts(vec_in[...])
        off_out[...] = apply(left, omega_node, omega_v[...])
        for d in range(chips - 1, 0, -1):
            @pl.when(chip - d >= 0)
            def _(d=d):
                send_off(d, 1).start()
                send_off(d, 0).start()
        x = apply(left, even_node, even_v[...])
        state[...] = x
        near_out[...] = apply(lefts(x), psi_own, psi_v[...])
        near.start()

    @pl.when(pos == 3)
    def _():
        state[...] = apply(lefts(state[...]), even_node, even_v[...])

    def send_sum(d):
        return pltpu.make_async_remote_copy(
            src_ref=sum_buf, dst_ref=sum_in.at[d], send_sem=sum_sem.at[0], recv_sem=sum_sem.at[1],
            device_id={"tm": lax.rem(pos + d + 1, n)}, device_id_type=MESH,
        )

    def score(priors):
        squares = jnp.zeros((total, states), F32)
        seen = jnp.zeros((total, states), F32)
        for i in range(WORD):
            error = at(obs, i) - mul(priors[i], held[6])
            squares = squares + at(mask, i) * error * error
            seen = seen + at(mask, i)
        squares = active * jnp.sum(squares, axis=0, keepdims=True)
        number = jnp.sum(seen, axis=0, keepdims=True)
        sum_buf[...] = jnp.where(row8 == 0, jnp.broadcast_to(squares, (8, states)), jnp.broadcast_to(number, (8, states)))
        for e in range(1, n):
            @pl.when(pos + e >= n)
            def _(e=e):
                send_sum(e - 1).start()

        for e in range(n - 1, 0, -1):
            @pl.when(pos + e < n)
            def _(e=e):
                send_sum(e - 1).start()

    def quick():
        start = ents[...]
        y = times(start, jnp.concatenate([step_rhs[...]] + [tall(pair_2[a]) for a in range(4)], axis=1))
        y = [y[:, k * states : (k + 1) * states] for k in range(6)]
        on = [at(mask, i) > 0.5 for i in range(2)]
        one = y[0] + jnp.where(on[0], y[1], 0.0) + at(drive, 0)
        two = jnp.where(on[0], jnp.where(on[1], y[5], y[4]), jnp.where(on[1], y[3], y[2])) + zero_2[...]
        score([start, one, two, advance(two, 2)[0]])

    def priors_held():
        return [prior[i * total : (i + 1) * total, :] for i in range(WORD)]

    @pl.when(headed)
    def _():
        x = state[...]
        spread = jnp.concatenate([jnp.concatenate([tall(heads[b * chunks + k]) for k in range(1, chunks)], axis=1) for b in range(seqs)], axis=0)
        y = product(lefts(x), spread)
        for b in range(seqs):
            ents[b * chunks : b * chunks + 1, :] = x[b : b + 1]
            for k in range(1, chunks):
                r = b * chunks + k
                ents[r : r + 1, :] = y[b : b + 1, (k - 1) * states : k * states] + head_vecs[r : r + 1, :]
        quick()

    @pl.when(jnp.logical_not(jnp.logical_or(headed, has_comp)))
    def _():
        sweep(state[...])

    @pl.when(direct)
    def _():
        quick()

    x = ents[...]
    for i in range(WORD):
        prior[i * total : (i + 1) * total, :] = x
        x, move = advance(x, i)
        filt[i * total : (i + 1) * total, :] = x
        moves[i * total : (i + 1) * total, :] = move

    chunk8[...] = jnp.zeros_like(chunk8)
    for i in range(WORD - 1):
        z = combine(moves, i)
        suffix[i * total : (i + 1) * total, :] = filt[i * total : (i + 1) * total, :] + z
        if i == 0:
            z = z + moves[0:total, :]
            for b in range(seqs):
                chunk8[pl.ds(b, chunks, stride=8), :] = z[b * chunks : (b + 1) * chunks]
    i = WORD - 1
    suffix[i * total : (i + 1) * total, :] = filt[i * total : (i + 1) * total, :]
    ends = chunk8[...].reshape(chunks, 8, states)

    ups = [ends]
    for level in range(levels):
        pair = ups[-1].reshape(ups[-1].shape[0] // 2, 2, 8, states)
        half = pair.shape[0]
        later = times(pair[:, 1].reshape(half * 8, states), tall(powers[1 << level]))
        ups.append(pair[:, 0] + later.reshape(half, 8, states))

    def send_first(slot, side):
        dst = off_in.at[0] if slot == 0 else first_in
        return pltpu.make_async_remote_copy(
            src_ref=off_out, dst_ref=dst, send_sem=off_send.at[0],
            recv_sem=off_recv.at[0] if slot == 0 else first_sem,
            device_id={"tm": side}, device_id_type=MESH,
        )

    @pl.when(near_4)
    def _():
        off_out[...] = ups[-1].reshape(8, states)
        near_out[...] = ups[-1].reshape(8, states)
        for slot in range(2):
            @pl.when(pos == 2 + slot)
            def _(slot=slot):
                send_first(slot, 0).start()
                send_first(slot, 1).start()

        @pl.when(odd)
        def _():
            near.start()

        score(priors_held())

    x = jnp.zeros((1, 8, states), F32)
    for level in range(levels - 1, -1, -1):
        count = x.shape[0]
        pair = ups[level].reshape(count, 2, 8, states)
        if level == levels - 1:
            sooner = pair[:, 1]
        else:
            moved = times(x.reshape(count * 8, states), tall(powers[1 << level]))
            sooner = moved.reshape(count, 8, states) + pair[:, 1]
        x = jnp.stack([sooner, x], axis=1).reshape(2 * count, 8, states)
    chunk8[...] = x.reshape(chunks * 8, states)
    fill()

    @pl.when(even)
    def _():
        near.wait_recv()

    @pl.when(chip == 0)
    def _():
        send_first(1, 0).wait_recv()

    for d in range(1, chips):
        @pl.when(chip + d < chips)
        def _(d=d):
            send_off(d, 0).wait_recv()

    left = jnp.concatenate([twice(stacked(a)) for a in [first_in[...]] + [off_in[d] for d in range(chips - 1)]], axis=1)
    rhs = jnp.concatenate([tall(laps[2 - par])] + [tall(laps[2 * d + 1 - par]) for d in range(chips - 1)], axis=0)
    x = near_in[...] + product(left, rhs)
    y = times(x, jnp.concatenate([tall(powers[chunks - 1 - k]) for k in range(chunks)], axis=1))
    for k in range(chunks):
        chunk8[k * 8 : (k + 1) * 8, :] += y[:, k * states : (k + 1) * states]
    x = jnp.concatenate([chunk8[pl.ds(b, chunks, stride=8), :] for b in range(seqs)], axis=0)
    y = times(x, jnp.concatenate([tall(a) for a in (held[3], held[2], held[1], held[0])], axis=1))
    for i in range(WORD):
        out[pl.ds(i, total, stride=WORD), :] = (
            suffix[i * total : (i + 1) * total, :] + y[:, i * states : (i + 1) * states]
        )

    @pl.when(gives_mat)
    def _():
        arrived(mat_out, mat_sem.at[0])

        @pl.when(quarter == 0)
        def _():
            arrived(mat_out.at[pl.ds(0, block)], early_sem.at[0])

    @pl.when(jnp.logical_and(gives_mat, far))
    def _():
        psi.wait_send()

    @pl.when(gives_comp)
    def _():
        arrived(comp_out.at[rest], comp_sem.at[0])
        arrived(mat_out.at[pl.ds(0, block)], early_sem.at[0])

    @pl.when(pos == 0)
    def _():
        to_next[2].wait_send()

    @pl.when(pos == 1)
    def _():
        arrived(off_in.at[pl.ds(0, 2)], vec_send.at[0])

    @pl.when(last_of_four)
    def _():
        arrived(off_in.at[pl.ds(0, 3)], vec_send.at[0])

    @pl.when(has_comp)
    def _():
        to_back.wait_send()

    @pl.when(odd)
    def _():
        near.wait_send()

    for d in range(1, chips):
        @pl.when(jnp.logical_and(jnp.logical_and(odd, far), chip - d >= 0))
        def _(d=d):
            arrived(off_in.at[pl.ds(0, 2)], off_send.at[d - 1])

    for slot in range(2):
        @pl.when(pos == 2 + slot)
        def _(slot=slot):
            arrived(off_in.at[pl.ds(0, 2)], off_send.at[0])

    arrived(sum_in.at[pl.ds(0, n - 1)], sum_sem.at[0])

    arrived(sum_in.at[pl.ds(0, n - 1)], sum_sem.at[1])
    sums = sum_buf[...]
    for d in range(n - 1):
        sums = sums + sum_in[d]
    squares, number = sums[0:1], sums[1:2]
    grad = 0.5 * active * (number - weight * squares)
    new_prec[...] = log_prec[...] + grad / (seqs * steps * n)
    terms = 0.5 * active * (log_prec[...] * number - weight * squares)
    loglik[...] = jnp.zeros_like(terms) + jnp.sum(terms, axis=1, keepdims=True) / (seqs * steps * n * states)


def mul_node(left, right):
    return split(wide(left, deep(right))[0])


def finish(smoothed, new_prec, loglik, out, out_prec, out_loglik):
    out[...] = smoothed[...]
    out_prec[...] = new_prec[...]
    out_loglik[...] = loglik[:, 0:1]


def local(n, obs, present, sensors, log_prec, dynamics, prior_var, obs_map, init_state):
    seqs, steps, channels = obs.shape
    states = dynamics.shape[0]
    assert n % 4 == 0 and states == 128 and channels == 128
    chunks = steps // WORD
    total = seqs * chunks
    chips = n // 2
    inner = sum(total >> level for level in range(1, int(math.log2(chunks)) + 1))
    vmem = pl.BlockSpec(memory_space=pltpu.VMEM)
    smem = pl.BlockSpec(memory_space=pltpu.SMEM)
    hbm = pl.BlockSpec(memory_space=pl.ANY)
    rows = seqs * steps
    block = seqs * (states + EXTRA)
    node = (states, 2 * states)
    tile = pltpu.VMEM((8, states), F32)
    whole = pltpu.VMEM((block, states), F32)
    level_rows = (inner + 7) // 8 * 8
    dma = pltpu.SemaphoreType.DMA
    smoothed, new_prec, loglik = pl.pallas_call(
        functools.partial(kernel, n, seqs, steps),
        out_shape=(
            pltpu.VMEM((rows, states), F32),
            pltpu.VMEM((1, channels), F32),
            pltpu.VMEM((1, channels), F32),
        ),
        in_specs=[hbm, smem] + [hbm] * 6,
        out_specs=(vmem, vmem, vmem),
        scratch_shapes=[
            pltpu.VMEM((states, states), F32),
            pltpu.VMEM((channels, states), F32),
            pltpu.VMEM((1, channels), F32),
            pltpu.VMEM((1, states), F32),
            pltpu.SMEM((seqs, steps), jnp.int32),
            pltpu.VMEM((seqs, steps), jnp.int32),
            pltpu.VMEM((rows, channels), F32),
            pltpu.VMEM((seqs, states), F32),
            dma((8,)),
            pltpu.SMEM((total,), jnp.int32),
            pltpu.VMEM((2**WORD,) + node, BF16),
            pltpu.VMEM((2**WORD, states, states), F32),
            pltpu.VMEM((2**WORD,) + node, BF16),
            pltpu.VMEM((inner,) + node, BF16),
            pltpu.VMEM((level_rows, states), F32),
            pltpu.VMEM((inner, states, states), F32),
            pltpu.VMEM((inner,) + node, BF16),
            pltpu.VMEM((level_rows, states), F32),
            pltpu.VMEM((total, states), F32),
            pltpu.VMEM((total, states), F32),
            pltpu.VMEM((total, states), F32),
            pltpu.VMEM((total, states), F32),
            pltpu.VMEM((chunks + 1,) + node, BF16),
            pltpu.VMEM((2 * chips - 2,) + node, BF16),
            pltpu.VMEM((2 * states, 2 * states), BF16),
            pltpu.VMEM((rows, states), F32),
            pltpu.VMEM((rows, states), F32),
            pltpu.VMEM((rows, states), F32),
            pltpu.VMEM((rows, states), F32),
            pltpu.VMEM((rows, states), F32),
            pltpu.VMEM((chunks * 8, states), F32),
            pltpu.VMEM((rows, states), F32),
            pltpu.VMEM((8,) + node, BF16),
            pltpu.VMEM((4,) + node, BF16),
            pltpu.VMEM((total, states), F32),
            pltpu.VMEM((3, states, states), F32),
            pltpu.VMEM((states, 6 * states), BF16),
            whole,
            pltpu.VMEM((total,) + node, BF16),
            pltpu.VMEM((total, states), F32),
            pltpu.VMEM((seqs,) + node, BF16), tile,
            pltpu.VMEM((seqs,) + node, BF16), tile,
            pltpu.VMEM((seqs,) + node, BF16), tile,
            pltpu.VMEM((seqs,) + node, BF16), tile,
            pltpu.VMEM((seqs,) + node, BF16), tile,
            tile,
            tile, tile, tile, whole, whole, whole, whole, pltpu.VMEM((2 * (states + EXTRA), states), F32), whole, whole,
            tile, pltpu.VMEM((chips - 1, 8, states), F32), tile, tile, tile, tile, pltpu.VMEM((n, 8, states), F32),
            dma((2,)), dma(()), dma((1 + seqs,)), dma((3,)), dma((2,)), dma((2,)), dma((2,)),
            dma((chips - 1,)), dma((chips - 1,)), dma(()), dma((2,)),
        ],
        compiler_params=pltpu.CompilerParams(collective_id=0, has_side_effects=True),
        name="kalman",
    )(
        present, sensors, obs.reshape(rows, channels), log_prec.reshape(1, channels),
        dynamics, prior_var.reshape(1, states), obs_map, init_state,
    )
    held = [pltpu.with_memory_space_constraint(a, pltpu.VMEM) for a in (smoothed, new_prec, loglik)]
    smoothed, new_prec, loglik = pl.pallas_call(
        finish,
        out_shape=(
            jax.ShapeDtypeStruct((rows, states), F32),
            jax.ShapeDtypeStruct((1, channels), F32),
            jax.ShapeDtypeStruct((1, 1), F32),
        ),
        in_specs=[vmem] * 3,
        out_specs=(vmem, vmem, vmem),
        name="finish",
    )(*held)
    return smoothed.reshape(seqs, steps, states), new_prec.reshape(channels), loglik.reshape(1)


def solution(mesh):
    in_specs = (
        P("cluster", "tm", None),
        P("cluster", "tm"),
        P("cluster"),
        P("cluster"),
        P("cluster", None),
        P("cluster"),
        P("cluster", None),
        P("cluster", None),
    )
    out_specs = (P("cluster", "tm", None), P("cluster"), P("cluster"))
    body = functools.partial(local, mesh.shape["tm"])
    return jax.shard_map(body, mesh=mesh, in_specs=in_specs, out_specs=out_specs, check_vma=False)
```

```python
import functools
import math

import jax
import jax.numpy as jnp
from jax import lax
from jax.experimental import pallas as pl
from jax.experimental.pallas import tpu as pltpu
from jax.sharding import PartitionSpec as P

F32 = jnp.float32
BF16 = jnp.bfloat16
MESH = pl.DeviceIdType.MESH
WORD = 4
EXTRA = 8


def split(a):
    high = a.astype(BF16).astype(F32)
    return jnp.concatenate([high, a - high], axis=1).astype(BF16)


def stacked(a):
    high = a.astype(BF16).astype(F32)
    return jnp.concatenate([high, a - high], axis=0).astype(BF16)


def deep(node):
    return jnp.concatenate([node, node], axis=0)


def tall(node):
    width = node.shape[1] // 2
    return jnp.concatenate([node[:, :width], node[:, width:]], axis=0)


def twice(s):
    return jnp.concatenate([s, s], axis=1)


def product(left, right):
    full = jnp.dot(left, right, preferred_element_type=F32)
    rows = full.shape[0] // 2
    return full[:rows] + full[rows:]


def times(a, right):
    return product(twice(stacked(a)), right)


def wide(left, right):
    full = jnp.dot(left, right, preferred_element_type=F32)
    half = left.shape[1] // 2 if left.shape[1] < 256 else 128
    return [
        full[:, 2 * k * half : (2 * k + 1) * half] + full[:, (2 * k + 1) * half : (2 * k + 2) * half]
        for k in range(full.shape[1] // (2 * half))
    ]


def mul(a, node):
    return wide(split(a), deep(node))[0]


def kernel(
    n, seqs, steps,
    present_h, sensors_s, obs_h, log_prec_h, dyn_h, prior_var_h, obs_map_h, init_h,
    out, new_prec, loglik,
    dyn, obs_map, log_prec, prior_var, present_s, present_v, obs, init, in_sem,
    words, table, theta, theta_4, nodes, vecs, psi_f, psi_n, us, offs, u_rows, u_4, ents, powers, laps, step_rhs,
    drive, mask, prior, filt, suffix, chunk8, moves, held, pair_2, zero_2, theta_2, theta_d, later, heads, head_vecs,
    even_node, even_v, pair_node, pair_v, prev_node, prev_v, omega_node, omega_v, psi_own, psi_v, state,
    vec_in, vec_out, vec_back, mat_out, mat_in, comp_out, comp_in, early_in, psi_out, psi_in,
    off_out, off_in, first_in, near_out, near_in, sum_buf, sum_in,
    vec_send, vec_recv, mat_sem, early_sem, comp_sem, psi_sem, near_sem, off_send, off_recv, first_sem, sum_sem,
):
    pos = lax.axis_index("tm")
    par = lax.rem(pos, 2)
    quarter = lax.rem(pos, 4)
    chip = lax.div(pos, 2)
    chips = n // 2
    states = dyn.shape[0]
    block = states + EXTRA
    chunks = steps // WORD
    total = seqs * chunks
    levels = int(math.log2(chunks))
    first = [0]
    for level in range(1, levels + 1):
        first.append(first[-1] + (total >> (level - 1) if level > 1 else 0))
    top = first[levels]

    loads = [
        pltpu.make_async_copy(src, dst, in_sem.at[k])
        for k, (src, dst) in enumerate([
            (dyn_h, dyn), (obs_map_h, obs_map), (log_prec_h, log_prec), (prior_var_h, prior_var),
            (present_h, present_s), (present_h, present_v), (obs_h, obs), (init_h, init),
        ])
    ]
    for copy in loads:
        copy.start()
    vec_in[...] = jnp.zeros_like(vec_in)
    off_in[...] = jnp.zeros_like(off_in)
    near_in[...] = jnp.zeros_like(near_in)
    first_in[...] = jnp.zeros_like(first_in)
    barrier = pltpu.get_barrier_semaphore()
    for d in range(1, n):
        pl.semaphore_signal(barrier, inc=1, device_id={"tm": lax.rem(pos + d, n)}, device_id_type=MESH)

    for copy in loads:
        copy.wait()
    lane = lax.broadcasted_iota(jnp.int32, (1, states), 1)
    row8 = lax.broadcasted_iota(jnp.int32, (8, states), 0)
    active = (lane < sensors_s[0]).astype(F32)
    weight = jnp.exp(log_prec[...])
    weight_on = weight * active
    pv = prior_var[...]
    d_mat = dyn[...]
    d_t = d_mat.T
    h_mat = obs_map[...]
    h_2 = split(h_mat)
    d_2n = split(d_mat)
    d_t2 = split(d_t)
    readout = wide(d_t2, deep(split(h_mat.T)))[0]
    gain = -(mul(readout * weight_on, h_2) * pv)
    f_t2 = split(d_t + gain)
    held[0] = d_2n
    held[4] = d_t2
    held[5] = split(gain)
    held[6] = split(readout)

    for b in range(seqs):
        for k in range(chunks):
            t = k * WORD
            w = present_s[b, t]
            for i in range(1, WORD):
                w = w * 2 + present_s[b, t + i]
            words[b * chunks + k] = w
        row = jnp.broadcast_to(present_v[b : b + 1, :].astype(F32), (steps, steps))
        same = lax.broadcasted_iota(jnp.int32, (steps, steps), 0) == lax.broadcasted_iota(jnp.int32, (steps, steps), 1)
        column = jnp.sum(jnp.where(same, row, 0.0), axis=1, keepdims=True)
        mask[b * steps : (b + 1) * steps, :] = jnp.broadcast_to(column, (steps, states))

    drive[...] = mul(obs[...] * weight_on, h_2) * pv * mask[...]

    step_rhs[...] = stacked(jnp.concatenate([d_t, gain], axis=1))
    singles = [d_t2, f_t2]
    both = deep(jnp.concatenate(singles, axis=1))
    pairs = []
    for a in range(2):
        pairs += [split(q) for q in wide(singles[a], both)]
    for a in range(4):
        pair_2[a] = pairs[a]
    held[7] = f_t2
    quad_rhs = deep(jnp.concatenate(pairs, axis=1))
    for a in range(4):
        quad = wide(pairs[a], quad_rhs)
        for c in range(4):
            table[a * 4 + c] = split(quad[c])

    def at(ref, i):
        return ref[pl.ds(i, total, stride=WORD), :]

    def advance(x, i):
        y = times(x, step_rhs[...])
        move = jnp.where(at(mask, i) > 0.5, y[:, states:], 0.0) + at(drive, i)
        return y[:, :states] + move, move

    x = at(drive, 0)
    moves[0:total, :] = x
    for i in range(1, WORD):
        x, move = advance(x, i)
        moves[i * total : (i + 1) * total, :] = move
        if i == 1:
            zero_2[...] = x
    offs[...] = x

    def combine(moved, first):
        left = jnp.concatenate([twice(stacked(moved[j * total : (j + 1) * total, :])) for j in range(first + 1, WORD)], axis=1)
        return product(left, jnp.concatenate([tall(held[j]) for j in range(WORD - 1 - first)], axis=0))

    def leading(matrix, v):
        return jnp.concatenate([matrix, split(jnp.broadcast_to(v, (16, states)))], axis=0)

    def child(level, j):
        if level == 1:
            return table[words[j]], offs[j : j + 1, :]
        j = first[level - 1] + j
        return nodes[j], vecs[j : j + 1, :]

    for level in range(1, levels + 1):
        for j in range(total >> level):
            left, v_left = child(level, 2 * j)
            right, v_right = child(level, 2 * j + 1)
            y = wide(leading(left, v_left), deep(right))[0]
            j = first[level] + j
            v = y[states : states + EXTRA] + v_right
            nodes[j] = split(y[:states])
            vecs[j : j + 1, :] = v[0:1]
            if level == levels:
                b = j - top
                mat_out[b * block : b * block + states, :] = y[:states]
                mat_out[b * block + states : (b + 1) * block, :] = v

    def lefts(x):
        return jnp.concatenate([twice(stacked(jnp.where(row8 == b, x, 0.0))) for b in range(seqs)], axis=1)

    def apply(left, node, v):
        rhs = jnp.concatenate([tall(node[b]) for b in range(seqs)], axis=0)
        return product(left, rhs) + v

    def rows_of(ref):
        v = jnp.zeros((8, states), F32)
        for b in range(seqs):
            v = jnp.where(row8 == b, ref[b * block + states : (b + 1) * block, :], v)
        return v

    own = nodes.at[pl.ds(top, seqs)]

    def own_v():
        v = jnp.zeros((8, states), F32)
        for b in range(seqs):
            v = jnp.where(row8 == b, vecs[top + b : top + b + 1, :], v)
        return v

    def send_vec(src, slot, to):
        return pltpu.make_async_remote_copy(
            src_ref=src, dst_ref=vec_in, send_sem=vec_send.at[slot // 3], recv_sem=vec_recv,
            device_id={"tm": to}, device_id_type=MESH,
        )

    def shift(by):
        return lax.rem(pos + (by + n), n)

    def send_mat(src, dst, sem, by):
        return pltpu.make_async_remote_copy(
            src_ref=src, dst_ref=dst, send_sem=sem.at[0], recv_sem=sem.at[1],
            device_id={"tm": shift(by)}, device_id_type=MESH,
        )

    def arrived(ref, sem):
        pltpu.make_async_copy(ref, ref, sem).wait()

    def send_part(src, dst, sem, by, b):
        rows = pl.ds(b * block, block)
        return pltpu.make_async_remote_copy(
            src_ref=src.at[rows], dst_ref=dst.at[rows], send_sem=sem.at[0], recv_sem=sem.at[1 + (b if by == 1 else 0)],
            device_id={"tm": shift(by)}, device_id_type=MESH,
        )

    def send_early(slot, by):
        return pltpu.make_async_remote_copy(
            src_ref=mat_out.at[pl.ds(0, block)], dst_ref=early_in.at[pl.ds(slot * block, block)],
            send_sem=early_sem.at[0], recv_sem=early_sem.at[1 + slot],
            device_id={"tm": shift(by)}, device_id_type=MESH,
        )

    early = [send_early(0, 3), send_early(1, 2)]
    order = list(range(1, seqs)) + [0]
    mats = [send_part(mat_out, mat_in, mat_sem, 1, b) for b in range(seqs)]
    comps = [None] + [send_part(comp_out, comp_in, comp_sem, 2, b) for b in range(1, seqs)]
    psi = send_mat(psi_out, psi_in, psi_sem, 1)
    near = send_mat(near_out, near_in, near_sem, -1)
    to_next = [send_vec(vec_out, k, shift(by)) for k, by in enumerate((2, 4, 1))]
    to_back = send_vec(vec_back, 3, shift(-1))

    even = par == 0
    odd = par == 1
    has_mat = jnp.logical_and(odd, pos >= 2)
    gives_mat = jnp.logical_and(even, pos >= 2)
    gives_comp = jnp.logical_and(quarter == 1, pos >= 4)
    has_comp = jnp.logical_and(quarter == 3, pos >= 4)
    last_of_four = jnp.logical_and(quarter == 3, pos < n - 1)

    pl.semaphore_wait(barrier, n - 1)

    @pl.when(gives_mat)
    def _():
        for b in order:
            mats[b].start()

        @pl.when(quarter == 0)
        def _():
            early[0].start()

    @pl.when(gives_comp)
    def _():
        early[1].start()

    @pl.when(pos == 0)
    def _():
        vec_in[0:seqs, :] = init[...]
        vec_out[...] = apply(lefts(vec_in[...]), own, own_v())
        to_next[2].start()

    near_4 = pos < 4
    far = pos >= 4

    base = held[0]
    held[1] = mul_node(base, base)
    square = held[1]
    held[2] = mul_node(base, square)
    held[3] = mul_node(square, square)
    powers[1] = held[3]
    rhs = deep(mul_node(held[5], base))
    change = held[5]
    change = change[:, :states].astype(F32) + change[:, states:].astype(F32)
    parts = [wide(held[4], rhs)[0], change, change + wide(held[7], rhs)[0]]
    for a in range(3):
        theta_2[a] = parts[a]
        theta_d[:, 2 * a * states : 2 * (a + 1) * states] = split(mul(parts[a], square))

    @pl.when(pos == 1)
    def _():
        to_back.wait_recv()
        vec_out[...] = apply(lefts(vec_in[...]), own, own_v())
        to_next[0].start()
        to_next[2].start()

    def pair(b):
        left = split(mat_in[b * block : b * block + states, :])
        even_node[b] = left
        v_left = mat_in[b * block + states : b * block + states + 1, :]
        y = wide(leading(left, v_left), deep(nodes[top + b]))[0]
        pair_node[b] = split(y[:states])
        comp_out[b * block : b * block + states, :] = y[:states]
        comp_out[b * block + states : (b + 1) * block, :] = y[states : states + EXTRA] + vecs[top + b : top + b + 1, :]

    def tables():
        fourth = held[3]
        u = moves[0:total, :] + combine(moves, 0)
        u_rows[...] = u
        u_4[...] = times(u, tall(fourth))
        rhs = deep(theta_d[...])
        whole = jnp.zeros((states, states), F32)
        theta[0] = jnp.zeros_like(whole)
        theta_4[0] = split(jnp.zeros_like(whole))
        for a in range(4):
            full = [None] + wide(pair_2[a], rhs)
            for c in range(4):
                if a + c > 0:
                    parts = [q for q in (theta_2[a - 1] if a > 0 else None, full[c]) if q is not None]
                    whole = sum(parts[1:], parts[0])
                    theta[a * 4 + c] = whole
                    theta_4[a * 4 + c] = split(mul(whole, fourth))

    @pl.when(jnp.logical_and(far, jnp.logical_not(gives_comp)))
    def _():
        tables()

    @pl.when(gives_comp)
    def _():
        for b in order:
            mats[b].wait_recv()
            if b > 0:
                pair(b)
                comps[b].start()
            else:
                even_node[b] = split(mat_in[b * block : b * block + states, :])
        even_v[...] = rows_of(mat_in)

    @pl.when(gives_comp)
    def _():
        tables()

    @pl.when(jnp.logical_and(has_mat, jnp.logical_not(gives_comp)))
    def _():
        for b in range(seqs):
            mats[b].wait_recv()
        for b in range(seqs):
            pair(b)
        even_v[...] = rows_of(mat_in)
        pair_v[...] = rows_of(comp_out)

    def double(level):
        half = 1 << (level - 1)
        powers[2 * half] = mul_node(powers[half], powers[half])

    def fill():
        powers[0] = split(
            (
                lax.broadcasted_iota(jnp.int32, (states, states), 0)
                == lax.broadcasted_iota(jnp.int32, (states, states), 1)
            ).astype(F32)
        )
        for level in range(1, levels):
            base = powers[1 << level]
            for e in range(1, 1 << level):
                powers[(1 << level) + e] = mul_node(powers[e], base)
        laps[0] = powers[0]
        laps[1] = powers[chunks]
        for m in range(2, 2 * chips - 2):
            laps[m] = mul_node(laps[m // 2], laps[m - m // 2])

    @pl.when(pos == 3)
    def _():
        to_back.wait_recv()
        vec_out[...] = apply(lefts(vec_in[...]), pair_node, pair_v[...])

        @pl.when(pos < n - 1)
        def _():
            for copy in to_next:
                copy.start()

    @pl.when(near_4)
    def _():
        for level in range(1, levels + 1):
            double(level)

    def prepare():
        for b in range(seqs):
            for level in range(levels, 0, -1):
                for p in range(chunks >> level):
                    mat_2, v = child(level, (b * (chunks >> level) + p) * 2)
                    k = (p << level) + (1 << (level - 1))
                    if p > 0:
                        before = b * chunks + (p << level)
                        lead = leading(heads[before], head_vecs[before : before + 1, :])
                        y = wide(lead, deep(mat_2))[0]
                        mat_2 = split(y[:states])
                        v = y[states : states + 1] + v
                    heads[b * chunks + k] = mat_2
                    head_vecs[b * chunks + k : b * chunks + k + 1, :] = v

    def compose(first_level, last_level):
        for level in range(first_level, last_level + 1):
            lag = powers[1 << (level - 1)]
            double(level)
            for j in range(total >> level):
                left, v_left = child(level, 2 * j)
                lead = leading(left, v_left)
                a, b = 2 * j, 2 * j + 1
                if level == 1:
                    y = wide(lead, deep(theta_4[words[b]]))[0]
                    whole = theta[words[a]] + y[:states]
                    u = y[states : states + EXTRA] + u_4[b : b + 1, :] + u_rows[a : a + 1, :]
                else:
                    a, b = first[level - 1] + a, first[level - 1] + b
                    y = wide(lead, deep(psi_n[b]))[0]
                    y = jnp.concatenate([y[:states], y[states:] + us[b : b + 1, :]], axis=0)
                    y = mul(y, lag)
                    whole = psi_f[a] + y[:states]
                    u = y[states : states + EXTRA] + us[a : a + 1, :]
                k = first[level] + j
                if level == levels:
                    psi_out[j * block : j * block + states, :] = whole
                    psi_out[j * block + states : (j + 1) * block, :] = u
                else:
                    us[k : k + 1, :] = u[0:1]
                    if j % 2 == 0:
                        psi_f[k] = whole
                    else:
                        psi_n[k] = split(whole)

    @pl.when(far)
    def _():
        compose(1, levels - 1)

    @pl.when(jnp.logical_and(far, jnp.logical_not(has_comp)))
    def _():
        compose(levels, levels)

    @pl.when(has_comp)
    def _():
        for copy in early:
            copy.wait_recv()
        v_left = early_in[states : states + 1, :]
        y = wide(leading(split(early_in[0:states, :]), v_left), deep(split(early_in[block : block + states, :])))[0]
        comp_in[0:states, :] = y[:states]
        comp_in[states:block, :] = y[states : states + EXTRA] + early_in[block + states : 2 * block, :]
        compose(levels, levels)

    @pl.when(jnp.logical_and(gives_mat, far))
    def _():
        psi.start()

    direct = jnp.logical_and(odd, far)

    headed = jnp.logical_and(even, far)

    @pl.when(headed)
    def _():
        prepare()

    def send_off(d, side):
        return pltpu.make_async_remote_copy(
            src_ref=off_out, dst_ref=off_in.at[d - 1], send_sem=off_send.at[d - 1], recv_sem=off_recv.at[d - 1],
            device_id={"tm": lax.rem(2 * (chip + chips - d) + side, n)}, device_id_type=MESH,
        )

    rest = pl.ds(block, (seqs - 1) * block)

    def sweep(x):
        entering = [jnp.broadcast_to(x[b : b + 1], (8, states)) for b in range(seqs)]
        for level in range(levels, 0, -1):
            below = []
            for j in range(total >> level):
                node, v = child(level, 2 * j)
                below.append(entering[j])
                below.append(times(entering[j], tall(node)) + v)
            entering = below
        for j in range(total):
            ents[j : j + 1, :] = entering[j][0:1]

    @pl.when(has_comp)
    def _():
        to_back.wait_recv()
        arrived(comp_in.at[rest], comp_sem.at[1])
        for b in range(seqs):
            prev_node[b] = split(comp_in[b * block : b * block + states, :])
        prev_v[...] = rows_of(comp_in)
        back = apply(lefts(vec_in[...]), prev_node, prev_v[...])
        vec_back[...] = back
        to_back.start()
        vec_in[...] = back
        x = apply(lefts(back), even_node, even_v[...])
        state[...] = x
        sweep(x)

    @pl.when(far)
    def _():
        for b in range(seqs):
            psi_own[b] = split(psi_out[b * block : b * block + states, :])
        psi_v[...] = rows_of(psi_out)

    @pl.when(jnp.logical_and(odd, far))
    def _():
        lap = powers[chunks]
        for b in range(seqs):
            v_left = mat_in[b * block + states : b * block + states + 1, :]
            y = wide(leading(even_node[b], v_left), deep(psi_own[b]))[0]
            u = psi_out[b * block + states : b * block + states + 1, :]
            y = jnp.concatenate([y[:states], y[states:] + u], axis=0)
            later[b * block : (b + 1) * block, :] = mul(y, lap)[:block]

    @pl.when(direct)
    def _():
        psi.wait_recv()
        for b in range(seqs):
            psi_in[b * block : (b + 1) * block, :] += later[b * block : (b + 1) * block, :]
            omega_node[b] = split(psi_in[b * block : b * block + states, :])
        omega_v[...] = rows_of(psi_in)

    @pl.when(jnp.logical_and(jnp.logical_or(pos == 2, pos >= 4), jnp.logical_not(has_comp)))
    def _():
        to_back.wait_recv()

    @pl.when(jnp.logical_not(has_comp))
    def _():
        state[...] = vec_in[...]

    @pl.when(jnp.logical_and(has_comp, pos < n - 1))
    def _():
        vec_out[...] = apply(lefts(vec_in[...]), pair_node, pair_v[...])
        for copy in to_next:
            copy.start()

    @pl.when(jnp.logical_and(odd, far))
    def _():
        left = lefts(vec_in[...])
        off_out[...] = apply(left, omega_node, omega_v[...])
        for d in range(chips - 1, 0, -1):
            @pl.when(chip - d >= 0)
            def _(d=d):
                send_off(d, 1).start()
                send_off(d, 0).start()
        x = apply(left, even_node, even_v[...])
        state[...] = x
        near_out[...] = apply(lefts(x), psi_own, psi_v[...])
        near.start()

    @pl.when(pos == 3)
    def _():
        state[...] = apply(lefts(state[...]), even_node, even_v[...])

    def send_sum(d):
        return pltpu.make_async_remote_copy(
            src_ref=sum_buf, dst_ref=sum_in.at[d], send_sem=sum_sem.at[0], recv_sem=sum_sem.at[1],
            device_id={"tm": lax.rem(pos + d + 1, n)}, device_id_type=MESH,
        )

    def score(priors):
        squares = jnp.zeros((total, states), F32)
        seen = jnp.zeros((total, states), F32)
        for i in range(WORD):
            error = at(obs, i) - mul(priors[i], held[6])
            squares = squares + at(mask, i) * error * error
            seen = seen + at(mask, i)
        squares = active * jnp.sum(squares, axis=0, keepdims=True)
        number = jnp.sum(seen, axis=0, keepdims=True)
        sum_buf[...] = jnp.where(row8 == 0, jnp.broadcast_to(squares, (8, states)), jnp.broadcast_to(number, (8, states)))
        for e in range(1, n):
            @pl.when(pos + e >= n)
            def _(e=e):
                send_sum(e - 1).start()

        for e in range(n - 1, 0, -1):
            @pl.when(pos + e < n)
            def _(e=e):
                send_sum(e - 1).start()

    def quick():
        start = ents[...]
        y = times(start, jnp.concatenate([step_rhs[...]] + [tall(pair_2[a]) for a in range(4)], axis=1))
        y = [y[:, k * states : (k + 1) * states] for k in range(6)]
        on = [at(mask, i) > 0.5 for i in range(2)]
        one = y[0] + jnp.where(on[0], y[1], 0.0) + at(drive, 0)
        two = jnp.where(on[0], jnp.where(on[1], y[5], y[4]), jnp.where(on[1], y[3], y[2])) + zero_2[...]
        score([start, one, two, advance(two, 2)[0]])

    def priors_held():
        return [prior[i * total : (i + 1) * total, :] for i in range(WORD)]

    @pl.when(headed)
    def _():
        x = state[...]
        spread = jnp.concatenate([jnp.concatenate([tall(heads[b * chunks + k]) for k in range(1, chunks)], axis=1) for b in range(seqs)], axis=0)
        y = product(lefts(x), spread)
        for b in range(seqs):
            ents[b * chunks : b * chunks + 1, :] = x[b : b + 1]
            for k in range(1, chunks):
                r = b * chunks + k
                ents[r : r + 1, :] = y[b : b + 1, (k - 1) * states : k * states] + head_vecs[r : r + 1, :]
        quick()

    @pl.when(jnp.logical_not(jnp.logical_or(headed, has_comp)))
    def _():
        sweep(state[...])

    @pl.when(direct)
    def _():
        quick()

    x = ents[...]
    for i in range(WORD):
        prior[i * total : (i + 1) * total, :] = x
        x, move = advance(x, i)
        filt[i * total : (i + 1) * total, :] = x
        moves[i * total : (i + 1) * total, :] = move

    chunk8[...] = jnp.zeros_like(chunk8)
    for i in range(WORD - 1):
        z = combine(moves, i)
        suffix[i * total : (i + 1) * total, :] = filt[i * total : (i + 1) * total, :] + z
        if i == 0:
            z = z + moves[0:total, :]
            for b in range(seqs):
                chunk8[pl.ds(b, chunks, stride=8), :] = z[b * chunks : (b + 1) * chunks]
    i = WORD - 1
    suffix[i * total : (i + 1) * total, :] = filt[i * total : (i + 1) * total, :]
    ends = chunk8[...].reshape(chunks, 8, states)

    ups = [ends]
    for level in range(levels):
        pair = ups[-1].reshape(ups[-1].shape[0] // 2, 2, 8, states)
        half = pair.shape[0]
        later = times(pair[:, 1].reshape(half * 8, states), tall(powers[1 << level]))
        ups.append(pair[:, 0] + later.reshape(half, 8, states))

    def send_first(slot, side):
        dst = off_in.at[0] if slot == 0 else first_in
        return pltpu.make_async_remote_copy(
            src_ref=off_out, dst_ref=dst, send_sem=off_send.at[0],
            recv_sem=off_recv.at[0] if slot == 0 else first_sem,
            device_id={"tm": side}, device_id_type=MESH,
        )

    @pl.when(near_4)
    def _():
        off_out[...] = ups[-1].reshape(8, states)
        near_out[...] = ups[-1].reshape(8, states)
        for slot in range(2):
            @pl.when(pos == 2 + slot)
            def _(slot=slot):
                send_first(slot, 0).start()
                send_first(slot, 1).start()

        @pl.when(odd)
        def _():
            near.start()

        score(priors_held())

    x = jnp.zeros((1, 8, states), F32)
    for level in range(levels - 1, -1, -1):
        count = x.shape[0]
        pair = ups[level].reshape(count, 2, 8, states)
        if level == levels - 1:
            sooner = pair[:, 1]
        else:
            moved = times(x.reshape(count * 8, states), tall(powers[1 << level]))
            sooner = moved.reshape(count, 8, states) + pair[:, 1]
        x = jnp.stack([sooner, x], axis=1).reshape(2 * count, 8, states)
    chunk8[...] = x.reshape(chunks * 8, states)
    fill()

    @pl.when(even)
    def _():
        near.wait_recv()

    @pl.when(chip == 0)
    def _():
        send_first(1, 0).wait_recv()

    for d in range(1, chips):
        @pl.when(chip + d < chips)
        def _(d=d):
            send_off(d, 0).wait_recv()

    left = jnp.concatenate([twice(stacked(a)) for a in [first_in[...]] + [off_in[d] for d in range(chips - 1)]], axis=1)
    rhs = jnp.concatenate([tall(laps[2 - par])] + [tall(laps[2 * d + 1 - par]) for d in range(chips - 1)], axis=0)
    x = near_in[...] + product(left, rhs)
    y = times(x, jnp.concatenate([tall(powers[chunks - 1 - k]) for k in range(chunks)], axis=1))
    for k in range(chunks):
        chunk8[k * 8 : (k + 1) * 8, :] += y[:, k * states : (k + 1) * states]
    x = jnp.concatenate([chunk8[pl.ds(b, chunks, stride=8), :] for b in range(seqs)], axis=0)
    y = times(x, jnp.concatenate([tall(a) for a in (held[3], held[2], held[1], held[0])], axis=1))
    for i in range(WORD):
        out[pl.ds(i, total, stride=WORD), :] = (
            suffix[i * total : (i + 1) * total, :] + y[:, i * states : (i + 1) * states]
        )

    @pl.when(gives_mat)
    def _():
        arrived(mat_out, mat_sem.at[0])

        @pl.when(quarter == 0)
        def _():
            arrived(mat_out.at[pl.ds(0, block)], early_sem.at[0])

    @pl.when(jnp.logical_and(gives_mat, far))
    def _():
        psi.wait_send()

    @pl.when(gives_comp)
    def _():
        arrived(comp_out.at[rest], comp_sem.at[0])
        arrived(mat_out.at[pl.ds(0, block)], early_sem.at[0])

    @pl.when(pos == 0)
    def _():
        to_next[2].wait_send()

    @pl.when(pos == 1)
    def _():
        arrived(off_in.at[pl.ds(0, 2)], vec_send.at[0])

    @pl.when(last_of_four)
    def _():
        arrived(off_in.at[pl.ds(0, 3)], vec_send.at[0])

    @pl.when(has_comp)
    def _():
        to_back.wait_send()

    @pl.when(odd)
    def _():
        near.wait_send()

    for d in range(1, chips):
        @pl.when(jnp.logical_and(jnp.logical_and(odd, far), chip - d >= 0))
        def _(d=d):
            arrived(off_in.at[pl.ds(0, 2)], off_send.at[d - 1])

    for slot in range(2):
        @pl.when(pos == 2 + slot)
        def _(slot=slot):
            arrived(off_in.at[pl.ds(0, 2)], off_send.at[0])

    arrived(sum_in.at[pl.ds(0, n - 1)], sum_sem.at[0])

    arrived(sum_in.at[pl.ds(0, n - 1)], sum_sem.at[1])
    sums = sum_buf[...]
    for d in range(n - 1):
        sums = sums + sum_in[d]
    squares, number = sums[0:1], sums[1:2]
    grad = 0.5 * active * (number - weight * squares)
    new_prec[...] = log_prec[...] + grad / (seqs * steps * n)
    terms = 0.5 * active * (log_prec[...] * number - weight * squares)
    loglik[...] = jnp.zeros_like(terms) + jnp.sum(terms, axis=1, keepdims=True) / (seqs * steps * n * states)


def mul_node(left, right):
    return split(wide(left, deep(right))[0])


def finish(smoothed, new_prec, loglik, out, out_prec, out_loglik):
    out[...] = smoothed[...]
    out_prec[...] = new_prec[...]
    out_loglik[...] = loglik[:, 0:1]


def local(n, obs, present, sensors, log_prec, dynamics, prior_var, obs_map, init_state):
    seqs, steps, channels = obs.shape
    states = dynamics.shape[0]
    assert n % 4 == 0 and states == 128 and channels == 128
    chunks = steps // WORD
    total = seqs * chunks
    chips = n // 2
    inner = sum(total >> level for level in range(1, int(math.log2(chunks)) + 1))
    vmem = pl.BlockSpec(memory_space=pltpu.VMEM)
    smem = pl.BlockSpec(memory_space=pltpu.SMEM)
    hbm = pl.BlockSpec(memory_space=pl.ANY)
    rows = seqs * steps
    block = seqs * (states + EXTRA)
    node = (states, 2 * states)
    tile = pltpu.VMEM((8, states), F32)
    whole = pltpu.VMEM((block, states), F32)
    level_rows = (inner + 7) // 8 * 8
    dma = pltpu.SemaphoreType.DMA
    smoothed, new_prec, loglik = pl.pallas_call(
        functools.partial(kernel, n, seqs, steps),
        out_shape=(
            pltpu.VMEM((rows, states), F32),
            pltpu.VMEM((1, channels), F32),
            pltpu.VMEM((1, channels), F32),
        ),
        in_specs=[hbm, smem] + [hbm] * 6,
        out_specs=(vmem, vmem, vmem),
        scratch_shapes=[
            pltpu.VMEM((states, states), F32),
            pltpu.VMEM((channels, states), F32),
            pltpu.VMEM((1, channels), F32),
            pltpu.VMEM((1, states), F32),
            pltpu.SMEM((seqs, steps), jnp.int32),
            pltpu.VMEM((seqs, steps), jnp.int32),
            pltpu.VMEM((rows, channels), F32),
            pltpu.VMEM((seqs, states), F32),
            dma((8,)),
            pltpu.SMEM((total,), jnp.int32),
            pltpu.VMEM((2**WORD,) + node, BF16),
            pltpu.VMEM((2**WORD, states, states), F32),
            pltpu.VMEM((2**WORD,) + node, BF16),
            pltpu.VMEM((inner,) + node, BF16),
            pltpu.VMEM((level_rows, states), F32),
            pltpu.VMEM((inner, states, states), F32),
            pltpu.VMEM((inner,) + node, BF16),
            pltpu.VMEM((level_rows, states), F32),
            pltpu.VMEM((total, states), F32),
            pltpu.VMEM((total, states), F32),
            pltpu.VMEM((total, states), F32),
            pltpu.VMEM((total, states), F32),
            pltpu.VMEM((chunks + 1,) + node, BF16),
            pltpu.VMEM((2 * chips - 2,) + node, BF16),
            pltpu.VMEM((2 * states, 2 * states), BF16),
            pltpu.VMEM((rows, states), F32),
            pltpu.VMEM((rows, states), F32),
            pltpu.VMEM((rows, states), F32),
            pltpu.VMEM((rows, states), F32),
            pltpu.VMEM((rows, states), F32),
            pltpu.VMEM((chunks * 8, states), F32),
            pltpu.VMEM((rows, states), F32),
            pltpu.VMEM((8,) + node, BF16),
            pltpu.VMEM((4,) + node, BF16),
            pltpu.VMEM((total, states), F32),
            pltpu.VMEM((3, states, states), F32),
            pltpu.VMEM((states, 6 * states), BF16),
            whole,
            pltpu.VMEM((total,) + node, BF16),
            pltpu.VMEM((total, states), F32),
            pltpu.VMEM((seqs,) + node, BF16), tile,
            pltpu.VMEM((seqs,) + node, BF16), tile,
            pltpu.VMEM((seqs,) + node, BF16), tile,
            pltpu.VMEM((seqs,) + node, BF16), tile,
            pltpu.VMEM((seqs,) + node, BF16), tile,
            tile,
            tile, tile, tile, whole, whole, whole, whole, pltpu.VMEM((2 * (states + EXTRA), states), F32), whole, whole,
            tile, pltpu.VMEM((chips - 1, 8, states), F32), tile, tile, tile, tile, pltpu.VMEM((n, 8, states), F32),
            dma((2,)), dma(()), dma((1 + seqs,)), dma((3,)), dma((2,)), dma((2,)), dma((2,)),
            dma((chips - 1,)), dma((chips - 1,)), dma(()), dma((2,)),
        ],
        compiler_params=pltpu.CompilerParams(collective_id=0, has_side_effects=True),
        name="kalman",
    )(
        present, sensors, obs.reshape(rows, channels), log_prec.reshape(1, channels),
        dynamics, prior_var.reshape(1, states), obs_map, init_state,
    )
    held = [pltpu.with_memory_space_constraint(a, pltpu.VMEM) for a in (smoothed, new_prec, loglik)]
    smoothed, new_prec, loglik = pl.pallas_call(
        finish,
        out_shape=(
            jax.ShapeDtypeStruct((rows, states), F32),
            jax.ShapeDtypeStruct((1, channels), F32),
            jax.ShapeDtypeStruct((1, 1), F32),
        ),
        in_specs=[vmem] * 3,
        out_specs=(vmem, vmem, vmem),
        name="finish",
    )(*held)
    return smoothed.reshape(seqs, steps, states), new_prec.reshape(channels), loglik.reshape(1)


def solution(mesh):
    in_specs = (
        P("cluster", "tm", None),
        P("cluster", "tm"),
        P("cluster"),
        P("cluster"),
        P("cluster", None),
        P("cluster"),
        P("cluster", None),
        P("cluster", None),
    )
    out_specs = (P("cluster", "tm", None), P("cluster"), P("cluster"))
    body = functools.partial(local, mesh.shape["tm"])
    return jax.shard_map(body, mesh=mesh, in_specs=in_specs, out_specs=out_specs, check_vma=False)
```
